128 devices in a mesh: row: 16 (over y, x), col: 8 (over z, core).
Axes of the slice: x: 4, y: 4, z: 4, core: 2. Of those that a mesh axis runs over, the one named last changes fastest.
Arguments:
- tangents: float32 [192, 128, 6144], P('row', None, 'col'), may hold values from -6 to 6
- base_flow: float32 [192, 128, 192], P('row', None, 'col'), may hold values from -0.0625 to 0.0625
- mode_mask: int32 [192, 192], P('row', 'col'), may hold values 0 or 1
- decay_rates: float32 [128], replicated, may hold values from 1 to 100
- to_eigen: float32 [128, 128], replicated, may hold values from -0.5 to 0.5
- from_eigen: float32 [128, 128], replicated, may hold values from -0.5 to 0.5
Outputs:
- vectors: float32 [192, 128, 6144], P('row', None, 'col')
- growth: float32 [32], replicated
The draws below stay inside these ranges and needn't reach their ends.
Inputs may be any that keep to these rules, and one draw needn't show every extreme that they name: `mode_mask`: 1 keeps a mode pair of the linearized product, 0 removes it.
All inputs are finite; a program needn't handle non-finite values. No bound on the sum of `mode_mask` on one device may be relied on, other than what follows from the above.
Results may differ from the reference program's by a relative error of at most 0.00005.
Values sent between devices are 32-bit elements; how exact they have to be, the bound alone decides.
No kernel may reach another device: no remote copies, remote signals or barrier semaphores. Data moves between devices by JAX's collectives and lax.ppermute only.
A program may use at most 128 MiB of HBM per device.

```python
import math
import jax
import jax.numpy as jnp
from jax import lax

NX = 192
NY = 128
NZ = 192
NV = 32


def plant(values, rng, least, top_value):
    longest = values.shape.index(max(values.shape))
    spots = []
    for shift in (0, 1):
        where = [jax.random.randint(jax.random.fold_in(rng, axis), (), 0, length) for axis, length in enumerate(values.shape)]
        where[longest] = (where[longest] + shift) % values.shape[longest]
        spots.append(tuple(where))
    return values.at[spots[0]].set(least).at[spots[1]].set(top_value)


def block_scale(rng, shape, pieces, least, high):
    factor_of, own = 1.0, jax.random.fold_in(rng, 6)
    for axis_at, parts in pieces:
        heights = jnp.exp(jax.random.uniform(jax.random.fold_in(own, axis_at), (parts,), jnp.float32, least / len(pieces), high / len(pieces)))
        factor_of = factor_of * jnp.repeat(heights, shape[axis_at] // parts).reshape([-1 if axis == axis_at else 1 for axis in range(len(shape))])
    return factor_of


def centred(rng, dims, deviation, most, cuts=(), kind=jnp.bfloat16):
    drawn = deviation * jax.random.normal(rng, dims, jnp.float32)
    if cuts:
        drawn = drawn * block_scale(rng, dims, cuts, -0.22, 0.18)
    return jnp.clip(drawn, -most, most).astype(kind)


def setup_inputs(seed: int = 0) -> dict:
    key_list = jax.random.split(jax.random.key(seed), 7)
    tangents = centred(key_list[0], (NX, NY, NZ * NV), 1.0, 6.0, ((0, 16), (2, 8)), jnp.float32)
    base_flow = centred(key_list[1], (NX, NY, NZ), (NX * NZ // 4) ** -0.5, 0.0625, ((0, 16), (2, 8)), jnp.float32)
    mode_mask = plant((jax.random.randint(key_list[2], (NX, NZ), 0, 4) < 3).astype(jnp.int32), jax.random.fold_in(key_list[2], 1), 0, 1)
    decay_rates = jnp.clip(jnp.exp(jax.random.uniform(key_list[3], (NY,), jnp.float32, math.log(1.0), math.log(100.0))), 1.0, 100.0)
    to_eigen = centred(key_list[4], (NY, NY), NY ** -0.5, 0.5, (), jnp.float32)
    from_eigen = centred(key_list[5], (NY, NY), NY ** -0.5, 0.5, (), jnp.float32)
    return dict(tangents=tangents, base_flow=base_flow, mode_mask=mode_mask, decay_rates=decay_rates, to_eigen=to_eigen, from_eigen=from_eigen)


PRECISE = lax.Precision.HIGHEST
STEP_COEF = 10.0
VISCOSITY = 0.01
ALPHA_X = 0.5
BETA_Z = 1.0

def local_waves(points_count, first_index, length):
    indices = first_index + jnp.arange(length, dtype=jnp.int32)
    middle = points_count // 2
    return jnp.where(indices <= middle, indices, indices - middle).astype(jnp.float32)

def synthesis(points_count):
    points = jnp.arange(points_count, dtype=jnp.int32)[:, None]
    mode_index = jnp.arange(points_count, dtype=jnp.int32)[None, :]
    middle = points_count // 2
    wave_index = jnp.where(mode_index <= middle, mode_index, mode_index - middle)
    turn_count = (points * wave_index % points_count).astype(jnp.float32)
    angles = turn_count * (2.0 * math.pi / points_count)
    return jnp.where(mode_index <= middle, jnp.cos(angles), jnp.sin(angles))

def analysis(points_count):
    mode_index = jnp.arange(points_count, dtype=jnp.int32)
    middle = points_count // 2
    weights = jnp.where((mode_index == 0) | (mode_index == middle), jnp.float32(1.0 / points_count), jnp.float32(2.0 / points_count))
    return weights[:, None] * synthesis(points_count).T

def derivative_analysis(points_count, wave_scale):
    rows_index = jnp.arange(points_count, dtype=jnp.int32)[:, None]
    cols_index = jnp.arange(points_count, dtype=jnp.int32)[None, :]
    middle = points_count // 2
    rising = (cols_index == rows_index + middle) & (rows_index >= 1) & (rows_index < middle)
    falling = (rows_index == cols_index + middle) & (cols_index >= 1) & (cols_index < middle)
    rows_float = jnp.broadcast_to(rows_index.astype(jnp.float32), (points_count, points_count))
    cols_float = jnp.broadcast_to(cols_index.astype(jnp.float32), (points_count, points_count))
    derivative = jnp.where(rising, rows_float, jnp.float32(0.0)) - jnp.where(falling, cols_float, jnp.float32(0.0))
    return -wave_scale * jnp.dot(derivative, analysis(points_count), precision=PRECISE)

def denominators(decay_rates, x_count, z_count, x_start, z_start, x_length, z_length):
    wave_x = ALPHA_X * local_waves(x_count, x_start, x_length)
    wave_z = BETA_Z * local_waves(z_count, z_start, z_length)
    return STEP_COEF + VISCOSITY * (wave_x[:, None, None] ** 2 + wave_z[None, None, :] ** 2) + decay_rates[None, :, None]

def reference(tangents, base_flow, mode_mask, decay_rates, to_eigen, from_eigen):
    x_count, y_count, z_count = base_flow.shape
    vec_count = tangents.shape[2] // z_count
    fields = jnp.transpose(tangents.reshape(x_count, y_count, z_count, vec_count), (3, 0, 1, 2))
    x_synthesis = synthesis(x_count)
    z_synthesis = synthesis(z_count)
    x_derivative = derivative_analysis(x_count, ALPHA_X)
    z_analysis = analysis(z_count)
    speed_field = jnp.einsum('pm,myn->pyn', x_synthesis, base_flow, precision=PRECISE)
    speed_field = jnp.einsum('pyn,sn->pys', speed_field, z_synthesis, precision=PRECISE)
    divisor = denominators(decay_rates, x_count, z_count, 0, 0, x_count, z_count)
    retained = mode_mask.astype(jnp.float32)[:, None, :]

    def advance(one_field):
        physical = jnp.einsum('pm,myn->pyn', x_synthesis, one_field, precision=PRECISE)
        physical = jnp.einsum('pyn,sn->pys', physical, z_synthesis, precision=PRECISE)
        product = speed_field * physical
        returned = jnp.einsum('mp,pys->mys', x_derivative, product, precision=PRECISE)
        returned = jnp.einsum('mys,ns->myn', returned, z_analysis, precision=PRECISE)
        right_side = STEP_COEF * one_field + retained * returned
        eigen_part = jnp.einsum('ji,min->mjn', to_eigen, right_side, precision=PRECISE) / divisor
        return jnp.einsum('yj,mjn->myn', from_eigen, eigen_part, precision=PRECISE)
    stepped = lax.map(advance, fields)
    cell_count = x_count * y_count * z_count
    gram_matrix = jnp.einsum('vmyn,umyn->vu', stepped, stepped, precision=PRECISE) / cell_count
    lower_factor = jnp.linalg.cholesky(gram_matrix)
    identity = jnp.eye(vec_count, dtype=jnp.float32)
    inverse = jax.scipy.linalg.solve_triangular(lower_factor, identity, lower=True)
    orthonormal = jnp.einsum('uv,vmyn->mynu', inverse, stepped, precision=PRECISE)
    growth = jnp.log(jnp.diagonal(lower_factor))
    return (orthonormal.reshape(x_count, y_count, z_count * vec_count), growth)
```

```python
import functools

import jax
import jax.numpy as jnp
import numpy as np
from jax import lax
from jax.experimental import pallas as pl
from jax.experimental.pallas import tpu as pltpu
from jax.sharding import PartitionSpec as P

STEP_COEF = 10.0
VISCOSITY = 0.01
ALPHA_X = 0.5
BETA_Z = 1.0
LANES = 128
F32 = jnp.float32
BF16 = jnp.bfloat16
NN = (((1,), (0,)), ((), ()))
NT = (((1,), (1,)), ((), ()))
TN = (((0,), (0,)), ((), ()))


def synthesis(count):
    points = np.arange(count)[:, None]
    modes = np.arange(count)[None, :]
    middle = count // 2
    waves = np.where(modes <= middle, modes, modes - middle)
    angles = (points * waves % count) * (2.0 * np.pi / count)
    return np.where(modes <= middle, np.cos(angles), np.sin(angles))


def analysis(count):
    modes = np.arange(count)
    weights = np.where((modes == 0) | (modes == count // 2), 1.0 / count, 2.0 / count)
    return weights[:, None] * synthesis(count).T


def derivative_analysis(count, scale):
    middle = count // 2
    derivative = np.zeros((count, count))
    for k in range(1, middle):
        derivative[k, middle + k] = k
        derivative[middle + k, k] = -k
    return -scale * (derivative @ analysis(count))


def halves_of_table(table):
    table = np.asarray(table, np.float64)
    high = table.astype(np.float32).astype(jnp.bfloat16)
    low = (table - high.astype(np.float64)).astype(np.float32).astype(jnp.bfloat16)
    return np.stack([high, low])


def split(x):
    high = x.astype(BF16)
    return high, (x - high.astype(F32)).astype(BF16)


def dot(a, b, dims):
    return lax.dot_general(a, b, dims, preferred_element_type=F32)


def dot3(a, b, dims):
    return dot(a[0], b[0], dims) + (dot(a[0], b[1], dims) + dot(a[1], b[0], dims))


def pack_kernel(q_ref, out_ref, *, rows, modes, planes, tiles):
    def step(m, carry):
        for nb in range(tiles):
            out_ref[pl.ds(nb * modes + m, planes, stride=rows), :] = q_ref[
                m, :, nb * LANES : (nb + 1) * LANES
            ]
        return carry

    lax.fori_loop(0, modes, step, 0)


def transform_kernel(
    d_ref, speed_ref, sx_ref, sz_ref, az_ref, g_ref, out_ref, *y_refs,
    rows, modes, row_devices, col_devices, tiles, vecs,
):
    count = modes * row_devices
    hop = col_devices * rows

    def forward_x(t, carry):
        c, nb = t // tiles, t % tiles
        start = c * rows + nb * modes
        pieces = [
            d_ref[pl.ds(start + m, row_devices, stride=hop), :] for m in range(modes)
        ]
        block = jnp.concatenate(pieces, axis=0)
        part = split(block.T)
        mixed = dot3(part, (sx_ref[0], sx_ref[1]), NN)
        at = pl.ds(pl.multiple_of(t * LANES, LANES), LANES)
        for k, y_ref in enumerate(y_refs):
            y_ref[at, :] = mixed[:, k * LANES : (k + 1) * LANES]
        return carry

    lax.fori_loop(0, col_devices * tiles, forward_x, 0)

    def plane(v, carry):
        at = pl.ds(v, count, stride=vecs)
        mixed = jnp.concatenate([y_ref[at, :] for y_ref in y_refs], axis=1)
        physical = dot3((sz_ref[0], sz_ref[1]), split(mixed), NN)
        product = physical * speed_ref[...]
        mixed = dot3((az_ref[0], az_ref[1]), split(product), NN)
        for k, y_ref in enumerate(y_refs):
            y_ref[at, :] = mixed[:, k * LANES : (k + 1) * LANES]
        return carry

    lax.fori_loop(0, vecs, plane, 0)

    def inverse_x(t, carry):
        c, nb = t // tiles, t % tiles
        start = c * rows + nb * modes
        at = pl.ds(pl.multiple_of(t * LANES, LANES), LANES)
        block = split(jnp.concatenate([y_ref[at, :] for y_ref in y_refs], axis=1))
        back = dot3((g_ref[0], g_ref[1]), block, NT)
        for m in range(modes):
            out_ref[pl.ds(start + m, row_devices, stride=hop), :] = back[
                m * row_devices : (m + 1) * row_devices
            ]
        return carry

    lax.fori_loop(0, col_devices * tiles, inverse_x, 0)


def column_kernel(
    nl_ref, q_ref, mask_ref, wave_ref, decay_ref, to_ref, from_ref, stepped_ref, gram_ref,
    *, rows, modes, planes, tiles, vecs, cells,
):
    to_eigen = split(to_ref[...])
    from_eigen = split(from_ref[...])
    decay = jnp.broadcast_to(decay_ref[...], (planes, tiles * LANES))

    def step(m, carry):
        high, cross = carry
        nonlinear = jnp.concatenate(
            [nl_ref[pl.ds(nb * modes + m, planes, stride=rows), :] for nb in range(tiles)],
            axis=1,
        )
        right = STEP_COEF * q_ref[m] + nonlinear * mask_ref[pl.ds(m, 1), :]
        eigen = dot3(to_eigen, split(right), NN)
        eigen = eigen / (wave_ref[pl.ds(m, 1), :] + decay)
        stepped = dot3(from_eigen, split(eigen), NN)
        stepped_ref[m] = stepped
        part = split(stepped)
        stacked = [
            jnp.concatenate([x[:, nb * LANES : (nb + 1) * LANES] for nb in range(tiles)], axis=0)
            for x in part
        ]
        return (
            high + dot(stacked[0], stacked[0], TN),
            cross + dot(stacked[0], stacked[1], TN),
        )

    zero = jnp.zeros((LANES, LANES), F32)
    high, cross = lax.fori_loop(0, modes, step, (zero, zero))
    full = (high + (cross + cross.T)) * (1.0 / cells)
    group = LANES // vecs
    lane = lax.broadcasted_iota(jnp.int32, (vecs, LANES), 1) // vecs
    folded = jnp.zeros((vecs, LANES), F32)
    for k in range(group):
        folded = folded + jnp.where(lane == k, full[k * vecs : (k + 1) * vecs], 0.0)
    folded = folded + pltpu.roll(folded, LANES // 2, 1)
    folded = folded + pltpu.roll(folded, LANES // 4, 1)
    piece = vecs // group
    lane = lax.broadcasted_iota(jnp.int32, (piece, LANES), 1) // vecs
    packed = jnp.zeros((piece, LANES), F32)
    for k in range(group):
        packed = jnp.where(lane == k, folded[k * piece : (k + 1) * piece], packed)
    gram_ref[...] = packed


def finish_kernel(grams_ref, stepped_ref, vectors_ref, growth_ref, w_ref, *, devices, vecs, wide):
    group = LANES // vecs
    piece = vecs // group

    @pl.when(pl.program_id(0) == 0)
    def _():
        packed = jnp.sum(grams_ref[...].reshape(devices, piece, LANES), axis=0)
        gram = jnp.concatenate(
            [pltpu.roll(packed, (LANES - k * vecs) % LANES, 1) for k in range(group)], axis=0
        )
        lane = lax.broadcasted_iota(jnp.int32, (vecs, LANES), 1)
        row = lax.broadcasted_iota(jnp.int32, (vecs, LANES), 0)
        work = jnp.where(lane < vecs, gram, jnp.where(lane == row + vecs, 1.0, 0.0))
        for k in range(vecs - 1):
            pivot_row = work[k : k + 1, :]
            scaled = pivot_row / work[k : k + 1, k : k + 1]
            column = jnp.broadcast_to(work[:, k : k + 1], (vecs, LANES))
            work = work - jnp.where(row > k, column * scaled, 0.0)
        pivots = jnp.sum(jnp.where(lane == row, work, 0.0), axis=1, keepdims=True)
        diagonal = jnp.sqrt(pivots)
        inverse = work / diagonal
        across = jnp.sum(jnp.where(lane == row, diagonal, 0.0), axis=0, keepdims=True)
        growth_ref[...] = jnp.log(jnp.where(lane[:1] < vecs, across, 1.0))
        inverse = jnp.where((lane >= vecs) & (lane < 2 * vecs), inverse, 0.0)
        inverse = inverse + pltpu.roll(inverse, LANES // 2, 1)
        inverse = inverse + pltpu.roll(inverse, LANES // 4, 1)
        repeats = wide // vecs
        tall = jnp.concatenate([inverse] * repeats, axis=0)
        tall = jnp.concatenate([tall] * (wide // LANES), axis=1)
        rows = lax.broadcasted_iota(jnp.int32, (wide, wide), 0) // vecs
        cols = lax.broadcasted_iota(jnp.int32, (wide, wide), 1) // vecs
        w_high, w_low = split(jnp.where(rows == cols, tall, 0.0))
        w_ref[0] = w_high
        w_ref[1] = w_low

    w = (w_ref[0], w_ref[1])
    for k in range(stepped_ref.shape[1] // wide):
        at = slice(k * wide, (k + 1) * wide)
        vectors_ref[:, at] = dot3(split(stepped_ref[:, at]), w, NT)


def vmem():
    return pl.BlockSpec(memory_space=pltpu.VMEM)


def cost(flops, moved):
    return pl.CostEstimate(flops=int(flops), bytes_accessed=int(moved), transcendentals=0)


def waves(count, first, length):
    index = first + jnp.arange(length, dtype=jnp.int32)
    return jnp.where(index <= count // 2, index, index - count // 2).astype(F32)


def body(tangents, base_flow, mode_mask, decay_rates, to_eigen, from_eigen):
    modes, planes, width = tangents.shape
    z_length = base_flow.shape[2]
    vecs = width // z_length
    row_devices, col_devices = lax.axis_size("row"), lax.axis_size("col")
    devices = row_devices * col_devices
    x_count, z_count = modes * row_devices, z_length * col_devices
    tiles = width // LANES
    rows = modes * tiles
    size = tangents.size * 4
    both = ("row", "col")

    order = np.arange(x_count)
    order = (order % row_devices) * modes + order // row_devices
    x_synthesis, z_synthesis = synthesis(x_count), synthesis(z_count)
    points = -(-x_count // LANES) * LANES
    extra = ((0, 0), (0, points - x_count))
    sx = halves_of_table(np.pad(x_synthesis[:, order].T, extra))
    sz = halves_of_table(z_synthesis)
    az = halves_of_table(analysis(z_count))
    gx = halves_of_table(np.pad(derivative_analysis(x_count, ALPHA_X)[order], extra))

    packed = pl.pallas_call(
        functools.partial(pack_kernel, rows=rows, modes=modes, planes=planes, tiles=tiles),
        out_shape=jax.ShapeDtypeStruct((planes * rows, LANES), F32),
        in_specs=[vmem()],
        out_specs=vmem(),
        cost_estimate=cost(0, 2 * size),
        name="pack",
    )(tangents)
    received = lax.all_to_all(packed.reshape(devices, rows, LANES), both, 0, 0, tiled=True)

    base = jnp.transpose(base_flow, (1, 0, 2)).reshape(devices, modes * z_length)
    base = lax.all_to_all(base, both, 0, 0, tiled=True)
    base = base.reshape(row_devices, col_devices, modes, z_length)
    base = jnp.transpose(base, (0, 2, 1, 3)).reshape(x_count, z_count)
    speed = jnp.dot(base, z_synthesis.T.astype(np.float32), precision=lax.Precision.HIGHEST)
    speed = lax.dot_general(
        speed, np.pad(x_synthesis.T, extra).astype(np.float32), TN, precision=lax.Precision.HIGHEST
    )

    flops = 8 * x_count * z_count * (x_count + z_count) * vecs
    returned = pl.pallas_call(
        functools.partial(
            transform_kernel, rows=rows, modes=modes, row_devices=row_devices,
            col_devices=col_devices, tiles=tiles, vecs=vecs,
        ),
        out_shape=jax.ShapeDtypeStruct((devices * rows, LANES), F32),
        in_specs=[vmem()] * 6,
        out_specs=vmem(),
        scratch_shapes=[pltpu.VMEM((z_count * vecs, LANES), F32)] * (points // LANES),
        cost_estimate=cost(flops, 2 * size),
        compiler_params=pltpu.CompilerParams(vmem_limit_bytes=48 * 2**20),
        name="transform",
    )(received.reshape(devices * rows, LANES), speed, sx, sz, az, gx)
    nonlinear = lax.all_to_all(returned.reshape(devices, rows, LANES), both, 0, 0, tiled=True)

    wave_x = ALPHA_X * waves(x_count, lax.axis_index("row") * modes, modes)
    wave_z = BETA_Z * waves(z_count, lax.axis_index("col") * z_length, z_length)
    wave = STEP_COEF + VISCOSITY * (wave_x[:, None] ** 2 + jnp.repeat(wave_z, vecs)[None, :] ** 2)
    mask = jnp.repeat(mode_mask.astype(F32), vecs, axis=1)
    stepped, gram = pl.pallas_call(
        functools.partial(
            column_kernel, rows=rows, modes=modes, planes=planes, tiles=tiles, vecs=vecs,
            cells=x_count * planes * z_count,
        ),
        out_shape=[
            jax.ShapeDtypeStruct(tangents.shape, F32),
            jax.ShapeDtypeStruct((vecs * vecs // LANES, LANES), F32),
        ],
        in_specs=[vmem()] * 7,
        out_specs=[vmem()] * 2,
        cost_estimate=cost(4 * planes * planes * modes * width, 3 * size),
        compiler_params=pltpu.CompilerParams(vmem_limit_bytes=48 * 2**20),
        name="column",
    )(
        nonlinear.reshape(planes * rows, LANES), tangents, mask, wave,
        decay_rates[:, None], to_eigen, from_eigen,
    )

    piece = vecs * vecs // LANES
    grams = lax.all_to_all(
        jnp.broadcast_to(gram[None], (devices, piece, LANES)), both, 0, 0, tiled=True
    ).reshape(devices * piece, LANES)

    height = modes * planes
    block = height // 6
    vectors, growth = pl.pallas_call(
        functools.partial(finish_kernel, devices=devices, vecs=vecs, wide=2 * LANES),
        out_shape=[
            jax.ShapeDtypeStruct((height, width), F32),
            jax.ShapeDtypeStruct((1, LANES), F32),
        ],
        grid=(height // block,),
        in_specs=[
            pl.BlockSpec((devices * piece, LANES), lambda i: (0, 0)),
            pl.BlockSpec((block, width), lambda i: (i, 0)),
        ],
        out_specs=[
            pl.BlockSpec((block, width), lambda i: (i, 0)),
            pl.BlockSpec((1, LANES), lambda i: (0, 0)),
        ],
        scratch_shapes=[pltpu.VMEM((2, 2 * LANES, 2 * LANES), BF16)],
        cost_estimate=cost(2 * height * width * 256, 2 * size),
        name="finish",
    )(grams, stepped.reshape(height, width))
    return vectors.reshape(tangents.shape), growth[0, :vecs]


def solution(mesh):
    placed = (P("row", None, "col"), P("row", None, "col"), P("row", "col"), P(), P(), P())
    return jax.shard_map(
        body, mesh=mesh, in_specs=placed, out_specs=(P("row", None, "col"), P()), check_vma=False
    )
```

```python
import functools

import jax
import jax.numpy as jnp
import numpy as np
from jax import lax
from jax.experimental import pallas as pl
from jax.experimental.pallas import tpu as pltpu
from jax.sharding import PartitionSpec as P

STEP_COEF = 10.0
VISCOSITY = 0.01
ALPHA_X = 0.5
BETA_Z = 1.0
LANES = 128
F32 = jnp.float32
BF16 = jnp.bfloat16
NN = (((1,), (0,)), ((), ()))
NT = (((1,), (1,)), ((), ()))
TN = (((0,), (0,)), ((), ()))


def synthesis(count):
    points = np.arange(count)[:, None]
    modes = np.arange(count)[None, :]
    middle = count // 2
    waves = np.where(modes <= middle, modes, modes - middle)
    angles = (points * waves % count) * (2.0 * np.pi / count)
    return np.where(modes <= middle, np.cos(angles), np.sin(angles))


def analysis(count):
    modes = np.arange(count)
    weights = np.where((modes == 0) | (modes == count // 2), 1.0 / count, 2.0 / count)
    return weights[:, None] * synthesis(count).T


def derivative_analysis(count, scale):
    middle = count // 2
    derivative = np.zeros((count, count))
    for k in range(1, middle):
        derivative[k, middle + k] = k
        derivative[middle + k, k] = -k
    return -scale * (derivative @ analysis(count))


def halves_of_table(table):
    table = np.asarray(table, np.float64)
    high = table.astype(np.float32).astype(jnp.bfloat16)
    low = (table - high.astype(np.float64)).astype(np.float32).astype(jnp.bfloat16)
    return np.stack([high, low])


def split(x):
    high = x.astype(BF16)
    return high, (x - high.astype(F32)).astype(BF16)


def dot(a, b, dims):
    return lax.dot_general(a, b, dims, preferred_element_type=F32)


def dot3(a, b, dims):
    return dot(a[0], b[0], dims) + (dot(a[0], b[1], dims) + dot(a[1], b[0], dims))


def pack_kernel(q_ref, base_ref, out_ref, *, modes, planes, tiles, extra, step_modes):
    stride = modes * tiles + extra

    @pl.when(pl.program_id(0) == 0)
    def _():
        part = base_ref.shape[0] // extra
        fill = jnp.zeros((LANES - part, planes), F32)
        for k in range(extra):
            block = jnp.concatenate([base_ref[k * part : (k + 1) * part, :], fill], axis=0)
            out_ref[pl.ds(modes * tiles + k, planes, stride=stride), :] = block.T

    for k in range(step_modes):
        m = pl.program_id(0) * step_modes + k
        for nb in range(tiles):
            out_ref[pl.ds(nb * modes + m, planes, stride=stride), :] = q_ref[
                k, :, nb * LANES : (nb + 1) * LANES
            ]


def transform_kernel(
    d_ref, sx_ref, sz_ref, az_ref, g_ref, out_ref, speed_ref, *scratch,
    modes, row_devices, col_devices, tiles, extra, vecs,
):
    halves = len(scratch) // 2
    y_refs, z_refs = scratch[:halves], scratch[halves:]
    rows = modes * tiles
    stride = rows + extra
    hop = col_devices * stride
    x_count = modes * row_devices
    height = tiles * LANES

    turned = []
    for k in range(extra):
        block = jnp.concatenate(
            [
                d_ref[pl.ds(c * stride + rows + k, row_devices, stride=hop), :]
                for c in range(col_devices)
            ],
            axis=0,
        )
        turned.append(block.T)
    z_length = sz_ref.shape[2] // col_devices
    slot = lax.broadcasted_iota(jnp.int32, (z_length, LANES), 1) // row_devices
    slots = LANES // row_devices
    share = modes // extra
    sheets = []
    for c in range(col_devices):
        parts = [jnp.zeros((z_length, LANES), F32) for _ in range(halves)]
        for m in range(modes):
            piece = turned[m // share][(m % share) * z_length : (m % share + 1) * z_length]
            shift = ((m % slots - c) * row_devices) % LANES
            piece = pltpu.roll(piece, shift, 1) if shift else piece
            parts[m // slots] = jnp.where(slot == m % slots, piece, parts[m // slots])
        sheets.append(jnp.concatenate(parts, axis=1))
    base = jnp.concatenate(sheets, axis=0)[:, :x_count]
    half_way = dot3(split(base), (sx_ref[0], sx_ref[1]), NN)
    speed_ref[...] = dot3((sz_ref[0], sz_ref[1]), split(half_way), NN)

    def forward_x(c, carry):
        parts = []
        for nb in range(tiles):
            start = c * stride + nb * modes
            block = jnp.concatenate(
                [d_ref[pl.ds(start + m, row_devices, stride=hop), :] for m in range(modes)],
                axis=0,
            )
            parts.append(block.T)
        mixed = dot3(split(jnp.concatenate(parts, axis=0)), (sx_ref[0], sx_ref[1]), NN)
        at = pl.ds(pl.multiple_of(c * height, height), height)
        for k, y_ref in enumerate(y_refs):
            y_ref[at, :] = mixed[:, k * LANES : (k + 1) * LANES]
        return carry

    lax.fori_loop(0, col_devices, forward_x, 0, unroll=4)

    def plane(i, carry):
        for j in range(4):
            at = pl.ds(i * 4 + j, y_refs[0].shape[0] // vecs, stride=vecs)
            mixed = jnp.concatenate([y_ref[at, :] for y_ref in y_refs], axis=1)
            physical = dot3((sz_ref[0], sz_ref[1]), split(mixed), NN)
            product = physical * speed_ref[...]
            mixed = dot3((az_ref[0], az_ref[1]), split(product), NN)
            for k, z_ref in enumerate(z_refs):
                z_ref[at, :] = mixed[:, k * LANES : (k + 1) * LANES]
        return carry

    lax.fori_loop(0, vecs // 4, plane, 0, unroll=2)

    batch = 3

    def inverse_x(i, carry):
        at = pl.ds(pl.multiple_of(i * (batch * LANES), LANES), batch * LANES)
        block = split(jnp.concatenate([z_ref[at, :] for z_ref in z_refs], axis=1))
        back = dot3((g_ref[0], g_ref[1]), block, NT)
        c, group = i // (tiles // batch), i % (tiles // batch)
        for nb in range(batch):
            start = c * stride + (group * batch + nb) * modes
            for m in range(modes):
                out_ref[pl.ds(start + m, row_devices, stride=hop), :] = back[
                    m * row_devices : (m + 1) * row_devices, nb * LANES : (nb + 1) * LANES
                ]
        return carry

    stride = rows
    hop = col_devices * stride
    lax.fori_loop(0, col_devices * tiles // batch, inverse_x, 0, unroll=4)


def column_kernel(
    nl_ref, q_ref, mask_ref, decay_ref, to_ref, from_ref, stepped_ref, gram_ref,
    mask_s, wave_s, decay_s, high_s, cross_s,
    *, modes, planes, tiles, vecs, step_modes, x_count, z_count, z_length,
):
    width = tiles * LANES

    @pl.when(pl.program_id(0) == 0)
    def _():
        lane = lax.broadcasted_iota(jnp.int32, (z_length, width), 1) // vecs
        row = lax.broadcasted_iota(jnp.int32, (z_length, width), 0)
        spread = jnp.where(lane == row, 1.0, 0.0).astype(BF16)
        mask_s[...] = dot(mask_ref[...].astype(F32).astype(BF16), spread, NN)
        n = lax.broadcasted_iota(jnp.int32, (modes, width), 1) // vecs
        n = n + lax.axis_index("col") * z_length
        m = lax.broadcasted_iota(jnp.int32, (modes, width), 0)
        m = m + lax.axis_index("row") * modes
        wave_x = jnp.where(m <= x_count // 2, m, m - x_count // 2).astype(F32) * ALPHA_X
        wave_z = jnp.where(n <= z_count // 2, n, n - z_count // 2).astype(F32) * BETA_Z
        wave_s[...] = STEP_COEF + VISCOSITY * (wave_x * wave_x + wave_z * wave_z)
        decay_s[...] = jnp.broadcast_to(decay_ref[...], (LANES, planes)).T
        high_s[...] = jnp.zeros_like(high_s)
        cross_s[...] = jnp.zeros_like(cross_s)

    to_eigen = split(to_ref[...])
    from_eigen = split(from_ref[...])
    decay = jnp.concatenate([decay_s[...]] * tiles, axis=1)
    high, cross = high_s[...], cross_s[...]
    for k in range(step_modes):
        m = pl.program_id(0) * step_modes + k
        nonlinear = jnp.concatenate(
            [
                nl_ref[pl.ds(nb * modes + m, planes, stride=tiles * modes), :]
                for nb in range(tiles)
            ],
            axis=1,
        )
        right = STEP_COEF * q_ref[k] + nonlinear * mask_s[pl.ds(m, 1), :]
        eigen = dot3(to_eigen, split(right), NN)
        eigen = eigen / (wave_s[pl.ds(m, 1), :] + decay)
        stepped = dot3(from_eigen, split(eigen), NN)
        stepped_ref[pl.ds(pl.multiple_of(m * planes, planes), planes), :] = stepped
        stacked = [
            jnp.concatenate([x[:, nb * LANES : (nb + 1) * LANES] for nb in range(tiles)], axis=0)
            for x in split(stepped)
        ]
        high = high + dot(stacked[0], stacked[0], TN)
        cross = cross + dot(stacked[0], stacked[1], TN)
    high_s[...] = high
    cross_s[...] = cross

    @pl.when(pl.program_id(0) == pl.num_programs(0) - 1)
    def _():
        full = (high + (cross + cross.T)) * (1.0 / (x_count * planes * z_count))
        group = LANES // vecs
        lane = lax.broadcasted_iota(jnp.int32, (vecs, LANES), 1) // vecs
        folded = jnp.zeros((vecs, LANES), F32)
        for k in range(group):
            folded = folded + jnp.where(lane == k, full[k * vecs : (k + 1) * vecs], 0.0)
        folded = folded + pltpu.roll(folded, LANES // 2, 1)
        folded = folded + pltpu.roll(folded, LANES // 4, 1)
        piece = vecs // group
        lane = lax.broadcasted_iota(jnp.int32, (piece, LANES), 1) // vecs
        packed = jnp.zeros((piece, LANES), F32)
        for k in range(group):
            packed = jnp.where(lane == k, folded[k * piece : (k + 1) * piece], packed)
        gram_ref[...] = jnp.broadcast_to(packed[None], gram_ref.shape)


def finish_kernel(grams_ref, stepped_ref, vectors_ref, growth_ref, w_ref, *, devices, vecs, wide):
    group = LANES // vecs
    piece = vecs // group

    @pl.when(pl.program_id(0) == 0)
    def _():
        packed = jnp.sum(grams_ref[...].reshape(devices, piece, LANES), axis=0)
        gram = jnp.concatenate(
            [pltpu.roll(packed, (LANES - k * vecs) % LANES, 1) for k in range(group)], axis=0
        )
        lane = lax.broadcasted_iota(jnp.int32, (vecs, LANES), 1)
        row = lax.broadcasted_iota(jnp.int32, (vecs, LANES), 0)
        work = jnp.where(lane < vecs, gram, jnp.where(lane == row + vecs, 1.0, 0.0))
        for k in range(vecs - 1):
            pivot_row = work[k : k + 1, :]
            scaled = pivot_row / work[k : k + 1, k : k + 1]
            column = jnp.broadcast_to(work[:, k : k + 1], (vecs, LANES))
            work = work - jnp.where(row > k, column * scaled, 0.0)
        pivots = jnp.sum(jnp.where(lane == row, work, 0.0), axis=1, keepdims=True)
        diagonal = jnp.sqrt(pivots)
        inverse = work / diagonal
        across = jnp.sum(jnp.where(lane == row, diagonal, 0.0), axis=0, keepdims=True)
        growth_ref[...] = jnp.log(across[:, :vecs])
        inverse = jnp.where((lane >= vecs) & (lane < 2 * vecs), inverse, 0.0)
        inverse = inverse + pltpu.roll(inverse, LANES // 2, 1)
        inverse = inverse + pltpu.roll(inverse, LANES // 4, 1)
        repeats = wide // vecs
        tall = jnp.concatenate([inverse] * repeats, axis=0)
        tall = jnp.concatenate([tall] * (wide // LANES), axis=1)
        rows = lax.broadcasted_iota(jnp.int32, (wide, wide), 0) // vecs
        cols = lax.broadcasted_iota(jnp.int32, (wide, wide), 1) // vecs
        w_high, w_low = split(jnp.where(rows == cols, tall, 0.0))
        w_ref[0] = w_high
        w_ref[1] = w_low

    w = (w_ref[0], w_ref[1])
    block = vectors_ref.shape[0]
    rows = pl.ds(pl.multiple_of(pl.program_id(0) * block, block), block)
    for k in range(vectors_ref.shape[1] // wide):
        at = slice(k * wide, (k + 1) * wide)
        vectors_ref[:, at] = dot3(split(stepped_ref[rows, at]), w, NT)


def vmem():
    return pl.BlockSpec(memory_space=pltpu.VMEM)


def cost(flops, moved):
    return pl.CostEstimate(flops=int(flops), bytes_accessed=int(moved), transcendentals=0)


def body(tangents, base_flow, mode_mask, decay_rates, to_eigen, from_eigen):
    modes, planes, width = tangents.shape
    z_length = base_flow.shape[2]
    vecs = width // z_length
    row_devices, col_devices = lax.axis_size("row"), lax.axis_size("col")
    devices = row_devices * col_devices
    x_count, z_count = modes * row_devices, z_length * col_devices
    tiles = width // LANES
    rows = modes * tiles
    extra = -(-modes * z_length // LANES)
    size = tangents.size * 4
    both = ("row", "col")
    big = pltpu.CompilerParams(vmem_limit_bytes=40 * 2**20)
    small = pltpu.CompilerParams(vmem_limit_bytes=24 * 2**20)

    order = np.arange(x_count)
    order = (order % row_devices) * modes + order // row_devices
    halves = -(-x_count // LANES)
    fill = ((0, 0), (0, halves * LANES - x_count))
    sx = halves_of_table(np.pad(synthesis(x_count)[:, order].T, fill))
    sz = halves_of_table(synthesis(z_count))
    az = halves_of_table(analysis(z_count))
    gx = halves_of_table(np.pad(derivative_analysis(x_count, ALPHA_X)[order], fill))

    steps = 4
    base = jnp.transpose(base_flow, (0, 2, 1)).reshape(modes * z_length, planes)
    packed = pl.pallas_call(
        functools.partial(
            pack_kernel, modes=modes, planes=planes, tiles=tiles, extra=extra,
            step_modes=modes // steps,
        ),
        out_shape=jax.ShapeDtypeStruct((planes * (rows + extra), LANES), F32),
        grid=(steps,),
        in_specs=[
            pl.BlockSpec((modes // steps, planes, width), lambda i: (i, 0, 0)),
            pl.BlockSpec(base.shape, lambda i: (0, 0)),
        ],
        out_specs=vmem(),
        cost_estimate=cost(10**9, 2 * size),
        compiler_params=small,
        name="pack",
    )(tangents, base)
    received = lax.all_to_all(
        packed.reshape(devices, rows + extra, 1, LANES), both, 0, 0, tiled=True
    ).reshape(packed.shape)

    returned = pl.pallas_call(
        functools.partial(
            transform_kernel, modes=modes, row_devices=row_devices,
            col_devices=col_devices, tiles=tiles, extra=extra, vecs=vecs,
        ),
        out_shape=jax.ShapeDtypeStruct((devices * rows, LANES), F32),
        in_specs=[vmem()] * 5,
        out_specs=vmem(),
        scratch_shapes=[pltpu.VMEM((z_count, halves * LANES), F32)]
        + [pltpu.VMEM((z_count * vecs, LANES), F32)] * (2 * halves),
        cost_estimate=cost(2 * 10**10, 2 * size),
        compiler_params=big,
        name="transform",
    )(received, sx, sz, az, gx)
    nonlinear = lax.all_to_all(
        returned.reshape(devices, rows, LANES), both, 0, 0, tiled=True
    ).reshape(returned.shape)

    piece = vecs * vecs // LANES
    height = modes * planes
    stepped, grams = pl.pallas_call(
        functools.partial(
            column_kernel, modes=modes, planes=planes, tiles=tiles, vecs=vecs,
            step_modes=modes // steps, x_count=x_count, z_count=z_count, z_length=z_length,
        ),
        out_shape=[
            jax.ShapeDtypeStruct((height, width), F32),
            jax.ShapeDtypeStruct((devices, piece, LANES), F32),
        ],
        grid=(steps,),
        in_specs=[
            vmem(),
            pl.BlockSpec((modes // steps, planes, width), lambda i: (i, 0, 0)),
        ]
        + [vmem()] * 4,
        out_specs=[vmem()] * 2,
        scratch_shapes=[
            pltpu.VMEM((modes, width), F32),
            pltpu.VMEM((modes, width), F32),
            pltpu.VMEM((planes, LANES), F32),
            pltpu.VMEM((LANES, LANES), F32),
            pltpu.VMEM((LANES, LANES), F32),
        ],
        cost_estimate=cost(10**10, 3 * size),
        compiler_params=big,
        name="column",
    )(nonlinear, tangents, mode_mask, decay_rates[None, :], to_eigen, from_eigen)
    grams = lax.all_to_all(grams, both, 0, 0, tiled=True).reshape(devices * piece, LANES)

    block = height // 6
    vectors, growth = pl.pallas_call(
        functools.partial(finish_kernel, devices=devices, vecs=vecs, wide=2 * LANES),
        out_shape=[
            jax.ShapeDtypeStruct((height, width), F32),
            jax.ShapeDtypeStruct((1, vecs), F32),
        ],
        grid=(height // block,),
        in_specs=[vmem()] * 2,
        out_specs=[
            pl.BlockSpec((block, width), lambda i: (i, 0)),
            pl.BlockSpec((1, vecs), lambda i: (0, 0)),
        ],
        scratch_shapes=[pltpu.VMEM((2, 2 * LANES, 2 * LANES), BF16)],
        cost_estimate=cost(2 * height * width * 256, 2 * size),
        compiler_params=small,
        name="finish",
    )(grams, stepped)
    return vectors.reshape(tangents.shape), growth[0]


def solution(mesh):
    placed = (P("row", None, "col"), P("row", None, "col"), P("row", "col"), P(), P(), P())
    return jax.shard_map(
        body, mesh=mesh, in_specs=placed, out_specs=(P("row", None, "col"), P()), check_vma=False
    )
```

```python
import functools

import jax
import jax.numpy as jnp
import numpy as np
from jax import lax
from jax.experimental import pallas as pl
from jax.experimental.pallas import tpu as pltpu
from jax.sharding import PartitionSpec as P

STEP_COEF = 10.0
VISCOSITY = 0.01
ALPHA_X = 0.5
BETA_Z = 1.0
LANES = 128
F32 = jnp.float32
BF16 = jnp.bfloat16
NN = (((1,), (0,)), ((), ()))
NT = (((1,), (1,)), ((), ()))
TN = (((0,), (0,)), ((), ()))


def synthesis(count):
    points = np.arange(count)[:, None]
    modes = np.arange(count)[None, :]
    middle = count // 2
    waves = np.where(modes <= middle, modes, modes - middle)
    angles = (points * waves % count) * (2.0 * np.pi / count)
    return np.where(modes <= middle, np.cos(angles), np.sin(angles))


def analysis(count):
    modes = np.arange(count)
    weights = np.where((modes == 0) | (modes == count // 2), 1.0 / count, 2.0 / count)
    return weights[:, None] * synthesis(count).T


def derivative_analysis(count, scale):
    middle = count // 2
    derivative = np.zeros((count, count))
    for k in range(1, middle):
        derivative[k, middle + k] = k
        derivative[middle + k, k] = -k
    return -scale * (derivative @ analysis(count))


def halves_of_table(table):
    table = np.asarray(table, np.float64)
    high = table.astype(np.float32).astype(jnp.bfloat16)
    low = (table - high.astype(np.float64)).astype(np.float32).astype(jnp.bfloat16)
    return np.stack([high, low])


def split(x):
    high = x.astype(BF16)
    return high, (x - high.astype(F32)).astype(BF16)


def dot(a, b, dims):
    return lax.dot_general(a, b, dims, preferred_element_type=F32)


def dot3(a, b, dims):
    return dot(a[0], b[0], dims) + (dot(a[0], b[1], dims) + dot(a[1], b[0], dims))


def stacked_dot(table, x):
    high, low = split(x)
    return dot(table, jnp.concatenate([high, high], axis=0), NN) + dot(
        table[:, : x.shape[0]], low, NN
    )


def table_dot(table_ref, x):
    high, low = split(x)
    return dot(table_ref[...], jnp.concatenate([high, high, low], axis=0), NN)


def pack_kernel(q_ref, base_ref, out_ref, *, modes, planes, tiles, extra, step_modes):
    stride = modes * tiles + extra

    @pl.when(pl.program_id(0) == 0)
    def _():
        part = base_ref.shape[0] // extra
        fill = jnp.zeros((LANES - part, planes), F32)
        for k in range(extra):
            block = jnp.concatenate([base_ref[k * part : (k + 1) * part, :], fill], axis=0)
            out_ref[pl.ds(modes * tiles + k, planes, stride=stride), :] = block.T

    for k in range(step_modes):
        m = pl.program_id(0) * step_modes + k
        for nb in range(tiles):
            out_ref[pl.ds(nb * modes + m, planes, stride=stride), :] = q_ref[
                k, :, nb * LANES : (nb + 1) * LANES
            ]


def transform_kernel(
    d_ref, sx_ref, sz_ref, az_ref, g_ref, out_ref, speed_ref, *scratch,
    modes, row_devices, col_devices, tiles, extra, vecs,
):
    halves = len(scratch) // 2
    y_refs, z_refs = scratch[:halves], scratch[halves:]
    rows = modes * tiles
    stride = rows + extra
    x_count = modes * row_devices
    z_count = sz_ref.shape[0]
    z_length = z_count // col_devices
    pitch = y_refs[0].shape[0] // vecs
    per_tile = LANES // vecs

    turned = []
    for k in range(extra):
        block = d_ref[pl.ds(rows + k, row_devices * col_devices, stride=stride), :]
        turned.append(block.T)
    slot = lax.broadcasted_iota(jnp.int32, (z_length, LANES), 1) // row_devices
    slots = LANES // row_devices
    share = modes // extra
    sheets = []
    for c in range(col_devices):
        parts = [jnp.zeros((z_length, LANES), F32) for _ in range(halves)]
        for m in range(modes):
            piece = turned[m // share][(m % share) * z_length : (m % share + 1) * z_length]
            shift = ((m % slots - c) * row_devices) % LANES
            piece = pltpu.roll(piece, shift, 1) if shift else piece
            parts[m // slots] = jnp.where(slot == m % slots, piece, parts[m // slots])
        sheets.append(jnp.concatenate(parts, axis=1))
    base = jnp.concatenate(sheets, axis=0)[:, :x_count]
    sx = (sx_ref[:x_count], sx_ref[2 * x_count :])
    speed_ref[...] = table_dot(sz_ref, dot3(split(base), sx, NN))

    def forward_x(c, carry):
        parts = []
        for nb in range(tiles):
            start = c * (row_devices * stride) + nb * modes
            block = jnp.concatenate(
                [d_ref[pl.ds(start + m, row_devices, stride=stride), :] for m in range(modes)],
                axis=0,
            )
            block = jnp.concatenate(split(block), axis=0).T
            parts.append(jnp.concatenate([block, block[:, :x_count]], axis=1))
        mixed = dot(jnp.concatenate(parts, axis=0), sx_ref[...], NN)
        for n in range(z_length):
            for k, y_ref in enumerate(y_refs):
                y_ref[pl.ds(c * z_length + n, vecs, stride=pitch), :] = mixed[
                    n * vecs : (n + 1) * vecs, k * LANES : (k + 1) * LANES
                ]
        return carry

    lax.fori_loop(0, col_devices, forward_x, 0, unroll=4)

    def plane(i, carry):
        for j in range(4):
            at = pl.ds(pl.multiple_of((i * 4 + j) * pitch, 8), z_count)
            mixed = jnp.concatenate([y_ref[at, :] for y_ref in y_refs], axis=1)
            product = table_dot(sz_ref, mixed) * speed_ref[...]
            mixed = table_dot(az_ref, product)
            for k, z_ref in enumerate(z_refs):
                z_ref[at, :] = mixed[:, k * LANES : (k + 1) * LANES]
        return carry

    lax.fori_loop(0, vecs // 4, plane, 0, unroll=2)

    batch = 3

    def inverse_x(i, carry):
        c, group = i // (tiles // batch), i % (tiles // batch)
        first = c * z_length + group * (batch * per_tile)
        block = jnp.concatenate(
            [
                jnp.concatenate(
                    [z_ref[pl.ds(first + n, vecs, stride=pitch), :] for z_ref in z_refs], axis=1
                )
                for n in range(batch * per_tile)
            ],
            axis=0,
        )
        high, low = split(block)
        back = dot(g_ref[...], jnp.concatenate([high, high, low], axis=1), NT)
        for nb in range(batch):
            start = c * (row_devices * rows) + (group * batch + nb) * modes
            for m in range(modes):
                out_ref[pl.ds(start + m, row_devices, stride=rows), :] = back[
                    m * row_devices : (m + 1) * row_devices, nb * LANES : (nb + 1) * LANES
                ]
        return carry

    lax.fori_loop(0, col_devices * tiles // batch, inverse_x, 0, unroll=4)


def column_kernel(
    nl_ref, q_ref, mask_ref, decay_ref, to_ref, from_ref, stepped_ref, gram_ref,
    mask_s, wave_s, decay_s, gram_s,
    *, modes, planes, tiles, vecs, step_modes, x_count, z_count, z_length,
):
    width = tiles * LANES

    @pl.when(pl.program_id(0) == 0)
    def _():
        lane = lax.broadcasted_iota(jnp.int32, (z_length, width), 1) // vecs
        row = lax.broadcasted_iota(jnp.int32, (z_length, width), 0)
        spread = jnp.where(lane == row, 1.0, 0.0).astype(BF16)
        mask_s[...] = dot(mask_ref[...].astype(F32).astype(BF16), spread, NN)
        n = lax.broadcasted_iota(jnp.int32, (modes, width), 1) // vecs
        n = n + lax.axis_index("col") * z_length
        m = lax.broadcasted_iota(jnp.int32, (modes, width), 0)
        m = m + lax.axis_index("row") * modes
        wave_x = jnp.where(m <= x_count // 2, m, m - x_count // 2).astype(F32) * ALPHA_X
        wave_z = jnp.where(n <= z_count // 2, n, n - z_count // 2).astype(F32) * BETA_Z
        wave_s[...] = STEP_COEF + VISCOSITY * (wave_x * wave_x + wave_z * wave_z)
        decay_s[...] = jnp.broadcast_to(decay_ref[...], (LANES, planes)).T
        gram_s[...] = jnp.zeros_like(gram_s)

    to_eigen = jnp.concatenate(split(to_ref[...]), axis=1)
    from_eigen = jnp.concatenate(split(from_ref[...]), axis=1)
    decay = jnp.concatenate([decay_s[...]] * tiles, axis=1)
    gram = gram_s[...]
    for k in range(step_modes):
        m = pl.program_id(0) * step_modes + k
        nonlinear = jnp.concatenate(
            [
                nl_ref[pl.ds(nb * modes + m, planes, stride=tiles * modes), :]
                for nb in range(tiles)
            ],
            axis=1,
        )
        right = STEP_COEF * q_ref[k] + nonlinear * mask_s[pl.ds(m, 1), :]
        eigen = stacked_dot(to_eigen, right)
        eigen = eigen / (wave_s[pl.ds(m, 1), :] + decay)
        stepped = stacked_dot(from_eigen, eigen)
        stepped_ref[pl.ds(pl.multiple_of(m * planes, planes), planes), :] = stepped
        columns = [stepped[:, nb * LANES : (nb + 1) * LANES] for nb in range(tiles)]
        left = jnp.concatenate([x.T.astype(BF16) for x in columns], axis=1)
        right = jnp.concatenate(
            [jnp.concatenate(split(x), axis=1) for x in columns], axis=0
        )
        gram = gram + dot(left, right, NN)
    gram_s[...] = gram

    @pl.when(pl.program_id(0) == pl.num_programs(0) - 1)
    def _():
        high, cross = gram[:, :LANES], gram[:, LANES:]
        full = (high + (cross + cross.T)) * (1.0 / (x_count * planes * z_count))
        group = LANES // vecs
        lane = lax.broadcasted_iota(jnp.int32, (vecs, LANES), 1) // vecs
        folded = jnp.zeros((vecs, LANES), F32)
        for k in range(group):
            folded = folded + jnp.where(lane == k, full[k * vecs : (k + 1) * vecs], 0.0)
        folded = folded + pltpu.roll(folded, LANES // 2, 1)
        folded = folded + pltpu.roll(folded, LANES // 4, 1)
        piece = vecs // group
        lane = lax.broadcasted_iota(jnp.int32, (piece, LANES), 1) // vecs
        packed = jnp.zeros((piece, LANES), F32)
        for k in range(group):
            packed = jnp.where(lane == k, folded[k * piece : (k + 1) * piece], packed)
        gram_ref[...] = jnp.broadcast_to(packed[None], gram_ref.shape)


def finish_kernel(grams_ref, stepped_ref, vectors_ref, growth_ref, w_ref, *, devices, vecs, wide):
    group = LANES // vecs
    piece = vecs // group

    @pl.when(pl.program_id(0) == 0)
    def _():
        packed = jnp.sum(grams_ref[...].reshape(devices, piece, LANES), axis=0)
        gram = jnp.concatenate(
            [pltpu.roll(packed, (LANES - k * vecs) % LANES, 1) for k in range(group)], axis=0
        )
        lane = lax.broadcasted_iota(jnp.int32, (vecs, LANES), 1)
        row = lax.broadcasted_iota(jnp.int32, (vecs, LANES), 0)
        work = jnp.where(lane < vecs, gram, jnp.where(lane == row + vecs, 1.0, 0.0))
        for k in range(vecs - 1):
            pivot_row = work[k : k + 1, :]
            scaled = pivot_row / work[k : k + 1, k : k + 1]
            column = jnp.broadcast_to(work[:, k : k + 1], (vecs, LANES))
            work = work - jnp.where(row > k, column * scaled, 0.0)
        pivots = jnp.sum(jnp.where(lane == row, work, 0.0), axis=1, keepdims=True)
        diagonal = jnp.sqrt(pivots)
        inverse = work / diagonal
        across = jnp.sum(jnp.where(lane == row, diagonal, 0.0), axis=0, keepdims=True)
        growth_ref[...] = jnp.log(across[:, :vecs])
        inverse = jnp.where((lane >= vecs) & (lane < 2 * vecs), inverse, 0.0)
        inverse = inverse + pltpu.roll(inverse, LANES // 2, 1)
        inverse = inverse + pltpu.roll(inverse, LANES // 4, 1)
        repeats = wide // vecs
        tall = jnp.concatenate([inverse] * repeats, axis=0)
        tall = jnp.concatenate([tall] * (wide // LANES), axis=1)
        rows = lax.broadcasted_iota(jnp.int32, (wide, wide), 0) // vecs
        cols = lax.broadcasted_iota(jnp.int32, (wide, wide), 1) // vecs
        w_high, w_low = split(jnp.where(rows == cols, tall, 0.0))
        w_ref[0] = w_high
        w_ref[1] = w_low

    w = (w_ref[0], w_ref[1])
    block = vectors_ref.shape[0]
    rows = pl.ds(pl.multiple_of(pl.program_id(0) * block, block), block)
    for k in range(vectors_ref.shape[1] // wide):
        at = slice(k * wide, (k + 1) * wide)
        vectors_ref[:, at] = dot3(split(stepped_ref[rows, at]), w, NT)


def vmem():
    return pl.BlockSpec(memory_space=pltpu.VMEM)


def cost(flops, moved):
    return pl.CostEstimate(flops=int(flops), bytes_accessed=int(moved), transcendentals=0)


def body(tangents, base_flow, mode_mask, decay_rates, to_eigen, from_eigen):
    modes, planes, width = tangents.shape
    z_length = base_flow.shape[2]
    vecs = width // z_length
    row_devices, col_devices = lax.axis_size("row"), lax.axis_size("col")
    devices = row_devices * col_devices
    x_count, z_count = modes * row_devices, z_length * col_devices
    tiles = width // LANES
    rows = modes * tiles
    extra = -(-modes * z_length // LANES)
    size = tangents.size * 4
    both = ("col", "row")
    pitch = 8 * (z_count // 8 + 1 - z_count // 8 % 2)
    big = pltpu.CompilerParams(vmem_limit_bytes=40 * 2**20)
    small = pltpu.CompilerParams(vmem_limit_bytes=24 * 2**20)

    order = np.arange(x_count)
    order = (order % row_devices) * modes + order // row_devices
    halves = -(-x_count // LANES)
    fill = ((0, 0), (0, halves * LANES - x_count))
    sx_high, sx_low = halves_of_table(np.pad(synthesis(x_count)[:, order].T, fill))
    sx = np.concatenate([sx_high, sx_high, sx_low], axis=0)
    sz, az, gx = (
        np.concatenate([high, low, high], axis=1)
        for high, low in map(
            halves_of_table,
            (
                synthesis(z_count),
                analysis(z_count),
                np.pad(derivative_analysis(x_count, ALPHA_X)[order], fill),
            ),
        )
    )

    steps = 4
    base = jnp.transpose(base_flow, (0, 2, 1)).reshape(modes * z_length, planes)
    packed = pl.pallas_call(
        functools.partial(
            pack_kernel, modes=modes, planes=planes, tiles=tiles, extra=extra,
            step_modes=modes // steps,
        ),
        out_shape=jax.ShapeDtypeStruct((planes * (rows + extra), LANES), F32),
        grid=(steps,),
        in_specs=[
            pl.BlockSpec((modes // steps, planes, width), lambda i: (i, 0, 0)),
            pl.BlockSpec(base.shape, lambda i: (0, 0)),
        ],
        out_specs=vmem(),
        cost_estimate=cost(10**9, 2 * size),
        compiler_params=small,
        name="pack",
    )(tangents, base)
    received = lax.all_to_all(
        packed.reshape(devices, rows + extra, 1, LANES), both, 0, 0, tiled=True
    ).reshape(packed.shape)

    returned = pl.pallas_call(
        functools.partial(
            transform_kernel, modes=modes, row_devices=row_devices,
            col_devices=col_devices, tiles=tiles, extra=extra, vecs=vecs,
        ),
        out_shape=jax.ShapeDtypeStruct((devices * rows, LANES), F32),
        in_specs=[vmem()] * 5,
        out_specs=vmem(),
        scratch_shapes=[pltpu.VMEM((z_count, halves * LANES), F32)]
        + [pltpu.VMEM((pitch * vecs, LANES), F32)] * (2 * halves),
        cost_estimate=cost(2 * 10**10, 2 * size),
        compiler_params=big,
        name="transform",
    )(received, sx, sz, az, gx)
    nonlinear = lax.all_to_all(
        returned.reshape(devices, rows, LANES), both, 0, 0, tiled=True
    ).reshape(returned.shape)

    piece = vecs * vecs // LANES
    height = modes * planes
    stepped, grams = pl.pallas_call(
        functools.partial(
            column_kernel, modes=modes, planes=planes, tiles=tiles, vecs=vecs,
            step_modes=modes // 2, x_count=x_count, z_count=z_count, z_length=z_length,
        ),
        out_shape=[
            jax.ShapeDtypeStruct((height, width), F32),
            jax.ShapeDtypeStruct((devices, piece, LANES), F32),
        ],
        grid=(2,),
        in_specs=[
            vmem(),
            pl.BlockSpec((modes // 2, planes, width), lambda i: (i, 0, 0)),
        ]
        + [vmem()] * 4,
        out_specs=[vmem()] * 2,
        scratch_shapes=[
            pltpu.VMEM((modes, width), F32),
            pltpu.VMEM((modes, width), F32),
            pltpu.VMEM((planes, LANES), F32),
            pltpu.VMEM((LANES, 2 * LANES), F32),
        ],
        cost_estimate=cost(10**10, 3 * size),
        compiler_params=big,
        name="column",
    )(nonlinear, tangents, mode_mask, decay_rates[None, :], to_eigen, from_eigen)
    grams = lax.all_to_all(grams, both, 0, 0, tiled=True).reshape(devices * piece, LANES)

    block = height // 3
    vectors, growth = pl.pallas_call(
        functools.partial(finish_kernel, devices=devices, vecs=vecs, wide=2 * LANES),
        out_shape=[
            jax.ShapeDtypeStruct((height, width), F32),
            jax.ShapeDtypeStruct((1, vecs), F32),
        ],
        grid=(height // block,),
        in_specs=[vmem()] * 2,
        out_specs=[
            pl.BlockSpec((block, width), lambda i: (i, 0)),
            pl.BlockSpec((1, vecs), lambda i: (0, 0)),
        ],
        scratch_shapes=[pltpu.VMEM((2, 2 * LANES, 2 * LANES), BF16)],
        cost_estimate=cost(2 * height * width * 256, 2 * size),
        compiler_params=small,
        name="finish",
    )(grams, stepped)
    return vectors.reshape(tangents.shape), growth[0]


def solution(mesh):
    placed = (P("row", None, "col"), P("row", None, "col"), P("row", "col"), P(), P(), P())
    return jax.shard_map(
        body, mesh=mesh, in_specs=placed, out_specs=(P("row", None, "col"), P()), check_vma=False
    )
```

```python
import functools

import jax
import jax.numpy as jnp
import numpy as np
from jax import lax
from jax.experimental import pallas as pl
from jax.experimental.pallas import tpu as pltpu
from jax.sharding import PartitionSpec as P

STEP_COEF = 10.0
VISCOSITY = 0.01
ALPHA_X = 0.5
BETA_Z = 1.0
LANES = 128
F32 = jnp.float32
BF16 = jnp.bfloat16
NN = (((1,), (0,)), ((), ()))
NT = (((1,), (1,)), ((), ()))
TN = (((0,), (0,)), ((), ()))


def synthesis(count):
    points = np.arange(count)[:, None]
    modes = np.arange(count)[None, :]
    middle = count // 2
    waves = np.where(modes <= middle, modes, modes - middle)
    angles = (points * waves % count) * (2.0 * np.pi / count)
    return np.where(modes <= middle, np.cos(angles), np.sin(angles))


def analysis(count):
    modes = np.arange(count)
    weights = np.where((modes == 0) | (modes == count // 2), 1.0 / count, 2.0 / count)
    return weights[:, None] * synthesis(count).T


def derivative_analysis(count, scale):
    middle = count // 2
    derivative = np.zeros((count, count))
    for k in range(1, middle):
        derivative[k, middle + k] = k
        derivative[middle + k, k] = -k
    return -scale * (derivative @ analysis(count))


def halves_of_table(table):
    table = np.asarray(table, np.float64)
    high = table.astype(np.float32).astype(jnp.bfloat16)
    low = (table - high.astype(np.float64)).astype(np.float32).astype(jnp.bfloat16)
    return np.stack([high, low])


def split(x):
    high = x.astype(BF16)
    return high, (x - high.astype(F32)).astype(BF16)


def dot(a, b, dims):
    return lax.dot_general(a, b, dims, preferred_element_type=F32)


def dot3(a, b, dims):
    return dot(a[0], b[0], dims) + (dot(a[0], b[1], dims) + dot(a[1], b[0], dims))


def stacked_dot(table, x):
    high, low = split(x)
    return dot(table, jnp.concatenate([high, high], axis=0), NN) + dot(
        table[:, : x.shape[0]], low, NN
    )


def table_dot(table_ref, x):
    high, low = split(x)
    return dot(table_ref[...], jnp.concatenate([high, high, low], axis=0), NN)


def pack_kernel(q_ref, base_ref, out_ref, q_s, base_s, sems, *, modes, planes, tiles, extra):
    stride = modes * tiles + extra
    copies = [pltpu.make_async_copy(q_ref.at[m], q_s.at[m], sems.at[m]) for m in range(modes)]
    base_copy = pltpu.make_async_copy(base_ref, base_s, sems.at[modes])
    base_copy.start()
    for copy in copies:
        copy.start()
    base_copy.wait()
    part = base_s.shape[0] // extra
    fill = jnp.zeros((LANES - part, planes), F32)
    for k in range(extra):
        block = jnp.concatenate([base_s[k * part : (k + 1) * part, :], fill], axis=0)
        out_ref[pl.ds(modes * tiles + k, planes, stride=stride), :] = block.T
    for m, copy in enumerate(copies):
        copy.wait()
        for nb in range(tiles):
            out_ref[pl.ds(nb * modes + m, planes, stride=stride), :] = q_s[
                m, :, nb * LANES : (nb + 1) * LANES
            ]


def transform_kernel(
    d_ref, sx_ref, sz_ref, az_ref, g_ref, out_ref, speed_ref, *scratch,
    modes, row_devices, col_devices, tiles, extra, vecs,
):
    halves = len(scratch) // 2
    y_refs, z_refs = scratch[:halves], scratch[halves:]
    rows = modes * tiles
    stride = rows + extra
    x_count = modes * row_devices
    z_count = sz_ref.shape[0]
    z_length = z_count // col_devices
    pitch = y_refs[0].shape[0] // vecs
    per_tile = LANES // vecs

    turned = []
    for k in range(extra):
        block = d_ref[pl.ds(rows + k, row_devices * col_devices, stride=stride), :]
        turned.append(block.T)
    slot = lax.broadcasted_iota(jnp.int32, (z_length, LANES), 1) // row_devices
    slots = LANES // row_devices
    share = modes // extra
    sheets = []
    for c in range(col_devices):
        parts = [jnp.zeros((z_length, LANES), F32) for _ in range(halves)]
        for m in range(modes):
            piece = turned[m // share][(m % share) * z_length : (m % share + 1) * z_length]
            shift = ((m % slots - c) * row_devices) % LANES
            piece = pltpu.roll(piece, shift, 1) if shift else piece
            parts[m // slots] = jnp.where(slot == m % slots, piece, parts[m // slots])
        sheets.append(jnp.concatenate(parts, axis=1))
    base = jnp.concatenate(sheets, axis=0)[:, :x_count]
    sx = (sx_ref[:x_count], sx_ref[2 * x_count :])
    speed_ref[...] = table_dot(sz_ref, dot3(split(base), sx, NN))

    def forward_x(c, carry):
        parts = []
        for nb in range(tiles):
            start = c * (row_devices * stride) + nb * modes
            block = jnp.concatenate(
                [d_ref[pl.ds(start + m, row_devices, stride=stride), :] for m in range(modes)],
                axis=0,
            )
            block = jnp.concatenate(split(block), axis=0).T
            parts.append(jnp.concatenate([block, block[:, :x_count]], axis=1))
        mixed = dot(jnp.concatenate(parts, axis=0), sx_ref[...], NN)
        for n in range(z_length):
            for k, y_ref in enumerate(y_refs):
                y_ref[pl.ds(c * z_length + n, vecs, stride=pitch), :] = mixed[
                    n * vecs : (n + 1) * vecs, k * LANES : (k + 1) * LANES
                ]
        return carry

    lax.fori_loop(0, col_devices, forward_x, 0, unroll=8)

    y_low, y_high = y_refs
    z_low, z_high = z_refs
    first = lax.broadcasted_iota(jnp.int32, (z_count, LANES), 1) < LANES // 2
    batch = 8

    def plane(i, carry):
        ats = [
            pl.ds(pl.multiple_of((i * batch + j) * pitch, 8), z_count) for j in range(batch)
        ]
        mixed = jnp.concatenate(
            [y_low[at, :] for at in ats]
            + [
                jnp.where(first, y_high[ats[j], :], y_high[ats[j + 1], :])
                for j in range(0, batch, 2)
            ],
            axis=1,
        )
        speed = jnp.concatenate(
            [speed_ref[:, :LANES]] * batch + [speed_ref[:, LANES:]] * (batch // 2), axis=1
        )
        mixed = table_dot(az_ref, table_dot(sz_ref, mixed) * speed)
        for j, at in enumerate(ats):
            k = batch + j // 2
            z_low[at, :] = mixed[:, j * LANES : (j + 1) * LANES]
            z_high[at, :] = mixed[:, k * LANES : (k + 1) * LANES]
        return carry

    lax.fori_loop(0, vecs // batch, plane, 0, unroll=2)

    rows_of = lax.broadcasted_iota(jnp.int32, (vecs, LANES), 0)
    lanes_of = lax.broadcasted_iota(jnp.int32, (vecs, LANES), 1)
    mine = (rows_of % 2) == (lanes_of // (LANES // 2))

    def inverse_x(c, carry):
        block = jnp.concatenate(
            [
                jnp.concatenate(
                    [
                        z_low[pl.ds(c * z_length + n, vecs, stride=pitch), :],
                        jnp.where(
                            mine, z_high[pl.ds(c * z_length + n, vecs, stride=pitch), :], 0.0
                        ),
                    ],
                    axis=1,
                )
                for n in range(z_length)
            ],
            axis=0,
        )
        high, low = split(block)
        both = dot(g_ref[...], high, NT)
        back = both[:x_count] + (both[x_count:] + dot(g_ref[:x_count], low, NT))
        for nb in range(tiles):
            start = c * (row_devices * rows) + nb * modes
            for m in range(modes):
                out_ref[pl.ds(start + m, row_devices, stride=rows), :] = back[
                    m * row_devices : (m + 1) * row_devices, nb * LANES : (nb + 1) * LANES
                ]
        return carry

    lax.fori_loop(0, col_devices, inverse_x, 0, unroll=8)


def column_kernel(
    nl_ref, q_ref, mask_ref, decay_ref, to_ref, from_ref, stepped_ref, gram_ref,
    mask_s, wave_s, decay_s, gram_s,
    *, modes, planes, tiles, vecs, step_modes, x_count, z_count, z_length,
):
    width = tiles * LANES

    @pl.when(pl.program_id(0) == 0)
    def _():
        lane = lax.broadcasted_iota(jnp.int32, (z_length, width), 1) // vecs
        row = lax.broadcasted_iota(jnp.int32, (z_length, width), 0)
        spread = jnp.where(lane == row, 1.0, 0.0).astype(BF16)
        mask_s[...] = dot(mask_ref[...].astype(F32).astype(BF16), spread, NN)
        n = lax.broadcasted_iota(jnp.int32, (modes, width), 1) // vecs
        n = n + lax.axis_index("col") * z_length
        m = lax.broadcasted_iota(jnp.int32, (modes, width), 0)
        m = m + lax.axis_index("row") * modes
        wave_x = jnp.where(m <= x_count // 2, m, m - x_count // 2).astype(F32) * ALPHA_X
        wave_z = jnp.where(n <= z_count // 2, n, n - z_count // 2).astype(F32) * BETA_Z
        wave_s[...] = STEP_COEF + VISCOSITY * (wave_x * wave_x + wave_z * wave_z)
        decay_s[...] = jnp.broadcast_to(decay_ref[...], (LANES, planes)).T
        gram_s[...] = jnp.zeros_like(gram_s)

    to_eigen = jnp.concatenate(split(to_ref[...]), axis=1)
    from_eigen = jnp.concatenate(split(from_ref[...]), axis=1)
    decay = jnp.concatenate([decay_s[...]] * tiles, axis=1)
    gram = gram_s[...]
    for k in range(step_modes):
        m = pl.program_id(0) * step_modes + k
        nonlinear = jnp.concatenate(
            [
                nl_ref[pl.ds(nb * modes + m, planes, stride=tiles * modes), :]
                for nb in range(tiles)
            ],
            axis=1,
        )
        right = STEP_COEF * q_ref[m] + nonlinear * mask_s[pl.ds(m, 1), :]
        eigen = stacked_dot(to_eigen, right)
        eigen = eigen / (wave_s[pl.ds(m, 1), :] + decay)
        stepped = stacked_dot(from_eigen, eigen)
        stepped_ref[pl.ds(pl.multiple_of(m * planes, planes), planes), :] = stepped
        columns = [stepped[:, nb * LANES : (nb + 1) * LANES] for nb in range(tiles)]
        left = jnp.concatenate([x.T.astype(BF16) for x in columns], axis=1)
        right = jnp.concatenate(
            [jnp.concatenate(split(x), axis=1) for x in columns], axis=0
        )
        gram = gram + dot(left, right, NN)
    gram_s[...] = gram

    @pl.when(pl.program_id(0) == pl.num_programs(0) - 1)
    def _():
        high, cross = gram[:, :LANES], gram[:, LANES:]
        full = (high + (cross + cross.T)) * (1.0 / (x_count * planes * z_count))
        group = LANES // vecs
        lane = lax.broadcasted_iota(jnp.int32, (vecs, LANES), 1) // vecs
        folded = jnp.zeros((vecs, LANES), F32)
        for k in range(group):
            folded = folded + jnp.where(lane == k, full[k * vecs : (k + 1) * vecs], 0.0)
        folded = folded + pltpu.roll(folded, LANES // 2, 1)
        folded = folded + pltpu.roll(folded, LANES // 4, 1)
        piece = vecs // group
        lane = lax.broadcasted_iota(jnp.int32, (piece, LANES), 1) // vecs
        packed = jnp.zeros((piece, LANES), F32)
        for k in range(group):
            packed = jnp.where(lane == k, folded[k * piece : (k + 1) * piece], packed)
        gram_ref[...] = jnp.broadcast_to(packed[None], gram_ref.shape)


def finish_kernel(grams_ref, stepped_ref, vectors_ref, growth_ref, w_ref, *, devices, vecs, panel):
    group = LANES // vecs
    piece = vecs // group

    @pl.when(pl.program_id(0) == 0)
    def _():
        packed = jnp.sum(grams_ref[...].reshape(devices, piece, LANES), axis=0)
        gram = jnp.concatenate(
            [pltpu.roll(packed, (LANES - k * vecs) % LANES, 1) for k in range(group)], axis=0
        )
        lane = lax.broadcasted_iota(jnp.int32, (vecs, LANES), 1)
        row = lax.broadcasted_iota(jnp.int32, (vecs, LANES), 0)
        work = jnp.where(lane < vecs, gram, jnp.where(lane == row + vecs, 1.0, 0.0))
        for first in range(0, vecs, panel):
            own = range(first, first + panel)
            columns = [jnp.broadcast_to(work[:, k : k + 1], (vecs, LANES)) for k in own]
            lines = [work[k : k + 1, :] for k in own]
            for j, k in enumerate(own):
                pivot = columns[j][k : k + 1]
                column = jnp.where(row > k, columns[j], 0.0)
                scaled = lines[j] / pivot
                for i in range(j + 1, panel):
                    columns[i] = columns[i] - column * (columns[i][k : k + 1] / pivot)
                    lines[i] = lines[i] - columns[j][first + i : first + i + 1] * scaled
                work = work - column * scaled
        pivots = jnp.sum(jnp.where(lane == row, work, 0.0), axis=1, keepdims=True)
        diagonal = jnp.sqrt(pivots)
        inverse = work / diagonal
        across = jnp.sum(jnp.where(lane == row, diagonal, 0.0), axis=0, keepdims=True)
        growth_ref[...] = jnp.log(across[:, :vecs])
        inverse = jnp.where((lane >= vecs) & (lane < 2 * vecs), inverse, 0.0)
        inverse = inverse + pltpu.roll(inverse, LANES // 2, 1)
        inverse = inverse + pltpu.roll(inverse, LANES // 4, 1)
        high, low = split(
            jnp.concatenate(
                [jnp.where(lane // vecs == k, inverse, 0.0) for k in range(group)], axis=0
            )
        )
        w_ref[...] = jnp.concatenate(
            [
                jnp.concatenate([high, high], axis=1),
                jnp.concatenate([low, jnp.zeros_like(low)], axis=1),
            ],
            axis=0,
        )

    block = vectors_ref.shape[0]
    rows = pl.ds(pl.multiple_of(pl.program_id(0) * block, block), block)
    for k in range(vectors_ref.shape[1] // LANES):
        at = slice(k * LANES, (k + 1) * LANES)
        both = dot(jnp.concatenate(split(stepped_ref[rows, at]), axis=1), w_ref[...], NT)
        vectors_ref[:, at] = both[:, :LANES] + both[:, LANES:]


def vmem():
    return pl.BlockSpec(memory_space=pltpu.VMEM)


def cost(flops, moved):
    return pl.CostEstimate(flops=int(flops), bytes_accessed=int(moved), transcendentals=0)


def body(tangents, base_flow, mode_mask, decay_rates, to_eigen, from_eigen):
    modes, planes, width = tangents.shape
    z_length = base_flow.shape[2]
    vecs = width // z_length
    row_devices, col_devices = lax.axis_size("row"), lax.axis_size("col")
    devices = row_devices * col_devices
    x_count, z_count = modes * row_devices, z_length * col_devices
    tiles = width // LANES
    rows = modes * tiles
    extra = -(-modes * z_length // LANES)
    size = tangents.size * 4
    both = ("col", "row")
    pitch = 8 * (z_count // 8 + 1 - z_count // 8 % 2)
    big = pltpu.CompilerParams(vmem_limit_bytes=40 * 2**20)
    small = pltpu.CompilerParams(vmem_limit_bytes=24 * 2**20)

    order = np.arange(x_count)
    order = (order % row_devices) * modes + order // row_devices
    halves = -(-x_count // LANES)
    points = np.arange(halves * LANES)
    points = np.where(points < x_count, points, points - (halves * LANES - x_count))
    sx_high, sx_low = halves_of_table(synthesis(x_count)[points][:, order].T)
    sx = np.concatenate([sx_high, sx_high, sx_low], axis=0)
    sz, az = (
        np.concatenate([high, low, high], axis=1)
        for high, low in map(halves_of_table, (synthesis(z_count), analysis(z_count)))
    )
    gx = np.concatenate(
        halves_of_table(derivative_analysis(x_count, ALPHA_X)[order][:, points]), axis=0
    )

    steps = 2
    base = jnp.transpose(base_flow, (0, 2, 1)).reshape(modes * z_length, planes)
    packed = pl.pallas_call(
        functools.partial(pack_kernel, modes=modes, planes=planes, tiles=tiles, extra=extra),
        out_shape=jax.ShapeDtypeStruct((planes * (rows + extra), LANES), F32),
        in_specs=[pl.BlockSpec(memory_space=pltpu.HBM)] * 2,
        out_specs=vmem(),
        scratch_shapes=[
            pltpu.VMEM(tangents.shape, F32),
            pltpu.VMEM(base.shape, F32),
            pltpu.SemaphoreType.DMA((modes + 1,)),
        ],
        cost_estimate=cost(10**9, 2 * size),
        compiler_params=pltpu.CompilerParams(vmem_limit_bytes=44 * 2**20),
        name="pack",
    )(tangents, base)
    received = lax.all_to_all(
        packed.reshape(devices, rows + extra, 1, LANES), both, 0, 0, tiled=True
    ).reshape(packed.shape)

    returned = pl.pallas_call(
        functools.partial(
            transform_kernel, modes=modes, row_devices=row_devices,
            col_devices=col_devices, tiles=tiles, extra=extra, vecs=vecs,
        ),
        out_shape=jax.ShapeDtypeStruct((devices * rows, LANES), F32),
        in_specs=[vmem()] * 5,
        out_specs=vmem(),
        scratch_shapes=[pltpu.VMEM((z_count, halves * LANES), F32)]
        + [pltpu.VMEM((pitch * vecs, LANES), F32)] * (2 * halves),
        cost_estimate=cost(2 * 10**10, 2 * size),
        compiler_params=big,
        name="transform",
    )(received, sx, sz, az, gx)
    nonlinear = lax.all_to_all(
        returned.reshape(devices, rows, LANES), both, 0, 0, tiled=True
    ).reshape(returned.shape)

    piece = vecs * vecs // LANES
    height = modes * planes
    stepped, grams = pl.pallas_call(
        functools.partial(
            column_kernel, modes=modes, planes=planes, tiles=tiles, vecs=vecs,
            step_modes=modes // steps, x_count=x_count, z_count=z_count, z_length=z_length,
        ),
        out_shape=[
            jax.ShapeDtypeStruct((height, width), F32),
            jax.ShapeDtypeStruct((devices, piece, LANES), F32),
        ],
        grid=(steps,),
        in_specs=[vmem()] * 6,
        out_specs=[vmem()] * 2,
        scratch_shapes=[
            pltpu.VMEM((modes, width), F32),
            pltpu.VMEM((modes, width), F32),
            pltpu.VMEM((planes, LANES), F32),
            pltpu.VMEM((LANES, 2 * LANES), F32),
        ],
        cost_estimate=cost(10**10, 3 * size),
        compiler_params=small,
        name="column",
    )(nonlinear, tangents, mode_mask, decay_rates[None, :], to_eigen, from_eigen)
    grams = lax.all_to_all(grams, both, 0, 0, tiled=True).reshape(devices * piece, LANES)

    block = height // 3
    vectors, growth = pl.pallas_call(
        functools.partial(finish_kernel, devices=devices, vecs=vecs, panel=8),
        out_shape=[
            jax.ShapeDtypeStruct((height, width), F32),
            jax.ShapeDtypeStruct((1, vecs), F32),
        ],
        grid=(height // block,),
        in_specs=[vmem()] * 2,
        out_specs=[
            pl.BlockSpec((block, width), lambda i: (i, 0)),
            pl.BlockSpec((1, vecs), lambda i: (0, 0)),
        ],
        scratch_shapes=[pltpu.VMEM((2 * LANES, 2 * LANES), BF16)],
        cost_estimate=cost(2 * height * width * 256, 2 * size),
        compiler_params=small,
        name="finish",
    )(grams, stepped)
    return vectors.reshape(tangents.shape), growth[0]


def solution(mesh):
    placed = (P("row", None, "col"), P("row", None, "col"), P("row", "col"), P(), P(), P())
    return jax.shard_map(
        body, mesh=mesh, in_specs=placed, out_specs=(P("row", None, "col"), P()), check_vma=False
    )
```

```python
import functools

import jax
import jax.numpy as jnp
import numpy as np
from jax import lax
from jax.experimental import pallas as pl
from jax.experimental.pallas import tpu as pltpu
from jax.sharding import PartitionSpec as P

STEP_COEF = 10.0
VISCOSITY = 0.01
ALPHA_X = 0.5
BETA_Z = 1.0
LANES = 128
F32 = jnp.float32
BF16 = jnp.bfloat16
NN = (((1,), (0,)), ((), ()))
NT = (((1,), (1,)), ((), ()))
TN = (((0,), (0,)), ((), ()))


def synthesis(count):
    points = np.arange(count)[:, None]
    modes = np.arange(count)[None, :]
    middle = count // 2
    waves = np.where(modes <= middle, modes, modes - middle)
    angles = (points * waves % count) * (2.0 * np.pi / count)
    return np.where(modes <= middle, np.cos(angles), np.sin(angles))


def analysis(count):
    modes = np.arange(count)
    weights = np.where((modes == 0) | (modes == count // 2), 1.0 / count, 2.0 / count)
    return weights[:, None] * synthesis(count).T


def derivative_analysis(count, scale):
    middle = count // 2
    derivative = np.zeros((count, count))
    for k in range(1, middle):
        derivative[k, middle + k] = k
        derivative[middle + k, k] = -k
    return -scale * (derivative @ analysis(count))


def halves_of_table(table):
    table = np.asarray(table, np.float64)
    high = table.astype(np.float32).astype(jnp.bfloat16)
    low = (table - high.astype(np.float64)).astype(np.float32).astype(jnp.bfloat16)
    return np.stack([high, low])


def split(x):
    high = x.astype(BF16)
    return high, (x - high.astype(F32)).astype(BF16)


def dot(a, b, dims):
    return lax.dot_general(a, b, dims, preferred_element_type=F32)


def dot3(a, b, dims):
    return dot(a[0], b[0], dims) + (dot(a[0], b[1], dims) + dot(a[1], b[0], dims))


def stacked_dot(table, x):
    high, low = split(x)
    return dot(table, jnp.concatenate([high, high], axis=0), NN) + dot(
        table[:, : x.shape[0]], low, NN
    )


def table_dot(table_ref, x):
    high, low = split(x)
    return dot(table_ref[...], jnp.concatenate([high, high, low], axis=0), NN)


def pack_kernel(q_ref, base_ref, out_ref, *, modes, planes, tiles, extra):
    stride = modes * tiles + extra
    part = base_ref.shape[0] // extra
    fill = jnp.zeros((LANES - part, planes), F32)
    for k in range(extra):
        block = jnp.concatenate([base_ref[k * part : (k + 1) * part, :], fill], axis=0)
        out_ref[pl.ds(modes * tiles + k, planes, stride=stride), :] = block.T
    for m in range(modes):
        for nb in range(tiles):
            out_ref[pl.ds(nb * modes + m, planes, stride=stride), :] = q_ref[
                m, :, nb * LANES : (nb + 1) * LANES
            ]


def transform_kernel(
    d_ref, sx_ref, sz_ref, az_ref, g_ref, out_ref, speed_ref, *scratch,
    modes, row_devices, col_devices, tiles, extra, vecs,
):
    halves = len(scratch) // 2
    y_refs, z_refs = scratch[:halves], scratch[halves:]
    rows = modes * tiles
    stride = rows + extra
    x_count = modes * row_devices
    z_count = sz_ref.shape[0]
    z_length = z_count // col_devices
    pitch = y_refs[0].shape[0] // vecs
    per_tile = LANES // vecs

    turned = []
    for k in range(extra):
        block = d_ref[pl.ds(rows + k, row_devices * col_devices, stride=stride), :]
        turned.append(block.T)
    slot = lax.broadcasted_iota(jnp.int32, (z_length, LANES), 1) // row_devices
    slots = LANES // row_devices
    share = modes // extra
    sheets = []
    for c in range(col_devices):
        parts = [jnp.zeros((z_length, LANES), F32) for _ in range(halves)]
        for m in range(modes):
            piece = turned[m // share][(m % share) * z_length : (m % share + 1) * z_length]
            shift = ((m % slots - c) * row_devices) % LANES
            piece = pltpu.roll(piece, shift, 1) if shift else piece
            parts[m // slots] = jnp.where(slot == m % slots, piece, parts[m // slots])
        sheets.append(jnp.concatenate(parts, axis=1))
    base = jnp.concatenate(sheets, axis=0)[:, :x_count]
    sx = (sx_ref[:x_count], sx_ref[2 * x_count :])
    speed_ref[...] = table_dot(sz_ref, dot3(split(base), sx, NN))

    def forward_x(c, carry):
        parts = []
        for nb in range(tiles):
            start = c * (row_devices * stride) + nb * modes
            block = jnp.concatenate(
                [d_ref[pl.ds(start + m, row_devices, stride=stride), :] for m in range(modes)],
                axis=0,
            )
            block = jnp.concatenate(split(block), axis=0).T
            parts.append(jnp.concatenate([block, block[:, :x_count]], axis=1))
        mixed = dot(jnp.concatenate(parts, axis=0), sx_ref[...], NN)
        for n in range(z_length):
            for k, y_ref in enumerate(y_refs):
                y_ref[pl.ds(c * z_length + n, vecs, stride=pitch), :] = mixed[
                    n * vecs : (n + 1) * vecs, k * LANES : (k + 1) * LANES
                ]
        return carry

    lax.fori_loop(0, col_devices, forward_x, 0, unroll=8)

    y_low, y_high = y_refs
    z_low, z_high = z_refs
    first = lax.broadcasted_iota(jnp.int32, (z_count, LANES), 1) < LANES // 2
    batch = 8

    def plane(i, carry):
        ats = [
            pl.ds(pl.multiple_of((i * batch + j) * pitch, 8), z_count) for j in range(batch)
        ]
        mixed = jnp.concatenate(
            [y_low[at, :] for at in ats]
            + [
                jnp.where(first, y_high[ats[j], :], y_high[ats[j + 1], :])
                for j in range(0, batch, 2)
            ],
            axis=1,
        )
        speed = jnp.concatenate(
            [speed_ref[:, :LANES]] * batch + [speed_ref[:, LANES:]] * (batch // 2), axis=1
        )
        mixed = table_dot(az_ref, table_dot(sz_ref, mixed) * speed)
        for j, at in enumerate(ats):
            k = batch + j // 2
            z_low[at, :] = mixed[:, j * LANES : (j + 1) * LANES]
            z_high[at, :] = mixed[:, k * LANES : (k + 1) * LANES]
        return carry

    lax.fori_loop(0, vecs // batch, plane, 0, unroll=2)

    rows_of = lax.broadcasted_iota(jnp.int32, (vecs, LANES), 0)
    lanes_of = lax.broadcasted_iota(jnp.int32, (vecs, LANES), 1)
    mine = (rows_of % 2) == (lanes_of // (LANES // 2))

    def inverse_x(c, carry):
        block = jnp.concatenate(
            [
                jnp.concatenate(
                    [
                        z_low[pl.ds(c * z_length + n, vecs, stride=pitch), :],
                        jnp.where(
                            mine, z_high[pl.ds(c * z_length + n, vecs, stride=pitch), :], 0.0
                        ),
                    ],
                    axis=1,
                )
                for n in range(z_length)
            ],
            axis=0,
        )
        high, low = split(block)
        both = dot(g_ref[...], high, NT)
        back = both[:x_count] + (both[x_count:] + dot(g_ref[:x_count], low, NT))
        for nb in range(tiles):
            start = c * (row_devices * rows) + nb * modes
            for m in range(modes):
                out_ref[pl.ds(start + m, row_devices, stride=rows), :] = back[
                    m * row_devices : (m + 1) * row_devices, nb * LANES : (nb + 1) * LANES
                ]
        return carry

    lax.fori_loop(0, col_devices, inverse_x, 0, unroll=8)


def column_kernel(
    nl_ref, q_ref, mask_ref, decay_ref, to_ref, from_ref, stepped_ref, gram_ref,
    mask_s, wave_s, decay_s, gram_s,
    *, modes, planes, tiles, vecs, step_modes, x_count, z_count, z_length,
):
    width = tiles * LANES

    @pl.when(pl.program_id(0) == 0)
    def _():
        lane = lax.broadcasted_iota(jnp.int32, (z_length, width), 1) // vecs
        row = lax.broadcasted_iota(jnp.int32, (z_length, width), 0)
        spread = jnp.where(lane == row, 1.0, 0.0).astype(BF16)
        mask_s[...] = dot(mask_ref[...].astype(F32).astype(BF16), spread, NN)
        n = lax.broadcasted_iota(jnp.int32, (modes, width), 1) // vecs
        n = n + lax.axis_index("col") * z_length
        m = lax.broadcasted_iota(jnp.int32, (modes, width), 0)
        m = m + lax.axis_index("row") * modes
        wave_x = jnp.where(m <= x_count // 2, m, m - x_count // 2).astype(F32) * ALPHA_X
        wave_z = jnp.where(n <= z_count // 2, n, n - z_count // 2).astype(F32) * BETA_Z
        wave_s[...] = STEP_COEF + VISCOSITY * (wave_x * wave_x + wave_z * wave_z)
        decay_s[...] = jnp.broadcast_to(decay_ref[...], (LANES, planes)).T
        gram_s[...] = jnp.zeros_like(gram_s)

    to_eigen = jnp.concatenate(split(to_ref[...]), axis=1)
    from_eigen = jnp.concatenate(split(from_ref[...]), axis=1)
    decay = jnp.concatenate([decay_s[...]] * tiles, axis=1)
    gram = gram_s[...]
    for k in range(step_modes):
        m = pl.program_id(0) * step_modes + k
        nonlinear = jnp.concatenate(
            [
                nl_ref[pl.ds(nb * modes + m, planes, stride=tiles * modes), :]
                for nb in range(tiles)
            ],
            axis=1,
        )
        right = STEP_COEF * q_ref[m] + nonlinear * mask_s[pl.ds(m, 1), :]
        eigen = stacked_dot(to_eigen, right)
        eigen = eigen / (wave_s[pl.ds(m, 1), :] + decay)
        stepped = stacked_dot(from_eigen, eigen)
        stepped_ref[pl.ds(pl.multiple_of(m * planes, planes), planes), :] = stepped
        columns = [stepped[:, nb * LANES : (nb + 1) * LANES] for nb in range(tiles)]
        left = jnp.concatenate([x.T.astype(BF16) for x in columns], axis=1)
        right = jnp.concatenate(
            [jnp.concatenate(split(x), axis=1) for x in columns], axis=0
        )
        gram = gram + dot(left, right, NN)
    gram_s[...] = gram

    @pl.when(pl.program_id(0) == pl.num_programs(0) - 1)
    def _():
        high, cross = gram[:, :LANES], gram[:, LANES:]
        full = (high + (cross + cross.T)) * (1.0 / (x_count * planes * z_count))
        group = LANES // vecs
        lane = lax.broadcasted_iota(jnp.int32, (vecs, LANES), 1) // vecs
        folded = jnp.zeros((vecs, LANES), F32)
        for k in range(group):
            folded = folded + jnp.where(lane == k, full[k * vecs : (k + 1) * vecs], 0.0)
        folded = folded + pltpu.roll(folded, LANES // 2, 1)
        folded = folded + pltpu.roll(folded, LANES // 4, 1)
        piece = vecs // group
        lane = lax.broadcasted_iota(jnp.int32, (piece, LANES), 1) // vecs
        packed = jnp.zeros((piece, LANES), F32)
        for k in range(group):
            packed = jnp.where(lane == k, folded[k * piece : (k + 1) * piece], packed)
        gram_ref[...] = jnp.broadcast_to(packed[None], gram_ref.shape)


def finish_kernel(grams_ref, stepped_ref, vectors_ref, growth_ref, w_ref, *, devices, vecs, panel):
    group = LANES // vecs
    piece = vecs // group

    @pl.when(pl.program_id(0) == 0)
    def _():
        packed = jnp.sum(grams_ref[...].reshape(devices, piece, LANES), axis=0)
        gram = jnp.concatenate(
            [pltpu.roll(packed, (LANES - k * vecs) % LANES, 1) for k in range(group)], axis=0
        )
        lane = lax.broadcasted_iota(jnp.int32, (vecs, LANES), 1)
        row = lax.broadcasted_iota(jnp.int32, (vecs, LANES), 0)
        work = jnp.where(lane < vecs, gram, jnp.where(lane == row + vecs, 1.0, 0.0))
        for first in range(0, vecs, panel):
            own = range(first, first + panel)
            columns = [jnp.broadcast_to(work[:, k : k + 1], (vecs, LANES)) for k in own]
            lines = [work[k : k + 1, :] for k in own]
            for j, k in enumerate(own):
                pivot = columns[j][k : k + 1]
                column = jnp.where(row > k, columns[j], 0.0)
                scaled = lines[j] / pivot
                for i in range(j + 1, panel):
                    columns[i] = columns[i] - column * (columns[i][k : k + 1] / pivot)
                    lines[i] = lines[i] - columns[j][first + i : first + i + 1] * scaled
                work = work - column * scaled
        pivots = jnp.sum(jnp.where(lane == row, work, 0.0), axis=1, keepdims=True)
        diagonal = jnp.sqrt(pivots)
        inverse = work / diagonal
        across = jnp.sum(jnp.where(lane == row, diagonal, 0.0), axis=0, keepdims=True)
        growth_ref[...] = jnp.log(across[:, :vecs])
        inverse = jnp.where((lane >= vecs) & (lane < 2 * vecs), inverse, 0.0)
        inverse = inverse + pltpu.roll(inverse, LANES // 2, 1)
        inverse = inverse + pltpu.roll(inverse, LANES // 4, 1)
        high, low = split(
            jnp.concatenate(
                [jnp.where(lane // vecs == k, inverse, 0.0) for k in range(group)], axis=0
            )
        )
        w_ref[...] = jnp.concatenate(
            [
                jnp.concatenate([high, high], axis=1),
                jnp.concatenate([low, jnp.zeros_like(low)], axis=1),
            ],
            axis=0,
        )

    block = vectors_ref.shape[0]
    rows = pl.ds(pl.multiple_of(pl.program_id(0) * block, block), block)
    for k in range(vectors_ref.shape[1] // LANES):
        at = slice(k * LANES, (k + 1) * LANES)
        both = dot(jnp.concatenate(split(stepped_ref[rows, at]), axis=1), w_ref[...], NT)
        vectors_ref[:, at] = both[:, :LANES] + both[:, LANES:]


def vmem():
    return pl.BlockSpec(memory_space=pltpu.VMEM)


def cost(flops, moved):
    return pl.CostEstimate(flops=int(flops), bytes_accessed=int(moved), transcendentals=0)


def body(tangents, base_flow, mode_mask, decay_rates, to_eigen, from_eigen):
    modes, planes, width = tangents.shape
    z_length = base_flow.shape[2]
    vecs = width // z_length
    row_devices, col_devices = lax.axis_size("row"), lax.axis_size("col")
    devices = row_devices * col_devices
    x_count, z_count = modes * row_devices, z_length * col_devices
    tiles = width // LANES
    rows = modes * tiles
    extra = -(-modes * z_length // LANES)
    size = tangents.size * 4
    both = ("col", "row")
    pitch = 8 * (z_count // 8 + 1 - z_count // 8 % 2)
    big = pltpu.CompilerParams(vmem_limit_bytes=40 * 2**20)
    small = pltpu.CompilerParams(vmem_limit_bytes=24 * 2**20)

    order = np.arange(x_count)
    order = (order % row_devices) * modes + order // row_devices
    halves = -(-x_count // LANES)
    points = np.arange(halves * LANES)
    points = np.where(points < x_count, points, points - (halves * LANES - x_count))
    sx_high, sx_low = halves_of_table(synthesis(x_count)[points][:, order].T)
    sx = np.concatenate([sx_high, sx_high, sx_low], axis=0)
    sz, az = (
        np.concatenate([high, low, high], axis=1)
        for high, low in map(halves_of_table, (synthesis(z_count), analysis(z_count)))
    )
    gx = np.concatenate(
        halves_of_table(derivative_analysis(x_count, ALPHA_X)[order][:, points]), axis=0
    )

    steps = 1
    base = jnp.transpose(base_flow, (0, 2, 1)).reshape(modes * z_length, planes)
    packed = pl.pallas_call(
        functools.partial(pack_kernel, modes=modes, planes=planes, tiles=tiles, extra=extra),
        out_shape=jax.ShapeDtypeStruct((planes * (rows + extra), LANES), F32),
        in_specs=[vmem()] * 2,
        out_specs=vmem(),
        cost_estimate=cost(10**9, 2 * size),
        compiler_params=small,
        name="pack",
    )(tangents, base)
    received = lax.all_to_all(
        packed.reshape(devices, rows + extra, 1, LANES), both, 0, 0, tiled=True
    ).reshape(packed.shape)

    returned = pl.pallas_call(
        functools.partial(
            transform_kernel, modes=modes, row_devices=row_devices,
            col_devices=col_devices, tiles=tiles, extra=extra, vecs=vecs,
        ),
        out_shape=jax.ShapeDtypeStruct((devices * rows, LANES), F32),
        in_specs=[vmem()] * 5,
        out_specs=vmem(),
        scratch_shapes=[pltpu.VMEM((z_count, halves * LANES), F32)]
        + [pltpu.VMEM((pitch * vecs, LANES), F32)] * (2 * halves),
        cost_estimate=cost(2 * 10**10, 2 * size),
        compiler_params=big,
        name="transform",
    )(received, sx, sz, az, gx)
    nonlinear = lax.all_to_all(
        returned.reshape(devices, rows, LANES), both, 0, 0, tiled=True
    ).reshape(returned.shape)

    piece = vecs * vecs // LANES
    height = modes * planes
    stepped, grams = pl.pallas_call(
        functools.partial(
            column_kernel, modes=modes, planes=planes, tiles=tiles, vecs=vecs,
            step_modes=modes // steps, x_count=x_count, z_count=z_count, z_length=z_length,
        ),
        out_shape=[
            jax.ShapeDtypeStruct((height, width), F32),
            jax.ShapeDtypeStruct((devices, piece, LANES), F32),
        ],
        grid=(steps,),
        in_specs=[vmem()] * 6,
        out_specs=[vmem()] * 2,
        scratch_shapes=[
            pltpu.VMEM((modes, width), F32),
            pltpu.VMEM((modes, width), F32),
            pltpu.VMEM((planes, LANES), F32),
            pltpu.VMEM((LANES, 2 * LANES), F32),
        ],
        cost_estimate=cost(10**10, 3 * size),
        compiler_params=small,
        name="column",
    )(nonlinear, tangents, mode_mask, decay_rates[None, :], to_eigen, from_eigen)
    grams = lax.all_to_all(grams, both, 0, 0, tiled=True).reshape(devices * piece, LANES)

    block = height // 2
    vectors, growth = pl.pallas_call(
        functools.partial(finish_kernel, devices=devices, vecs=vecs, panel=8),
        out_shape=[
            jax.ShapeDtypeStruct((height, width), F32),
            jax.ShapeDtypeStruct((1, vecs), F32),
        ],
        grid=(height // block,),
        in_specs=[vmem()] * 2,
        out_specs=[
            pl.BlockSpec((block, width), lambda i: (i, 0)),
            pl.BlockSpec((1, vecs), lambda i: (0, 0)),
        ],
        scratch_shapes=[pltpu.VMEM((2 * LANES, 2 * LANES), BF16)],
        cost_estimate=cost(2 * height * width * 256, 2 * size),
        compiler_params=small,
        name="finish",
    )(grams, stepped)
    return vectors.reshape(tangents.shape), growth[0]


def solution(mesh):
    placed = (P("row", None, "col"), P("row", None, "col"), P("row", "col"), P(), P(), P())
    return jax.shard_map(
        body, mesh=mesh, in_specs=placed, out_specs=(P("row", None, "col"), P()), check_vma=False
    )
```

```python
import functools

import jax
import jax.numpy as jnp
import numpy as np
from jax import lax
from jax.experimental import pallas as pl
from jax.experimental.pallas import tpu as pltpu
from jax.sharding import PartitionSpec as P

STEP_COEF = 10.0
VISCOSITY = 0.01
ALPHA_X = 0.5
BETA_Z = 1.0
LANES = 128
F32 = jnp.float32
BF16 = jnp.bfloat16
NN = (((1,), (0,)), ((), ()))
NT = (((1,), (1,)), ((), ()))
TN = (((0,), (0,)), ((), ()))


def synthesis(count):
    points = np.arange(count)[:, None]
    modes = np.arange(count)[None, :]
    middle = count // 2
    waves = np.where(modes <= middle, modes, modes - middle)
    angles = (points * waves % count) * (2.0 * np.pi / count)
    return np.where(modes <= middle, np.cos(angles), np.sin(angles))


def analysis(count):
    modes = np.arange(count)
    weights = np.where((modes == 0) | (modes == count // 2), 1.0 / count, 2.0 / count)
    return weights[:, None] * synthesis(count).T


def derivative_analysis(count, scale):
    middle = count // 2
    derivative = np.zeros((count, count))
    for k in range(1, middle):
        derivative[k, middle + k] = k
        derivative[middle + k, k] = -k
    return -scale * (derivative @ analysis(count))


def halves_of_table(table):
    table = np.asarray(table, np.float64)
    high = table.astype(np.float32).astype(jnp.bfloat16)
    low = (table - high.astype(np.float64)).astype(np.float32).astype(jnp.bfloat16)
    return np.stack([high, low])


def split(x):
    high = x.astype(BF16)
    return high, (x - high.astype(F32)).astype(BF16)


def dot(a, b, dims):
    return lax.dot_general(a, b, dims, preferred_element_type=F32)


def dot3(a, b, dims):
    return dot(a[0], b[0], dims) + (dot(a[0], b[1], dims) + dot(a[1], b[0], dims))


def stacked_dot(table, x):
    high, low = split(x)
    return dot(table, jnp.concatenate([high, high], axis=0), NN) + dot(
        table[:, : x.shape[0]], low, NN
    )


def table_dot(table_ref, x):
    high, low = split(x)
    return dot(table_ref[...], jnp.concatenate([high, high, low], axis=0), NN)


def pack_kernel(q_ref, base_ref, out_ref, *, modes, planes, tiles, extra):
    stride = modes * tiles + extra
    part = base_ref.shape[0] // extra
    fill = jnp.zeros((LANES - part, planes), F32)
    for k in range(extra):
        block = jnp.concatenate([base_ref[k * part : (k + 1) * part, :], fill], axis=0)
        out_ref[pl.ds(modes * tiles + k, planes, stride=stride), :] = block.T
    for m in range(modes):
        for nb in range(tiles):
            out_ref[pl.ds(nb * modes + m, planes, stride=stride), :] = q_ref[
                m, :, nb * LANES : (nb + 1) * LANES
            ]


def transform_kernel(
    d_ref, sx_ref, sz_ref, az_ref, g_ref, out_ref, speed_ref, *scratch,
    modes, row_devices, col_devices, tiles, extra, vecs,
):
    halves = len(scratch) // 2
    y_refs, z_refs = scratch[:halves], scratch[halves:]
    rows = modes * tiles
    stride = rows + extra
    x_count = modes * row_devices
    z_count = sz_ref.shape[0]
    z_length = z_count // col_devices
    pitch = y_refs[0].shape[0] // vecs
    per_tile = LANES // vecs

    turned = []
    for k in range(extra):
        block = d_ref[pl.ds(rows + k, row_devices * col_devices, stride=stride), :]
        turned.append(block.T)
    slot = lax.broadcasted_iota(jnp.int32, (z_length, LANES), 1) // row_devices
    slots = LANES // row_devices
    share = modes // extra
    sheets = []
    for c in range(col_devices):
        parts = [jnp.zeros((z_length, LANES), F32) for _ in range(halves)]
        for m in range(modes):
            piece = turned[m // share][(m % share) * z_length : (m % share + 1) * z_length]
            shift = ((m % slots - c) * row_devices) % LANES
            piece = pltpu.roll(piece, shift, 1) if shift else piece
            parts[m // slots] = jnp.where(slot == m % slots, piece, parts[m // slots])
        sheets.append(jnp.concatenate(parts, axis=1))
    base = jnp.concatenate(sheets, axis=0)[:, :x_count]
    sx = (sx_ref[:x_count], sx_ref[2 * x_count :])
    speed_ref[...] = table_dot(sz_ref, dot3(split(base), sx, NN))

    def forward_x(c, carry):
        parts = []
        for nb in range(tiles):
            start = c * (row_devices * stride) + nb * modes
            block = jnp.concatenate(
                [d_ref[pl.ds(start + m, row_devices, stride=stride), :] for m in range(modes)],
                axis=0,
            )
            block = jnp.concatenate(split(block), axis=0).T
            parts.append(jnp.concatenate([block, block[:, :x_count]], axis=1))
        mixed = dot(jnp.concatenate(parts, axis=0), sx_ref[...], NN)
        for n in range(z_length):
            for k, y_ref in enumerate(y_refs):
                y_ref[pl.ds(c * z_length + n, vecs, stride=pitch), :] = mixed[
                    n * vecs : (n + 1) * vecs, k * LANES : (k + 1) * LANES
                ]
        return carry

    lax.fori_loop(0, col_devices, forward_x, 0, unroll=8)

    y_low, y_high = y_refs
    z_low, z_high = z_refs
    first = lax.broadcasted_iota(jnp.int32, (z_count, LANES), 1) < LANES // 2
    batch = 8

    def plane(i, carry):
        ats = [
            pl.ds(pl.multiple_of((i * batch + j) * pitch, 8), z_count) for j in range(batch)
        ]
        mixed = jnp.concatenate(
            [y_low[at, :] for at in ats]
            + [
                jnp.where(first, y_high[ats[j], :], y_high[ats[j + 1], :])
                for j in range(0, batch, 2)
            ],
            axis=1,
        )
        speed = jnp.concatenate(
            [speed_ref[:, :LANES]] * batch + [speed_ref[:, LANES:]] * (batch // 2), axis=1
        )
        mixed = table_dot(az_ref, table_dot(sz_ref, mixed) * speed)
        for j, at in enumerate(ats):
            k = batch + j // 2
            z_low[at, :] = mixed[:, j * LANES : (j + 1) * LANES]
            z_high[at, :] = mixed[:, k * LANES : (k + 1) * LANES]
        return carry

    lax.fori_loop(0, vecs // batch, plane, 0, unroll=2)

    rows_of = lax.broadcasted_iota(jnp.int32, (vecs, LANES), 0)
    lanes_of = lax.broadcasted_iota(jnp.int32, (vecs, LANES), 1)
    mine = (rows_of % 2) == (lanes_of // (LANES // 2))

    def inverse_x(c, carry):
        block = jnp.concatenate(
            [
                jnp.concatenate(
                    [
                        z_low[pl.ds(c * z_length + n, vecs, stride=pitch), :],
                        jnp.where(
                            mine, z_high[pl.ds(c * z_length + n, vecs, stride=pitch), :], 0.0
                        ),
                    ],
                    axis=1,
                )
                for n in range(z_length)
            ],
            axis=0,
        )
        high, low = split(block)
        both = dot(g_ref[...], high, NT)
        back = both[:x_count] + (both[x_count:] + dot(g_ref[:x_count], low, NT))
        for nb in range(tiles):
            start = c * (row_devices * rows) + nb * modes
            for m in range(modes):
                out_ref[pl.ds(start + m, row_devices, stride=rows), :] = back[
                    m * row_devices : (m + 1) * row_devices, nb * LANES : (nb + 1) * LANES
                ]
        return carry

    lax.fori_loop(0, col_devices, inverse_x, 0, unroll=8)


def column_kernel(
    nl_ref, q_ref, mask_ref, decay_ref, to_ref, from_ref, stepped_ref, gram_ref,
    mask_s, wave_s, decay_s, gram_s,
    *, modes, planes, tiles, vecs, step_modes, x_count, z_count, z_length,
):
    width = tiles * LANES

    @pl.when(pl.program_id(0) == 0)
    def _():
        lane = lax.broadcasted_iota(jnp.int32, (z_length, width), 1) // vecs
        row = lax.broadcasted_iota(jnp.int32, (z_length, width), 0)
        spread = jnp.where(lane == row, 1.0, 0.0).astype(BF16)
        mask_s[...] = dot(mask_ref[...].astype(F32).astype(BF16), spread, NN)
        n = lax.broadcasted_iota(jnp.int32, (modes, width), 1) // vecs
        n = n + lax.axis_index("col") * z_length
        m = lax.broadcasted_iota(jnp.int32, (modes, width), 0)
        m = m + lax.axis_index("row") * modes
        wave_x = jnp.where(m <= x_count // 2, m, m - x_count // 2).astype(F32) * ALPHA_X
        wave_z = jnp.where(n <= z_count // 2, n, n - z_count // 2).astype(F32) * BETA_Z
        wave_s[...] = STEP_COEF + VISCOSITY * (wave_x * wave_x + wave_z * wave_z)
        decay_s[...] = jnp.broadcast_to(decay_ref[...], (LANES, planes)).T
        gram_s[...] = jnp.zeros_like(gram_s)

    to_eigen = jnp.concatenate(split(to_ref[...]), axis=1)
    from_eigen = jnp.concatenate(split(from_ref[...]), axis=1)
    decay = jnp.concatenate([decay_s[...]] * tiles, axis=1)
    gram = gram_s[...]
    for k in range(step_modes):
        m = pl.program_id(0) * step_modes + k
        nonlinear = jnp.concatenate(
            [
                nl_ref[pl.ds(nb * modes + m, planes, stride=tiles * modes), :]
                for nb in range(tiles)
            ],
            axis=1,
        )
        right = STEP_COEF * q_ref[m] + nonlinear * mask_s[pl.ds(m, 1), :]
        eigen = stacked_dot(to_eigen, right)
        eigen = eigen / (wave_s[pl.ds(m, 1), :] + decay)
        stepped = stacked_dot(from_eigen, eigen)
        stepped_ref[pl.ds(pl.multiple_of(m * planes, planes), planes), :] = stepped
        columns = [stepped[:, nb * LANES : (nb + 1) * LANES] for nb in range(tiles)]
        left = jnp.concatenate([x.T.astype(BF16) for x in columns], axis=1)
        right = jnp.concatenate(
            [jnp.concatenate(split(x), axis=1) for x in columns], axis=0
        )
        gram = gram + dot(left, right, NN)
    gram_s[...] = gram

    @pl.when(pl.program_id(0) == pl.num_programs(0) - 1)
    def _():
        high, cross = gram[:, :LANES], gram[:, LANES:]
        full = (high + (cross + cross.T)) * (1.0 / (x_count * planes * z_count))
        group = LANES // vecs
        lane = lax.broadcasted_iota(jnp.int32, (vecs, LANES), 1) // vecs
        folded = jnp.zeros((vecs, LANES), F32)
        for k in range(group):
            folded = folded + jnp.where(lane == k, full[k * vecs : (k + 1) * vecs], 0.0)
        folded = folded + pltpu.roll(folded, LANES // 2, 1)
        folded = folded + pltpu.roll(folded, LANES // 4, 1)
        half = vecs // 2
        lane = lax.broadcasted_iota(jnp.int32, (half, LANES), 1)
        row = lax.broadcasted_iota(jnp.int32, (half, LANES), 0)
        top, shifted = folded[:half], pltpu.roll(folded[half:], LANES - half, 1)
        square = jnp.where((lane % vecs < half) & (lane % vecs < row), shifted, top)
        piece = half // group
        spread = lane[:piece] // vecs
        packed = jnp.zeros((piece, LANES), F32)
        for k in range(group):
            packed = jnp.where(spread == k, square[k * piece : (k + 1) * piece], packed)
        diagonal = jnp.sum(jnp.where(lane % vecs == row, shifted, 0.0), axis=0, keepdims=True)
        sent = [packed[k : k + 1] for k in range(piece)] + [diagonal]
        for k, line in enumerate(sent):
            gram_ref[pl.ds(k, planes, stride=len(sent)), :] = jnp.broadcast_to(
                line, (planes, LANES)
            )


def finish_kernel(grams_ref, stepped_ref, vectors_ref, growth_ref, w_ref, *, devices, vecs, panel):
    group = LANES // vecs
    half = vecs // 2
    piece = half // group

    @pl.when(pl.program_id(0) == 0)
    def _():
        lines = [
            jnp.sum(
                grams_ref[pl.ds(k, devices, stride=piece + 1), :], axis=0, keepdims=True
            )
            for k in range(piece + 1)
        ]
        packed = jnp.concatenate(lines[:piece], axis=0)
        square = jnp.concatenate(
            [pltpu.roll(packed, (LANES - k * vecs) % LANES, 1) for k in range(group)], axis=0
        )
        turned = jnp.concatenate([square, jnp.zeros((LANES - half, LANES), F32)], axis=0).T
        lane = lax.broadcasted_iota(jnp.int32, (half, LANES), 1)
        row = lax.broadcasted_iota(jnp.int32, (half, LANES), 0)
        top = jnp.where((lane < half) & (lane < row), turned[:half], square)
        right = jnp.where(lane < row, square, jnp.where(lane == row, lines[piece], turned[:half]))
        bottom = jnp.where(lane < half, turned[half:vecs], pltpu.roll(right, half, 1))
        gram = jnp.concatenate([top, bottom], axis=0)
        lane = lax.broadcasted_iota(jnp.int32, (vecs, LANES), 1)
        row = lax.broadcasted_iota(jnp.int32, (vecs, LANES), 0)
        work = jnp.where(lane < vecs, gram, jnp.where(lane == row + vecs, 1.0, 0.0))
        for first in range(0, vecs, panel):
            own = range(first, first + panel)
            columns = [jnp.broadcast_to(work[:, k : k + 1], (vecs, LANES)) for k in own]
            lines = [work[k : k + 1, :] for k in own]
            for j, k in enumerate(own):
                pivot = columns[j][k : k + 1]
                column = jnp.where(row > k, columns[j], 0.0)
                scaled = lines[j] / pivot
                for i in range(j + 1, panel):
                    columns[i] = columns[i] - column * (columns[i][k : k + 1] / pivot)
                    lines[i] = lines[i] - columns[j][first + i : first + i + 1] * scaled
                work = work - column * scaled
        pivots = jnp.sum(jnp.where(lane == row, work, 0.0), axis=1, keepdims=True)
        diagonal = jnp.sqrt(pivots)
        inverse = work / diagonal
        across = jnp.sum(jnp.where(lane == row, diagonal, 0.0), axis=0, keepdims=True)
        growth_ref[...] = jnp.log(across[:, :vecs])
        inverse = jnp.where((lane >= vecs) & (lane < 2 * vecs), inverse, 0.0)
        inverse = inverse + pltpu.roll(inverse, LANES // 2, 1)
        inverse = inverse + pltpu.roll(inverse, LANES // 4, 1)
        high, low = split(
            jnp.concatenate(
                [jnp.where(lane // vecs == k, inverse, 0.0) for k in range(group)], axis=0
            )
        )
        w_ref[...] = jnp.concatenate(
            [
                jnp.concatenate([high, high], axis=1),
                jnp.concatenate([low, jnp.zeros_like(low)], axis=1),
            ],
            axis=0,
        )

    block = vectors_ref.shape[0]
    rows = pl.ds(pl.multiple_of(pl.program_id(0) * block, block), block)
    for k in range(vectors_ref.shape[1] // LANES):
        at = slice(k * LANES, (k + 1) * LANES)
        both = dot(jnp.concatenate(split(stepped_ref[rows, at]), axis=1), w_ref[...], NT)
        vectors_ref[:, at] = both[:, :LANES] + both[:, LANES:]


def vmem():
    return pl.BlockSpec(memory_space=pltpu.VMEM)


def cost(flops, moved):
    return pl.CostEstimate(flops=int(flops), bytes_accessed=int(moved), transcendentals=0)


def body(tangents, base_flow, mode_mask, decay_rates, to_eigen, from_eigen):
    modes, planes, width = tangents.shape
    z_length = base_flow.shape[2]
    vecs = width // z_length
    row_devices, col_devices = lax.axis_size("row"), lax.axis_size("col")
    devices = row_devices * col_devices
    x_count, z_count = modes * row_devices, z_length * col_devices
    tiles = width // LANES
    rows = modes * tiles
    extra = -(-modes * z_length // LANES)
    size = tangents.size * 4
    both = ("col", "row")
    pitch = 8 * (z_count // 8 + 1 - z_count // 8 % 2)
    big = pltpu.CompilerParams(vmem_limit_bytes=40 * 2**20)
    small = pltpu.CompilerParams(vmem_limit_bytes=24 * 2**20)

    order = np.arange(x_count)
    order = (order % row_devices) * modes + order // row_devices
    halves = -(-x_count // LANES)
    points = np.arange(halves * LANES)
    points = np.where(points < x_count, points, points - (halves * LANES - x_count))
    sx_high, sx_low = halves_of_table(synthesis(x_count)[points][:, order].T)
    sx = np.concatenate([sx_high, sx_high, sx_low], axis=0)
    sz, az = (
        np.concatenate([high, low, high], axis=1)
        for high, low in map(halves_of_table, (synthesis(z_count), analysis(z_count)))
    )
    gx = np.concatenate(
        halves_of_table(derivative_analysis(x_count, ALPHA_X)[order][:, points]), axis=0
    )

    steps = 1
    base = jnp.transpose(base_flow, (0, 2, 1)).reshape(modes * z_length, planes)
    packed = pl.pallas_call(
        functools.partial(pack_kernel, modes=modes, planes=planes, tiles=tiles, extra=extra),
        out_shape=jax.ShapeDtypeStruct((planes * (rows + extra), LANES), F32),
        in_specs=[vmem()] * 2,
        out_specs=vmem(),
        cost_estimate=cost(10**9, 2 * size),
        compiler_params=small,
        name="pack",
    )(tangents, base)
    received = lax.all_to_all(
        packed.reshape(devices, rows + extra, 1, LANES), both, 0, 0, tiled=True
    ).reshape(packed.shape)

    returned = pl.pallas_call(
        functools.partial(
            transform_kernel, modes=modes, row_devices=row_devices,
            col_devices=col_devices, tiles=tiles, extra=extra, vecs=vecs,
        ),
        out_shape=jax.ShapeDtypeStruct((devices * rows, LANES), F32),
        in_specs=[vmem()] * 5,
        out_specs=vmem(),
        scratch_shapes=[pltpu.VMEM((z_count, halves * LANES), F32)]
        + [pltpu.VMEM((pitch * vecs, LANES), F32)] * (2 * halves),
        cost_estimate=cost(2 * 10**10, 2 * size),
        compiler_params=big,
        name="transform",
    )(received, sx, sz, az, gx)
    nonlinear = lax.all_to_all(
        returned.reshape(devices, rows, LANES), both, 0, 0, tiled=True
    ).reshape(returned.shape)

    lines = vecs * vecs // (2 * LANES) + 1
    height = modes * planes
    stepped, grams = pl.pallas_call(
        functools.partial(
            column_kernel, modes=modes, planes=planes, tiles=tiles, vecs=vecs,
            step_modes=modes // steps, x_count=x_count, z_count=z_count, z_length=z_length,
        ),
        out_shape=[
            jax.ShapeDtypeStruct((height, width), F32),
            jax.ShapeDtypeStruct((devices * lines, LANES), F32),
        ],
        grid=(steps,),
        in_specs=[vmem()] * 6,
        out_specs=[vmem()] * 2,
        scratch_shapes=[
            pltpu.VMEM((modes, width), F32),
            pltpu.VMEM((modes, width), F32),
            pltpu.VMEM((planes, LANES), F32),
            pltpu.VMEM((LANES, 2 * LANES), F32),
        ],
        cost_estimate=cost(10**10, 3 * size),
        compiler_params=small,
        name="column",
    )(nonlinear, tangents, mode_mask, decay_rates[None, :], to_eigen, from_eigen)
    grams = lax.all_to_all(
        grams.reshape(devices, lines, 1, LANES), both, 0, 0, tiled=True
    ).reshape(grams.shape)

    block = height // 2
    vectors, growth = pl.pallas_call(
        functools.partial(finish_kernel, devices=devices, vecs=vecs, panel=8),
        out_shape=[
            jax.ShapeDtypeStruct((height, width), F32),
            jax.ShapeDtypeStruct((1, vecs), F32),
        ],
        grid=(height // block,),
        in_specs=[vmem()] * 2,
        out_specs=[
            pl.BlockSpec((block, width), lambda i: (i, 0)),
            pl.BlockSpec((1, vecs), lambda i: (0, 0)),
        ],
        scratch_shapes=[pltpu.VMEM((2 * LANES, 2 * LANES), BF16)],
        cost_estimate=cost(2 * height * width * 256, 2 * size),
        compiler_params=small,
        name="finish",
    )(grams, stepped)
    return vectors.reshape(tangents.shape), growth[0]


def solution(mesh):
    placed = (P("row", None, "col"), P("row", None, "col"), P("row", "col"), P(), P(), P())
    return jax.shard_map(
        body, mesh=mesh, in_specs=placed, out_specs=(P("row", None, "col"), P()), check_vma=False
    )
```

```python
import functools

import jax
import jax.numpy as jnp
import numpy as np
from jax import lax
from jax.experimental import pallas as pl
from jax.experimental.pallas import tpu as pltpu
from jax.sharding import PartitionSpec as P

STEP_COEF = 10.0
VISCOSITY = 0.01
ALPHA_X = 0.5
BETA_Z = 1.0
LANES = 128
F32 = jnp.float32
BF16 = jnp.bfloat16
NN = (((1,), (0,)), ((), ()))
NT = (((1,), (1,)), ((), ()))
TN = (((0,), (0,)), ((), ()))


def synthesis(count):
    points = np.arange(count)[:, None]
    modes = np.arange(count)[None, :]
    middle = count // 2
    waves = np.where(modes <= middle, modes, modes - middle)
    angles = (points * waves % count) * (2.0 * np.pi / count)
    return np.where(modes <= middle, np.cos(angles), np.sin(angles))


def analysis(count):
    modes = np.arange(count)
    weights = np.where((modes == 0) | (modes == count // 2), 1.0 / count, 2.0 / count)
    return weights[:, None] * synthesis(count).T


def derivative_analysis(count, scale):
    middle = count // 2
    derivative = np.zeros((count, count))
    for k in range(1, middle):
        derivative[k, middle + k] = k
        derivative[middle + k, k] = -k
    return -scale * (derivative @ analysis(count))


def halves_of_table(table):
    table = np.asarray(table, np.float64)
    high = table.astype(np.float32).astype(jnp.bfloat16)
    low = (table - high.astype(np.float64)).astype(np.float32).astype(jnp.bfloat16)
    return np.stack([high, low])


def split(x):
    high = x.astype(BF16)
    return high, (x - high.astype(F32)).astype(BF16)


def dot(a, b, dims):
    return lax.dot_general(a, b, dims, preferred_element_type=F32)


def dot3(a, b, dims):
    return dot(a[0], b[0], dims) + (dot(a[0], b[1], dims) + dot(a[1], b[0], dims))


def stacked_dot(table, x):
    high, low = split(x)
    return dot(table, jnp.concatenate([high, high], axis=0), NN) + dot(
        table[:, : x.shape[0]], low, NN
    )


def tripled(table):
    high, low = halves_of_table(table)
    return np.concatenate([high, low, high], axis=1)


def table_dot(table_ref, high, low):
    return dot(table_ref[...], jnp.concatenate([high, high, low], axis=0), NN)


def parity_tables(count):
    middle = count // 2
    wide, tall = middle + 16, middle + 8
    to_points, to_modes = synthesis(count), analysis(count)
    weights = np.where(np.arange(middle + 1) % middle == 0, 1.0, 2.0)
    even_points = np.zeros((wide, wide))
    even_points[: middle + 1, : middle + 1] = to_points[: middle + 1, : middle + 1]
    odd_points = np.zeros((middle, middle))
    odd_points[1:, 1:] = to_points[1:middle, middle + 1 :]
    even_modes = np.zeros((tall, wide))
    even_modes[: middle + 1, : middle + 1] = to_modes[: middle + 1, : middle + 1] * weights
    odd_modes = np.zeros((middle, middle))
    odd_modes[1:, 1:] = 2.0 * to_modes[middle + 1 :, 1:middle]
    return [tripled(t) for t in (even_points, odd_points, even_modes, odd_modes)]


def to_parity_points(even_ref, odd_ref, x):
    high, low = split(x)
    wide, middle = even_ref.shape[0], odd_ref.shape[0]
    return (
        table_dot(even_ref, high[:wide], low[:wide]),
        table_dot(odd_ref, high[middle:], low[middle:]),
    )


def pack_kernel(q_ref, base_ref, out_ref, *, modes, planes, tiles, extra):
    stride = modes * tiles + extra
    part = base_ref.shape[0] // extra
    fill = jnp.zeros((LANES - part, planes), F32)
    for k in range(extra):
        block = jnp.concatenate([base_ref[k * part : (k + 1) * part, :], fill], axis=0)
        out_ref[pl.ds(modes * tiles + k, planes, stride=stride), :] = block.T
    for m in range(modes):
        for nb in range(tiles):
            out_ref[pl.ds(nb * modes + m, planes, stride=stride), :] = q_ref[
                m, :, nb * LANES : (nb + 1) * LANES
            ]


def transform_kernel(
    d_ref, sx_ref, even_p_ref, odd_p_ref, even_m_ref, odd_m_ref, g_ref, out_ref, speed_ref,
    *scratch,
    modes, row_devices, col_devices, tiles, extra, vecs,
):
    halves = len(scratch) // 2
    y_refs, z_refs = scratch[:halves], scratch[halves:]
    rows = modes * tiles
    stride = rows + extra
    x_count = modes * row_devices
    wide, tall, middle = even_p_ref.shape[0], even_m_ref.shape[0], odd_p_ref.shape[0]
    z_count = 2 * middle
    z_length = z_count // col_devices
    pitch = y_refs[0].shape[0] // vecs
    per_tile = LANES // vecs

    turned = []
    for k in range(extra):
        block = d_ref[pl.ds(rows + k, row_devices * col_devices, stride=stride), :]
        turned.append(block.T)
    slot = lax.broadcasted_iota(jnp.int32, (z_length, LANES), 1) // row_devices
    slots = LANES // row_devices
    share = modes // extra
    sheets = []
    for c in range(col_devices):
        parts = [jnp.zeros((z_length, LANES), F32) for _ in range(halves)]
        for m in range(modes):
            piece = turned[m // share][(m % share) * z_length : (m % share + 1) * z_length]
            shift = ((m % slots - c) * row_devices) % LANES
            piece = pltpu.roll(piece, shift, 1) if shift else piece
            parts[m // slots] = jnp.where(slot == m % slots, piece, parts[m // slots])
        sheets.append(jnp.concatenate(parts, axis=1))
    base = jnp.concatenate(sheets, axis=0)[:, :x_count]
    sx = (sx_ref[:x_count], sx_ref[2 * x_count :])
    even, odd = to_parity_points(even_p_ref, odd_p_ref, dot3(split(base), sx, NN))
    speed_ref[:wide] = even
    speed_ref[wide:] = odd

    def forward_x(c, carry):
        parts = []
        for nb in range(tiles):
            start = c * (row_devices * stride) + nb * modes
            block = jnp.concatenate(
                [d_ref[pl.ds(start + m, row_devices, stride=stride), :] for m in range(modes)],
                axis=0,
            )
            block = jnp.concatenate(split(block), axis=0).T
            parts.append(jnp.concatenate([block, block[:, :x_count]], axis=1))
        mixed = dot(jnp.concatenate(parts, axis=0), sx_ref[...], NN)
        for n in range(z_length):
            for k, y_ref in enumerate(y_refs):
                y_ref[pl.ds(c * z_length + n, vecs, stride=pitch), :] = mixed[
                    n * vecs : (n + 1) * vecs, k * LANES : (k + 1) * LANES
                ]
        return carry

    lax.fori_loop(0, col_devices, forward_x, 0, unroll=8)

    y_low, y_high = y_refs
    z_low, z_high = z_refs
    first = lax.broadcasted_iota(jnp.int32, (z_count, LANES), 1) < LANES // 2
    batch = 8

    def plane(i, carry):
        ats = [
            pl.ds(pl.multiple_of((i * batch + j) * pitch, 8), z_count) for j in range(batch)
        ]
        mixed = jnp.concatenate(
            [y_low[at, :] for at in ats]
            + [
                jnp.where(first, y_high[ats[j], :], y_high[ats[j + 1], :])
                for j in range(0, batch, 2)
            ],
            axis=1,
        )
        speed = jnp.concatenate(
            [speed_ref[:, :LANES]] * batch + [speed_ref[:, LANES:]] * (batch // 2), axis=1
        )
        even, odd = to_parity_points(even_p_ref, odd_p_ref, mixed)
        even_speed, odd_speed = speed[:wide], speed[wide:]
        cross = even[:middle] * odd_speed + odd * even_speed[:middle]
        even = even * even_speed
        even = jnp.concatenate([even[:middle] + odd * odd_speed, even[middle:]], axis=0)
        even = table_dot(even_m_ref, *split(even))
        odd = table_dot(odd_m_ref, *split(cross))
        mixed = jnp.concatenate(
            [
                even[:middle],
                even[middle:] + odd[: tall - middle],
                odd[tall - middle :],
            ],
            axis=0,
        )
        for j, at in enumerate(ats):
            k = batch + j // 2
            z_low[at, :] = mixed[:, j * LANES : (j + 1) * LANES]
            z_high[at, :] = mixed[:, k * LANES : (k + 1) * LANES]
        return carry

    lax.fori_loop(0, vecs // batch, plane, 0, unroll=4)

    rows_of = lax.broadcasted_iota(jnp.int32, (vecs, LANES), 0)
    lanes_of = lax.broadcasted_iota(jnp.int32, (vecs, LANES), 1)
    mine = (rows_of % 2) == (lanes_of // (LANES // 2))

    def inverse_x(c, carry):
        block = jnp.concatenate(
            [
                jnp.concatenate(
                    [
                        z_low[pl.ds(c * z_length + n, vecs, stride=pitch), :],
                        jnp.where(
                            mine, z_high[pl.ds(c * z_length + n, vecs, stride=pitch), :], 0.0
                        ),
                    ],
                    axis=1,
                )
                for n in range(z_length)
            ],
            axis=0,
        )
        high, low = split(block)
        both = dot(g_ref[...], high, NT)
        back = both[:x_count] + (both[x_count:] + dot(g_ref[:x_count], low, NT))
        for nb in range(tiles):
            start = c * (row_devices * rows) + nb * modes
            for m in range(modes):
                out_ref[pl.ds(start + m, row_devices, stride=rows), :] = back[
                    m * row_devices : (m + 1) * row_devices, nb * LANES : (nb + 1) * LANES
                ]
        return carry

    lax.fori_loop(0, col_devices, inverse_x, 0, unroll=8)


def column_kernel(
    nl_ref, q_ref, mask_ref, decay_ref, to_ref, from_ref, stepped_ref, gram_ref,
    mask_s, wave_s, decay_s, gram_s,
    *, modes, planes, tiles, vecs, step_modes, x_count, z_count, z_length,
):
    width = tiles * LANES

    @pl.when(pl.program_id(0) == 0)
    def _():
        lane = lax.broadcasted_iota(jnp.int32, (z_length, width), 1) // vecs
        row = lax.broadcasted_iota(jnp.int32, (z_length, width), 0)
        spread = jnp.where(lane == row, 1.0, 0.0).astype(BF16)
        mask_s[...] = dot(mask_ref[...].astype(F32).astype(BF16), spread, NN)
        n = lax.broadcasted_iota(jnp.int32, (modes, width), 1) // vecs
        n = n + lax.axis_index("col") * z_length
        m = lax.broadcasted_iota(jnp.int32, (modes, width), 0)
        m = m + lax.axis_index("row") * modes
        wave_x = jnp.where(m <= x_count // 2, m, m - x_count // 2).astype(F32) * ALPHA_X
        wave_z = jnp.where(n <= z_count // 2, n, n - z_count // 2).astype(F32) * BETA_Z
        wave_s[...] = STEP_COEF + VISCOSITY * (wave_x * wave_x + wave_z * wave_z)
        decay_s[...] = jnp.broadcast_to(decay_ref[...], (LANES, planes)).T
        gram_s[...] = jnp.zeros_like(gram_s)

    to_eigen = jnp.concatenate(split(to_ref[...]), axis=1)
    from_eigen = jnp.concatenate(split(from_ref[...]), axis=1)
    decay = jnp.concatenate([decay_s[...]] * tiles, axis=1)
    gram = gram_s[...]
    for k in range(step_modes):
        m = pl.program_id(0) * step_modes + k
        nonlinear = jnp.concatenate(
            [
                nl_ref[pl.ds(nb * modes + m, planes, stride=tiles * modes), :]
                for nb in range(tiles)
            ],
            axis=1,
        )
        right = STEP_COEF * q_ref[m] + nonlinear * mask_s[pl.ds(m, 1), :]
        eigen = stacked_dot(to_eigen, right)
        eigen = eigen / (wave_s[pl.ds(m, 1), :] + decay)
        stepped = stacked_dot(from_eigen, eigen)
        stepped_ref[pl.ds(pl.multiple_of(m * planes, planes), planes), :] = stepped
        columns = [stepped[:, nb * LANES : (nb + 1) * LANES] for nb in range(tiles)]
        left = jnp.concatenate([x.T.astype(BF16) for x in columns], axis=1)
        right = jnp.concatenate(
            [jnp.concatenate(split(x), axis=1) for x in columns], axis=0
        )
        gram = gram + dot(left, right, NN)
    gram_s[...] = gram

    @pl.when(pl.program_id(0) == pl.num_programs(0) - 1)
    def _():
        high, cross = gram[:, :LANES], gram[:, LANES:]
        full = (high + (cross + cross.T)) * (1.0 / (x_count * planes * z_count))
        group = LANES // vecs
        lane = lax.broadcasted_iota(jnp.int32, (vecs, LANES), 1) // vecs
        folded = jnp.zeros((vecs, LANES), F32)
        for k in range(group):
            folded = folded + jnp.where(lane == k, full[k * vecs : (k + 1) * vecs], 0.0)
        folded = folded + pltpu.roll(folded, LANES // 2, 1)
        folded = folded + pltpu.roll(folded, LANES // 4, 1)
        half = vecs // 2
        lane = lax.broadcasted_iota(jnp.int32, (half, LANES), 1)
        row = lax.broadcasted_iota(jnp.int32, (half, LANES), 0)
        top, shifted = folded[:half], pltpu.roll(folded[half:], LANES - half, 1)
        square = jnp.where((lane % vecs < half) & (lane % vecs < row), shifted, top)
        piece = half // group
        spread = lane[:piece] // vecs
        packed = jnp.zeros((piece, LANES), F32)
        for k in range(group):
            packed = jnp.where(spread == k, square[k * piece : (k + 1) * piece], packed)
        diagonal = jnp.sum(jnp.where(lane % vecs == row, shifted, 0.0), axis=0, keepdims=True)
        sent = [packed[k : k + 1] for k in range(piece)] + [diagonal]
        for k, line in enumerate(sent):
            gram_ref[pl.ds(k, planes, stride=len(sent)), :] = jnp.broadcast_to(
                line, (planes, LANES)
            )


def finish_kernel(grams_ref, stepped_ref, vectors_ref, growth_ref, w_ref, *, devices, vecs, panel):
    group = LANES // vecs
    half = vecs // 2
    piece = half // group

    @pl.when(pl.program_id(0) == 0)
    def _():
        lines = [
            jnp.sum(
                grams_ref[pl.ds(k, devices, stride=piece + 1), :], axis=0, keepdims=True
            )
            for k in range(piece + 1)
        ]
        packed = jnp.concatenate(lines[:piece], axis=0)
        square = jnp.concatenate(
            [pltpu.roll(packed, (LANES - k * vecs) % LANES, 1) for k in range(group)], axis=0
        )
        turned = jnp.concatenate([square, jnp.zeros((LANES - half, LANES), F32)], axis=0).T
        lane = lax.broadcasted_iota(jnp.int32, (half, LANES), 1)
        row = lax.broadcasted_iota(jnp.int32, (half, LANES), 0)
        top = jnp.where((lane < half) & (lane < row), turned[:half], square)
        right = jnp.where(lane < row, square, jnp.where(lane == row, lines[piece], turned[:half]))
        bottom = jnp.where(lane < half, turned[half:vecs], pltpu.roll(right, half, 1))
        gram = jnp.concatenate([top, bottom], axis=0)
        lane = lax.broadcasted_iota(jnp.int32, (vecs, LANES), 1)
        row = lax.broadcasted_iota(jnp.int32, (vecs, LANES), 0)
        work = jnp.where(lane < vecs, gram, jnp.where(lane == row + vecs, 1.0, 0.0))
        for first in range(0, vecs, panel):
            own = range(first, first + panel)
            columns = [jnp.broadcast_to(work[:, k : k + 1], (vecs, LANES)) for k in own]
            lines = [work[k : k + 1, :] for k in own]
            for j, k in enumerate(own):
                pivot = columns[j][k : k + 1]
                column = jnp.where(row > k, columns[j], 0.0)
                scaled = lines[j] / pivot
                for i in range(j + 1, panel):
                    columns[i] = columns[i] - column * (columns[i][k : k + 1] / pivot)
                    lines[i] = lines[i] - columns[j][first + i : first + i + 1] * scaled
                work = work - column * scaled
        pivots = jnp.sum(jnp.where(lane == row, work, 0.0), axis=1, keepdims=True)
        diagonal = jnp.sqrt(pivots)
        inverse = work / diagonal
        across = jnp.sum(jnp.where(lane == row, diagonal, 0.0), axis=0, keepdims=True)
        growth_ref[...] = jnp.log(across[:, :vecs])
        inverse = jnp.where((lane >= vecs) & (lane < 2 * vecs), inverse, 0.0)
        inverse = inverse + pltpu.roll(inverse, LANES // 2, 1)
        inverse = inverse + pltpu.roll(inverse, LANES // 4, 1)
        high, low = split(
            jnp.concatenate(
                [jnp.where(lane // vecs == k, inverse, 0.0) for k in range(group)], axis=0
            )
        )
        w_ref[...] = jnp.concatenate(
            [
                jnp.concatenate([high, high], axis=1),
                jnp.concatenate([low, jnp.zeros_like(low)], axis=1),
            ],
            axis=0,
        )

    block = vectors_ref.shape[0]
    rows = pl.ds(pl.multiple_of(pl.program_id(0) * block, block), block)
    for k in range(vectors_ref.shape[1] // LANES):
        at = slice(k * LANES, (k + 1) * LANES)
        both = dot(jnp.concatenate(split(stepped_ref[rows, at]), axis=1), w_ref[...], NT)
        vectors_ref[:, at] = both[:, :LANES] + both[:, LANES:]


def vmem():
    return pl.BlockSpec(memory_space=pltpu.VMEM)


def cost(flops, moved):
    return pl.CostEstimate(flops=int(flops), bytes_accessed=int(moved), transcendentals=0)


def body(tangents, base_flow, mode_mask, decay_rates, to_eigen, from_eigen):
    modes, planes, width = tangents.shape
    z_length = base_flow.shape[2]
    vecs = width // z_length
    row_devices, col_devices = lax.axis_size("row"), lax.axis_size("col")
    devices = row_devices * col_devices
    x_count, z_count = modes * row_devices, z_length * col_devices
    tiles = width // LANES
    rows = modes * tiles
    extra = -(-modes * z_length // LANES)
    size = tangents.size * 4
    both = ("col", "row")
    pitch = 8 * (z_count // 8 + 1 - z_count // 8 % 2)
    big = pltpu.CompilerParams(vmem_limit_bytes=40 * 2**20)
    small = pltpu.CompilerParams(vmem_limit_bytes=24 * 2**20)

    order = np.arange(x_count)
    order = (order % row_devices) * modes + order // row_devices
    halves = -(-x_count // LANES)
    points = np.arange(halves * LANES)
    points = np.where(points < x_count, points, points - (halves * LANES - x_count))
    sx_high, sx_low = halves_of_table(synthesis(x_count)[points][:, order].T)
    sx = np.concatenate([sx_high, sx_high, sx_low], axis=0)
    line_tables = parity_tables(z_count)
    gx = np.concatenate(
        halves_of_table(derivative_analysis(x_count, ALPHA_X)[order][:, points]), axis=0
    )

    steps = 1
    base = jnp.transpose(base_flow, (0, 2, 1)).reshape(modes * z_length, planes)
    packed = pl.pallas_call(
        functools.partial(pack_kernel, modes=modes, planes=planes, tiles=tiles, extra=extra),
        out_shape=jax.ShapeDtypeStruct((planes * (rows + extra), LANES), F32),
        in_specs=[vmem()] * 2,
        out_specs=vmem(),
        cost_estimate=cost(10**9, 2 * size),
        compiler_params=small,
        name="pack",
    )(tangents, base)
    received = lax.all_to_all(
        packed.reshape(devices, rows + extra, 1, LANES), both, 0, 0, tiled=True
    ).reshape(packed.shape)

    returned = pl.pallas_call(
        functools.partial(
            transform_kernel, modes=modes, row_devices=row_devices,
            col_devices=col_devices, tiles=tiles, extra=extra, vecs=vecs,
        ),
        out_shape=jax.ShapeDtypeStruct((devices * rows, LANES), F32),
        in_specs=[vmem()] * 7,
        out_specs=vmem(),
        scratch_shapes=[pltpu.VMEM((z_count + 16, halves * LANES), F32)]
        + [pltpu.VMEM((pitch * vecs, LANES), F32)] * (2 * halves),
        cost_estimate=cost(2 * 10**10, 2 * size),
        compiler_params=big,
        name="transform",
    )(received, sx, *line_tables, gx)
    nonlinear = lax.all_to_all(
        returned.reshape(devices, rows, LANES), both, 0, 0, tiled=True
    ).reshape(returned.shape)

    lines = vecs * vecs // (2 * LANES) + 1
    height = modes * planes
    stepped, grams = pl.pallas_call(
        functools.partial(
            column_kernel, modes=modes, planes=planes, tiles=tiles, vecs=vecs,
            step_modes=modes // steps, x_count=x_count, z_count=z_count, z_length=z_length,
        ),
        out_shape=[
            jax.ShapeDtypeStruct((height, width), F32),
            jax.ShapeDtypeStruct((devices * lines, LANES), F32),
        ],
        grid=(steps,),
        in_specs=[vmem()] * 6,
        out_specs=[vmem()] * 2,
        scratch_shapes=[
            pltpu.VMEM((modes, width), F32),
            pltpu.VMEM((modes, width), F32),
            pltpu.VMEM((planes, LANES), F32),
            pltpu.VMEM((LANES, 2 * LANES), F32),
        ],
        cost_estimate=cost(10**10, 3 * size),
        compiler_params=small,
        name="column",
    )(nonlinear, tangents, mode_mask, decay_rates[None, :], to_eigen, from_eigen)
    grams = lax.all_to_all(
        grams.reshape(devices, lines, 1, LANES), both, 0, 0, tiled=True
    ).reshape(grams.shape)

    block = height // 2
    vectors, growth = pl.pallas_call(
        functools.partial(finish_kernel, devices=devices, vecs=vecs, panel=8),
        out_shape=[
            jax.ShapeDtypeStruct((height, width), F32),
            jax.ShapeDtypeStruct((1, vecs), F32),
        ],
        grid=(height // block,),
        in_specs=[vmem()] * 2,
        out_specs=[
            pl.BlockSpec((block, width), lambda i: (i, 0)),
            pl.BlockSpec((1, vecs), lambda i: (0, 0)),
        ],
        scratch_shapes=[pltpu.VMEM((2 * LANES, 2 * LANES), BF16)],
        cost_estimate=cost(2 * height * width * 256, 2 * size),
        compiler_params=small,
        name="finish",
    )(grams, stepped)
    return vectors.reshape(tangents.shape), growth[0]


def solution(mesh):
    placed = (P("row", None, "col"), P("row", None, "col"), P("row", "col"), P(), P(), P())
    return jax.shard_map(
        body, mesh=mesh, in_specs=placed, out_specs=(P("row", None, "col"), P()), check_vma=False
    )
```

```python
import functools

import jax
import jax.numpy as jnp
import numpy as np
from jax import lax
from jax.experimental import pallas as pl
from jax.experimental.pallas import tpu as pltpu
from jax.sharding import PartitionSpec as P

STEP_COEF = 10.0
VISCOSITY = 0.01
ALPHA_X = 0.5
BETA_Z = 1.0
LANES = 128
F32 = jnp.float32
BF16 = jnp.bfloat16
NN = (((1,), (0,)), ((), ()))
NT = (((1,), (1,)), ((), ()))
TN = (((0,), (0,)), ((), ()))


def synthesis(count):
    points = np.arange(count)[:, None]
    modes = np.arange(count)[None, :]
    middle = count // 2
    waves = np.where(modes <= middle, modes, modes - middle)
    angles = (points * waves % count) * (2.0 * np.pi / count)
    return np.where(modes <= middle, np.cos(angles), np.sin(angles))


def analysis(count):
    modes = np.arange(count)
    weights = np.where((modes == 0) | (modes == count // 2), 1.0 / count, 2.0 / count)
    return weights[:, None] * synthesis(count).T


def derivative_analysis(count, scale):
    middle = count // 2
    derivative = np.zeros((count, count))
    for k in range(1, middle):
        derivative[k, middle + k] = k
        derivative[middle + k, k] = -k
    return -scale * (derivative @ analysis(count))


def halves_of_table(table):
    table = np.asarray(table, np.float64)
    high = table.astype(np.float32).astype(jnp.bfloat16)
    low = (table - high.astype(np.float64)).astype(np.float32).astype(jnp.bfloat16)
    return np.stack([high, low])


def split(x):
    high = x.astype(BF16)
    return high, (x - high.astype(F32)).astype(BF16)


def dot(a, b, dims):
    return lax.dot_general(a, b, dims, preferred_element_type=F32)


def dot3(a, b, dims):
    return dot(a[0], b[0], dims) + (dot(a[0], b[1], dims) + dot(a[1], b[0], dims))


def stacked_dot(table, x):
    high, low = split(x)
    return dot(table, jnp.concatenate([high, high], axis=0), NN) + dot(
        table[:, : x.shape[0]], low, NN
    )


def tripled(table):
    high, low = halves_of_table(table)
    return np.concatenate([high, low, high], axis=1)


def table_dot(table_ref, high, low):
    return dot(table_ref[...], jnp.concatenate([high, high, low], axis=0), NN)


def parity_tables(count):
    middle = count // 2
    wide, tall = middle + 16, middle + 8
    to_points, to_modes = synthesis(count), analysis(count)
    weights = np.where(np.arange(middle + 1) % middle == 0, 1.0, 2.0)
    even_points = np.zeros((wide, wide))
    even_points[: middle + 1, : middle + 1] = to_points[: middle + 1, : middle + 1]
    odd_points = np.zeros((middle, middle))
    odd_points[1:, 1:] = to_points[1:middle, middle + 1 :]
    even_modes = np.zeros((tall, wide))
    even_modes[: middle + 1, : middle + 1] = to_modes[: middle + 1, : middle + 1] * weights
    odd_modes = np.zeros((middle, middle))
    odd_modes[1:, 1:] = 2.0 * to_modes[middle + 1 :, 1:middle]
    return [tripled(t) for t in (even_points, odd_points, even_modes, odd_modes)]


def to_parity_points(even_ref, odd_ref, x):
    high, low = split(x)
    wide, middle = even_ref.shape[0], odd_ref.shape[0]
    return (
        table_dot(even_ref, high[:wide], low[:wide]),
        table_dot(odd_ref, high[middle:], low[middle:]),
    )


def pack_kernel(base_ref, *refs, modes, planes, tiles, extra):
    q_refs, out_ref = refs[:-1], refs[-1]
    share = modes // len(q_refs)
    stride = modes * tiles + extra
    part = base_ref.shape[0] // extra
    fill = jnp.zeros((LANES - part, planes), F32)
    for k in range(extra):
        block = jnp.concatenate([base_ref[k * part : (k + 1) * part, :], fill], axis=0)
        out_ref[pl.ds(modes * tiles + k, planes, stride=stride), :] = block.T
    for m in range(modes):
        for nb in range(tiles):
            out_ref[pl.ds(nb * modes + m, planes, stride=stride), :] = q_refs[m // share][
                m % share, :, nb * LANES : (nb + 1) * LANES
            ]


def transform_kernel(
    d_ref, sx_ref, even_p_ref, odd_p_ref, even_m_ref, odd_m_ref, g_ref, out_ref, speed_ref,
    *scratch,
    modes, row_devices, col_devices, tiles, extra, vecs,
):
    halves = len(scratch) // 2
    y_refs, z_refs = scratch[:halves], scratch[halves:]
    rows = modes * tiles
    stride = rows + extra
    x_count = modes * row_devices
    wide, tall, middle = even_p_ref.shape[0], even_m_ref.shape[0], odd_p_ref.shape[0]
    z_count = 2 * middle
    z_length = z_count // col_devices
    pitch = y_refs[0].shape[0] // vecs
    per_tile = LANES // vecs

    turned = []
    for k in range(extra):
        block = d_ref[pl.ds(rows + k, row_devices * col_devices, stride=stride), :]
        turned.append(block.T)
    slot = lax.broadcasted_iota(jnp.int32, (z_length, LANES), 1) // row_devices
    slots = LANES // row_devices
    share = modes // extra
    sheets = []
    for c in range(col_devices):
        parts = [jnp.zeros((z_length, LANES), F32) for _ in range(halves)]
        for m in range(modes):
            piece = turned[m // share][(m % share) * z_length : (m % share + 1) * z_length]
            shift = ((m % slots - c) * row_devices) % LANES
            piece = pltpu.roll(piece, shift, 1) if shift else piece
            parts[m // slots] = jnp.where(slot == m % slots, piece, parts[m // slots])
        sheets.append(jnp.concatenate(parts, axis=1))
    base = jnp.concatenate(sheets, axis=0)[:, :x_count]
    sx = (sx_ref[:x_count], sx_ref[2 * x_count :])
    even, odd = to_parity_points(even_p_ref, odd_p_ref, dot3(split(base), sx, NN))
    speed_ref[:wide] = even
    speed_ref[wide:] = odd

    def forward_x(c, carry):
        parts = []
        for nb in range(tiles):
            start = c * (row_devices * stride) + nb * modes
            block = jnp.concatenate(
                [d_ref[pl.ds(start + m, row_devices, stride=stride), :] for m in range(modes)],
                axis=0,
            )
            block = jnp.concatenate(split(block), axis=0).T
            parts.append(jnp.concatenate([block, block[:, :x_count]], axis=1))
        mixed = dot(jnp.concatenate(parts, axis=0), sx_ref[...], NN)
        for n in range(z_length):
            for k, y_ref in enumerate(y_refs):
                y_ref[pl.ds(c * z_length + n, vecs, stride=pitch), :] = mixed[
                    n * vecs : (n + 1) * vecs, k * LANES : (k + 1) * LANES
                ]
        return carry

    lax.fori_loop(0, col_devices, forward_x, 0, unroll=8)

    y_low, y_high = y_refs
    z_low, z_high = z_refs
    first = lax.broadcasted_iota(jnp.int32, (z_count, LANES), 1) < LANES // 2
    batch = 8

    def plane(i, carry):
        ats = [
            pl.ds(pl.multiple_of((i * batch + j) * pitch, 8), z_count) for j in range(batch)
        ]
        mixed = jnp.concatenate(
            [y_low[at, :] for at in ats]
            + [
                jnp.where(first, y_high[ats[j], :], y_high[ats[j + 1], :])
                for j in range(0, batch, 2)
            ],
            axis=1,
        )
        speed = jnp.concatenate(
            [speed_ref[:, :LANES]] * batch + [speed_ref[:, LANES:]] * (batch // 2), axis=1
        )
        even, odd = to_parity_points(even_p_ref, odd_p_ref, mixed)
        even_speed, odd_speed = speed[:wide], speed[wide:]
        cross = even[:middle] * odd_speed + odd * even_speed[:middle]
        even = even * even_speed
        even = jnp.concatenate([even[:middle] + odd * odd_speed, even[middle:]], axis=0)
        even = table_dot(even_m_ref, *split(even))
        odd = table_dot(odd_m_ref, *split(cross))
        mixed = jnp.concatenate(
            [
                even[:middle],
                even[middle:] + odd[: tall - middle],
                odd[tall - middle :],
            ],
            axis=0,
        )
        for j, at in enumerate(ats):
            k = batch + j // 2
            z_low[at, :] = mixed[:, j * LANES : (j + 1) * LANES]
            z_high[at, :] = mixed[:, k * LANES : (k + 1) * LANES]
        return carry

    lax.fori_loop(0, vecs // batch, plane, 0, unroll=4)

    rows_of = lax.broadcasted_iota(jnp.int32, (vecs, LANES), 0)
    lanes_of = lax.broadcasted_iota(jnp.int32, (vecs, LANES), 1)
    mine = (rows_of % 2) == (lanes_of // (LANES // 2))

    def inverse_x(c, carry):
        block = jnp.concatenate(
            [
                jnp.concatenate(
                    [
                        z_low[pl.ds(c * z_length + n, vecs, stride=pitch), :],
                        jnp.where(
                            mine, z_high[pl.ds(c * z_length + n, vecs, stride=pitch), :], 0.0
                        ),
                    ],
                    axis=1,
                )
                for n in range(z_length)
            ],
            axis=0,
        )
        high, low = split(block)
        both = dot(g_ref[...], high, NT)
        back = both[:x_count] + (both[x_count:] + dot(g_ref[:x_count], low, NT))
        for nb in range(tiles):
            start = c * (row_devices * rows) + nb * modes
            for m in range(modes):
                out_ref[pl.ds(start + m, row_devices, stride=rows), :] = back[
                    m * row_devices : (m + 1) * row_devices, nb * LANES : (nb + 1) * LANES
                ]
        return carry

    lax.fori_loop(0, col_devices, inverse_x, 0, unroll=8)


def column_kernel(
    nl_ref, q_ref, mask_ref, decay_ref, to_ref, from_ref, stepped_ref, gram_ref,
    mask_s, wave_s, decay_s, gram_s,
    *, modes, planes, tiles, vecs, step_modes, x_count, z_count, z_length,
):
    width = tiles * LANES

    @pl.when(pl.program_id(0) == 0)
    def _():
        lane = lax.broadcasted_iota(jnp.int32, (z_length, width), 1) // vecs
        row = lax.broadcasted_iota(jnp.int32, (z_length, width), 0)
        spread = jnp.where(lane == row, 1.0, 0.0).astype(BF16)
        mask_s[...] = dot(mask_ref[...].astype(F32).astype(BF16), spread, NN)
        n = lax.broadcasted_iota(jnp.int32, (modes, width), 1) // vecs
        n = n + lax.axis_index("col") * z_length
        m = lax.broadcasted_iota(jnp.int32, (modes, width), 0)
        m = m + lax.axis_index("row") * modes
        wave_x = jnp.where(m <= x_count // 2, m, m - x_count // 2).astype(F32) * ALPHA_X
        wave_z = jnp.where(n <= z_count // 2, n, n - z_count // 2).astype(F32) * BETA_Z
        wave_s[...] = STEP_COEF + VISCOSITY * (wave_x * wave_x + wave_z * wave_z)
        decay_s[...] = jnp.broadcast_to(decay_ref[...], (LANES, planes)).T
        gram_s[...] = jnp.zeros_like(gram_s)

    to_eigen = jnp.concatenate(split(to_ref[...]), axis=1)
    from_eigen = jnp.concatenate(split(from_ref[...]), axis=1)
    decay = jnp.concatenate([decay_s[...]] * tiles, axis=1)
    gram = gram_s[...]
    for k in range(step_modes):
        m = pl.program_id(0) * step_modes + k
        nonlinear = jnp.concatenate(
            [
                nl_ref[pl.ds(nb * modes + m, planes, stride=tiles * modes), :]
                for nb in range(tiles)
            ],
            axis=1,
        )
        right = STEP_COEF * q_ref[m] + nonlinear * mask_s[pl.ds(m, 1), :]
        eigen = stacked_dot(to_eigen, right)
        eigen = eigen / (wave_s[pl.ds(m, 1), :] + decay)
        stepped = stacked_dot(from_eigen, eigen)
        stepped_ref[pl.ds(pl.multiple_of(m * planes, planes), planes), :] = stepped
        columns = [stepped[:, nb * LANES : (nb + 1) * LANES] for nb in range(tiles)]
        left = jnp.concatenate([x.T.astype(BF16) for x in columns], axis=1)
        right = jnp.concatenate(
            [jnp.concatenate(split(x), axis=1) for x in columns], axis=0
        )
        gram = gram + dot(left, right, NN)
    gram_s[...] = gram

    @pl.when(pl.program_id(0) == pl.num_programs(0) - 1)
    def _():
        high, cross = gram[:, :LANES], gram[:, LANES:]
        full = (high + (cross + cross.T)) * (1.0 / (x_count * planes * z_count))
        group = LANES // vecs
        lane = lax.broadcasted_iota(jnp.int32, (vecs, LANES), 1) // vecs
        folded = jnp.zeros((vecs, LANES), F32)
        for k in range(group):
            folded = folded + jnp.where(lane == k, full[k * vecs : (k + 1) * vecs], 0.0)
        folded = folded + pltpu.roll(folded, LANES // 2, 1)
        folded = folded + pltpu.roll(folded, LANES // 4, 1)
        half = vecs // 2
        lane = lax.broadcasted_iota(jnp.int32, (half, LANES), 1)
        row = lax.broadcasted_iota(jnp.int32, (half, LANES), 0)
        top, shifted = folded[:half], pltpu.roll(folded[half:], LANES - half, 1)
        square = jnp.where((lane % vecs < half) & (lane % vecs < row), shifted, top)
        piece = half // group
        spread = lane[:piece] // vecs
        packed = jnp.zeros((piece, LANES), F32)
        for k in range(group):
            packed = jnp.where(spread == k, square[k * piece : (k + 1) * piece], packed)
        diagonal = jnp.sum(jnp.where(lane % vecs == row, shifted, 0.0), axis=0, keepdims=True)
        sent = [packed[k : k + 1] for k in range(piece)] + [diagonal]
        for k, line in enumerate(sent):
            gram_ref[pl.ds(k, planes, stride=len(sent)), :] = jnp.broadcast_to(
                line, (planes, LANES)
            )


def finish_kernel(grams_ref, stepped_ref, vectors_ref, growth_ref, w_ref, *, devices, vecs, panel):
    group = LANES // vecs
    half = vecs // 2
    piece = half // group

    @pl.when(pl.program_id(0) == 0)
    def _():
        lines = [
            jnp.sum(
                grams_ref[pl.ds(k, devices, stride=piece + 1), :], axis=0, keepdims=True
            )
            for k in range(piece + 1)
        ]
        packed = jnp.concatenate(lines[:piece], axis=0)
        square = jnp.concatenate(
            [pltpu.roll(packed, (LANES - k * vecs) % LANES, 1) for k in range(group)], axis=0
        )
        turned = jnp.concatenate([square, jnp.zeros((LANES - half, LANES), F32)], axis=0).T
        lane = lax.broadcasted_iota(jnp.int32, (half, LANES), 1)
        row = lax.broadcasted_iota(jnp.int32, (half, LANES), 0)
        top = jnp.where((lane < half) & (lane < row), turned[:half], square)
        right = jnp.where(lane < row, square, jnp.where(lane == row, lines[piece], turned[:half]))
        bottom = jnp.where(lane < half, turned[half:vecs], pltpu.roll(right, half, 1))
        gram = jnp.concatenate([top, bottom], axis=0)
        lane = lax.broadcasted_iota(jnp.int32, (vecs, LANES), 1)
        row = lax.broadcasted_iota(jnp.int32, (vecs, LANES), 0)
        work = jnp.where(lane < vecs, gram, jnp.where(lane == row + vecs, 1.0, 0.0))
        for first in range(0, vecs, panel):
            own = range(first, first + panel)
            columns = [jnp.broadcast_to(work[:, k : k + 1], (vecs, LANES)) for k in own]
            lines = [work[k : k + 1, :] for k in own]
            for j, k in enumerate(own):
                pivot = columns[j][k : k + 1]
                column = jnp.where(row > k, columns[j], 0.0)
                scaled = lines[j] / pivot
                for i in range(j + 1, panel):
                    columns[i] = columns[i] - column * (columns[i][k : k + 1] / pivot)
                    lines[i] = lines[i] - columns[j][first + i : first + i + 1] * scaled
                work = work - column * scaled
        pivots = jnp.sum(jnp.where(lane == row, work, 0.0), axis=1, keepdims=True)
        diagonal = jnp.sqrt(pivots)
        inverse = work / diagonal
        across = jnp.sum(jnp.where(lane == row, diagonal, 0.0), axis=0, keepdims=True)
        growth_ref[...] = jnp.log(across[:, :vecs])
        inverse = jnp.where((lane >= vecs) & (lane < 2 * vecs), inverse, 0.0)
        inverse = inverse + pltpu.roll(inverse, LANES // 2, 1)
        inverse = inverse + pltpu.roll(inverse, LANES // 4, 1)
        high, low = split(
            jnp.concatenate(
                [jnp.where(lane // vecs == k, inverse, 0.0) for k in range(group)], axis=0
            )
        )
        w_ref[...] = jnp.concatenate(
            [
                jnp.concatenate([high, high], axis=1),
                jnp.concatenate([low, jnp.zeros_like(low)], axis=1),
            ],
            axis=0,
        )

    block = vectors_ref.shape[0]
    rows = pl.ds(pl.multiple_of(pl.program_id(0) * block, block), block)
    for k in range(vectors_ref.shape[1] // LANES):
        at = slice(k * LANES, (k + 1) * LANES)
        both = dot(jnp.concatenate(split(stepped_ref[rows, at]), axis=1), w_ref[...], NT)
        vectors_ref[:, at] = both[:, :LANES] + both[:, LANES:]


def vmem():
    return pl.BlockSpec(memory_space=pltpu.VMEM)


def cost(flops, moved):
    return pl.CostEstimate(flops=int(flops), bytes_accessed=int(moved), transcendentals=0)


def body(tangents, base_flow, mode_mask, decay_rates, to_eigen, from_eigen):
    modes, planes, width = tangents.shape
    z_length = base_flow.shape[2]
    vecs = width // z_length
    row_devices, col_devices = lax.axis_size("row"), lax.axis_size("col")
    devices = row_devices * col_devices
    x_count, z_count = modes * row_devices, z_length * col_devices
    tiles = width // LANES
    rows = modes * tiles
    extra = -(-modes * z_length // LANES)
    size = tangents.size * 4
    both = ("col", "row")
    pitch = 8 * (z_count // 8 + 1 - z_count // 8 % 2)
    big = pltpu.CompilerParams(vmem_limit_bytes=40 * 2**20)
    small = pltpu.CompilerParams(vmem_limit_bytes=24 * 2**20)

    order = np.arange(x_count)
    order = (order % row_devices) * modes + order // row_devices
    halves = -(-x_count // LANES)
    points = np.arange(halves * LANES)
    points = np.where(points < x_count, points, points - (halves * LANES - x_count))
    sx_high, sx_low = halves_of_table(synthesis(x_count)[points][:, order].T)
    sx = np.concatenate([sx_high, sx_high, sx_low], axis=0)
    line_tables = parity_tables(z_count)
    gx = np.concatenate(
        halves_of_table(derivative_analysis(x_count, ALPHA_X)[order][:, points]), axis=0
    )

    steps = 1
    base = jnp.transpose(base_flow, (0, 2, 1)).reshape(modes * z_length, planes)
    packed = pl.pallas_call(
        functools.partial(pack_kernel, modes=modes, planes=planes, tiles=tiles, extra=extra),
        out_shape=jax.ShapeDtypeStruct((planes * (rows + extra), LANES), F32),
        in_specs=[vmem()] * 3,
        out_specs=vmem(),
        cost_estimate=cost(10**9, 2 * size),
        compiler_params=small,
        name="pack",
    )(base, tangents[: modes // 2], tangents[modes // 2 :])
    received = lax.all_to_all(
        packed.reshape(devices, rows + extra, 1, LANES), both, 0, 0, tiled=True
    ).reshape(packed.shape)

    returned = pl.pallas_call(
        functools.partial(
            transform_kernel, modes=modes, row_devices=row_devices,
            col_devices=col_devices, tiles=tiles, extra=extra, vecs=vecs,
        ),
        out_shape=jax.ShapeDtypeStruct((devices * rows, LANES), F32),
        in_specs=[vmem()] * 7,
        out_specs=vmem(),
        scratch_shapes=[pltpu.VMEM((z_count + 16, halves * LANES), F32)]
        + [pltpu.VMEM((pitch * vecs, LANES), F32)] * (2 * halves),
        cost_estimate=cost(2 * 10**10, 2 * size),
        compiler_params=big,
        name="transform",
    )(received, sx, *line_tables, gx)
    nonlinear = lax.all_to_all(
        returned.reshape(devices, rows, LANES), both, 0, 0, tiled=True
    ).reshape(returned.shape)

    lines = vecs * vecs // (2 * LANES) + 1
    height = modes * planes
    stepped, grams = pl.pallas_call(
        functools.partial(
            column_kernel, modes=modes, planes=planes, tiles=tiles, vecs=vecs,
            step_modes=modes // steps, x_count=x_count, z_count=z_count, z_length=z_length,
        ),
        out_shape=[
            jax.ShapeDtypeStruct((height, width), F32),
            jax.ShapeDtypeStruct((devices * lines, LANES), F32),
        ],
        grid=(steps,),
        in_specs=[vmem()] * 6,
        out_specs=[vmem()] * 2,
        scratch_shapes=[
            pltpu.VMEM((modes, width), F32),
            pltpu.VMEM((modes, width), F32),
            pltpu.VMEM((planes, LANES), F32),
            pltpu.VMEM((LANES, 2 * LANES), F32),
        ],
        cost_estimate=cost(10**10, 3 * size),
        compiler_params=small,
        name="column",
    )(nonlinear, tangents, mode_mask, decay_rates[None, :], to_eigen, from_eigen)
    grams = lax.all_to_all(
        grams.reshape(devices, lines, 1, LANES), both, 0, 0, tiled=True
    ).reshape(grams.shape)

    block = height // 2
    vectors, growth = pl.pallas_call(
        functools.partial(finish_kernel, devices=devices, vecs=vecs, panel=8),
        out_shape=[
            jax.ShapeDtypeStruct((height, width), F32),
            jax.ShapeDtypeStruct((1, vecs), F32),
        ],
        grid=(height // block,),
        in_specs=[vmem()] * 2,
        out_specs=[
            pl.BlockSpec((block, width), lambda i: (i, 0)),
            pl.BlockSpec((1, vecs), lambda i: (0, 0)),
        ],
        scratch_shapes=[pltpu.VMEM((2 * LANES, 2 * LANES), BF16)],
        cost_estimate=cost(2 * height * width * 256, 2 * size),
        compiler_params=small,
        name="finish",
    )(grams, stepped)
    return vectors.reshape(tangents.shape), growth[0]


def solution(mesh):
    placed = (P("row", None, "col"), P("row", None, "col"), P("row", "col"), P(), P(), P())
    return jax.shard_map(
        body, mesh=mesh, in_specs=placed, out_specs=(P("row", None, "col"), P()), check_vma=False
    )
```

```python
import functools

import jax
import jax.numpy as jnp
import numpy as np
from jax import lax
from jax.experimental import pallas as pl
from jax.experimental.pallas import tpu as pltpu
from jax.sharding import PartitionSpec as P

STEP_COEF = 10.0
VISCOSITY = 0.01
ALPHA_X = 0.5
BETA_Z = 1.0
LANES = 128
F32 = jnp.float32
BF16 = jnp.bfloat16
NN = (((1,), (0,)), ((), ()))
NT = (((1,), (1,)), ((), ()))
TN = (((0,), (0,)), ((), ()))


def synthesis(count):
    points = np.arange(count)[:, None]
    modes = np.arange(count)[None, :]
    middle = count // 2
    waves = np.where(modes <= middle, modes, modes - middle)
    angles = (points * waves % count) * (2.0 * np.pi / count)
    return np.where(modes <= middle, np.cos(angles), np.sin(angles))


def analysis(count):
    modes = np.arange(count)
    weights = np.where((modes == 0) | (modes == count // 2), 1.0 / count, 2.0 / count)
    return weights[:, None] * synthesis(count).T


def derivative_analysis(count, scale):
    middle = count // 2
    derivative = np.zeros((count, count))
    for k in range(1, middle):
        derivative[k, middle + k] = k
        derivative[middle + k, k] = -k
    return -scale * (derivative @ analysis(count))


def halves_of_table(table):
    table = np.asarray(table, np.float64)
    high = table.astype(np.float32).astype(jnp.bfloat16)
    low = (table - high.astype(np.float64)).astype(np.float32).astype(jnp.bfloat16)
    return np.stack([high, low])


def split(x):
    high = x.astype(BF16)
    return high, (x - high.astype(F32)).astype(BF16)


def dot(a, b, dims):
    return lax.dot_general(a, b, dims, preferred_element_type=F32)


def dot3(a, b, dims):
    return dot(a[0], b[0], dims) + (dot(a[0], b[1], dims) + dot(a[1], b[0], dims))


def stacked_dot(table, x):
    high, low = split(x)
    return dot(table, jnp.concatenate([high, high], axis=0), NN) + dot(
        table[:, : x.shape[0]], low, NN
    )


def tripled(table):
    high, low = halves_of_table(table)
    return np.concatenate([high, low, high], axis=1)


def table_dot(table_ref, high, low):
    return dot(table_ref[...], jnp.concatenate([high, high, low], axis=0), NN)


def parity_tables(count):
    middle = count // 2
    wide, tall = middle + 16, middle + 8
    to_points, to_modes = synthesis(count), analysis(count)
    weights = np.where(np.arange(middle + 1) % middle == 0, 1.0, 2.0)
    even_points = np.zeros((wide, wide))
    even_points[: middle + 1, : middle + 1] = to_points[: middle + 1, : middle + 1]
    odd_points = np.zeros((middle, middle))
    odd_points[1:, 1:] = to_points[1:middle, middle + 1 :]
    even_modes = np.zeros((tall, wide))
    even_modes[: middle + 1, : middle + 1] = to_modes[: middle + 1, : middle + 1] * weights
    odd_modes = np.zeros((middle, middle))
    odd_modes[1:, 1:] = 2.0 * to_modes[middle + 1 :, 1:middle]
    return [tripled(t) for t in (even_points, odd_points, even_modes, odd_modes)]


def to_parity_points(even_ref, odd_ref, x):
    high, low = split(x)
    wide, middle = even_ref.shape[0], odd_ref.shape[0]
    return (
        table_dot(even_ref, high[:wide], low[:wide]),
        table_dot(odd_ref, high[middle:], low[middle:]),
    )


def pack_kernel(base_ref, *refs, modes, planes, tiles, extra):
    q_refs, out_ref = refs[:-1], refs[-1]
    share = modes // len(q_refs)
    stride = modes * tiles + extra
    part = base_ref.shape[0] // extra
    fill = jnp.zeros((LANES - part, planes), F32)
    for k in range(extra):
        block = jnp.concatenate([base_ref[k * part : (k + 1) * part, :], fill], axis=0)
        out_ref[pl.ds(modes * tiles + k, planes, stride=stride), :] = block.T
    for m in range(modes):
        for nb in range(tiles):
            out_ref[pl.ds(nb * modes + m, planes, stride=stride), :] = q_refs[m // share][
                m % share, :, nb * LANES : (nb + 1) * LANES
            ]


def transform_kernel(
    d_ref, sx_ref, even_p_ref, odd_p_ref, even_m_ref, odd_m_ref, g_ref, out_ref, speed_ref,
    *scratch,
    modes, row_devices, col_devices, tiles, extra, vecs,
):
    halves = len(scratch) // 2
    y_refs, z_refs = scratch[:halves], scratch[halves:]
    rows = modes * tiles
    stride = rows + extra
    x_count = modes * row_devices
    wide, tall, middle = even_p_ref.shape[0], even_m_ref.shape[0], odd_p_ref.shape[0]
    z_count = 2 * middle
    z_length = z_count // col_devices
    pitch = y_refs[0].shape[0] // vecs
    per_tile = LANES // vecs

    turned = []
    for k in range(extra):
        block = d_ref[pl.ds(rows + k, row_devices * col_devices, stride=stride), :]
        turned.append(block.T)
    slot = lax.broadcasted_iota(jnp.int32, (z_length, LANES), 1) // row_devices
    slots = LANES // row_devices
    share = modes // extra
    sheets = []
    for c in range(col_devices):
        parts = [jnp.zeros((z_length, LANES), F32) for _ in range(halves)]
        for m in range(modes):
            piece = turned[m // share][(m % share) * z_length : (m % share + 1) * z_length]
            shift = ((m % slots - c) * row_devices) % LANES
            piece = pltpu.roll(piece, shift, 1) if shift else piece
            parts[m // slots] = jnp.where(slot == m % slots, piece, parts[m // slots])
        sheets.append(jnp.concatenate(parts, axis=1))
    base = jnp.concatenate(sheets, axis=0)[:, :x_count]
    sx = (sx_ref[:x_count], sx_ref[2 * x_count :])
    even, odd = to_parity_points(even_p_ref, odd_p_ref, dot3(split(base), sx, NN))
    speed_ref[:wide] = even
    speed_ref[wide:] = odd

    def forward_x(c, carry):
        parts = []
        for nb in range(tiles):
            start = c * (row_devices * stride) + nb * modes
            block = jnp.concatenate(
                [d_ref[pl.ds(start + m, row_devices, stride=stride), :] for m in range(modes)],
                axis=0,
            )
            block = jnp.concatenate(split(block), axis=0).T
            parts.append(jnp.concatenate([block, block[:, :x_count]], axis=1))
        mixed = dot(jnp.concatenate(parts, axis=0), sx_ref[...], NN)
        for n in range(z_length):
            for k, y_ref in enumerate(y_refs):
                y_ref[pl.ds(c * z_length + n, vecs, stride=pitch), :] = mixed[
                    n * vecs : (n + 1) * vecs, k * LANES : (k + 1) * LANES
                ]
        return carry

    lax.fori_loop(0, col_devices, forward_x, 0, unroll=8)

    y_low, y_high = y_refs
    z_low, z_high = z_refs
    first = lax.broadcasted_iota(jnp.int32, (z_count, LANES), 1) < LANES // 2
    batch = 8

    def plane(i, carry):
        ats = [
            pl.ds(pl.multiple_of((i * batch + j) * pitch, 8), z_count) for j in range(batch)
        ]
        mixed = jnp.concatenate(
            [y_low[at, :] for at in ats]
            + [
                jnp.where(first, y_high[ats[j], :], y_high[ats[j + 1], :])
                for j in range(0, batch, 2)
            ],
            axis=1,
        )
        speed = jnp.concatenate(
            [speed_ref[:, :LANES]] * batch + [speed_ref[:, LANES:]] * (batch // 2), axis=1
        )
        even, odd = to_parity_points(even_p_ref, odd_p_ref, mixed)
        even_speed, odd_speed = speed[:wide], speed[wide:]
        cross = even[:middle] * odd_speed + odd * even_speed[:middle]
        even = even * even_speed
        even = jnp.concatenate([even[:middle] + odd * odd_speed, even[middle:]], axis=0)
        even = table_dot(even_m_ref, *split(even))
        odd = table_dot(odd_m_ref, *split(cross))
        mixed = jnp.concatenate(
            [
                even[:middle],
                even[middle:] + odd[: tall - middle],
                odd[tall - middle :],
            ],
            axis=0,
        )
        for j, at in enumerate(ats):
            k = batch + j // 2
            z_low[at, :] = mixed[:, j * LANES : (j + 1) * LANES]
            z_high[at, :] = mixed[:, k * LANES : (k + 1) * LANES]
        return carry

    lax.fori_loop(0, vecs // batch, plane, 0, unroll=4)

    rows_of = lax.broadcasted_iota(jnp.int32, (vecs, LANES), 0)
    lanes_of = lax.broadcasted_iota(jnp.int32, (vecs, LANES), 1)
    mine = (rows_of % 2) == (lanes_of // (LANES // 2))

    def inverse_x(c, carry):
        block = jnp.concatenate(
            [
                jnp.concatenate(
                    [
                        z_low[pl.ds(c * z_length + n, vecs, stride=pitch), :],
                        jnp.where(
                            mine, z_high[pl.ds(c * z_length + n, vecs, stride=pitch), :], 0.0
                        ),
                    ],
                    axis=1,
                )
                for n in range(z_length)
            ],
            axis=0,
        )
        high, low = split(block)
        both = dot(g_ref[...], high, NT)
        back = both[:x_count] + (both[x_count:] + dot(g_ref[:x_count], low, NT))
        for nb in range(tiles):
            start = c * (row_devices * rows) + nb * modes
            for m in range(modes):
                out_ref[pl.ds(start + m, row_devices, stride=rows), :] = back[
                    m * row_devices : (m + 1) * row_devices, nb * LANES : (nb + 1) * LANES
                ]
        return carry

    lax.fori_loop(0, col_devices, inverse_x, 0, unroll=8)


def column_kernel(
    nl_ref, q_ref, mask_ref, decay_ref, to_ref, from_ref, stepped_ref, gram_ref,
    mask_s, wave_s, decay_s, gram_s,
    *, modes, planes, tiles, vecs, step_modes, x_count, z_count, z_length,
):
    width = tiles * LANES

    @pl.when(pl.program_id(0) == 0)
    def _():
        lane = lax.broadcasted_iota(jnp.int32, (z_length, width), 1) // vecs
        row = lax.broadcasted_iota(jnp.int32, (z_length, width), 0)
        spread = jnp.where(lane == row, 1.0, 0.0).astype(BF16)
        mask_s[...] = dot(mask_ref[...].astype(F32).astype(BF16), spread, NN)
        n = lax.broadcasted_iota(jnp.int32, (modes, width), 1) // vecs
        n = n + lax.axis_index("col") * z_length
        m = lax.broadcasted_iota(jnp.int32, (modes, width), 0)
        m = m + lax.axis_index("row") * modes
        wave_x = jnp.where(m <= x_count // 2, m, m - x_count // 2).astype(F32) * ALPHA_X
        wave_z = jnp.where(n <= z_count // 2, n, n - z_count // 2).astype(F32) * BETA_Z
        wave_s[...] = STEP_COEF + VISCOSITY * (wave_x * wave_x + wave_z * wave_z)
        decay_s[...] = jnp.broadcast_to(decay_ref[...], (LANES, planes)).T
        gram_s[...] = jnp.zeros_like(gram_s)

    to_eigen = jnp.concatenate(split(to_ref[...]), axis=1)
    from_eigen = jnp.concatenate(split(from_ref[...]), axis=1)
    decay = jnp.concatenate([decay_s[...]] * tiles, axis=1)
    gram = gram_s[...]
    for k in range(step_modes):
        m = pl.program_id(0) * step_modes + k
        nonlinear = jnp.concatenate(
            [
                nl_ref[pl.ds(nb * modes + m, planes, stride=tiles * modes), :]
                for nb in range(tiles)
            ],
            axis=1,
        )
        right = STEP_COEF * q_ref[m] + nonlinear * mask_s[pl.ds(m, 1), :]
        eigen = stacked_dot(to_eigen, right)
        eigen = eigen / (wave_s[pl.ds(m, 1), :] + decay)
        stepped = stacked_dot(from_eigen, eigen)
        stepped_ref[pl.ds(pl.multiple_of(m * planes, planes), planes), :] = stepped
        columns = [stepped[:, nb * LANES : (nb + 1) * LANES] for nb in range(tiles)]
        left = jnp.concatenate([x.T.astype(BF16) for x in columns], axis=1)
        right = jnp.concatenate(
            [jnp.concatenate(split(x), axis=1) for x in columns], axis=0
        )
        gram = gram + dot(left, right, NN)
    gram_s[...] = gram

    @pl.when(pl.program_id(0) == pl.num_programs(0) - 1)
    def _():
        high, cross = gram[:, :LANES], gram[:, LANES:]
        full = (high + (cross + cross.T)) * (1.0 / (x_count * planes * z_count))
        group = LANES // vecs
        lane = lax.broadcasted_iota(jnp.int32, (vecs, LANES), 1) // vecs
        folded = jnp.zeros((vecs, LANES), F32)
        for k in range(group):
            folded = folded + jnp.where(lane == k, full[k * vecs : (k + 1) * vecs], 0.0)
        folded = folded + pltpu.roll(folded, LANES // 2, 1)
        folded = folded + pltpu.roll(folded, LANES // 4, 1)
        half = vecs // 2
        lane = lax.broadcasted_iota(jnp.int32, (half, LANES), 1)
        row = lax.broadcasted_iota(jnp.int32, (half, LANES), 0)
        top, shifted = folded[:half], pltpu.roll(folded[half:], LANES - half, 1)
        square = jnp.where((lane % vecs < half) & (lane % vecs < row), shifted, top)
        piece = half // group
        spread = lane[:piece] // vecs
        packed = jnp.zeros((piece, LANES), F32)
        for k in range(group):
            packed = jnp.where(spread == k, square[k * piece : (k + 1) * piece], packed)
        diagonal = jnp.sum(jnp.where(lane % vecs == row, shifted, 0.0), axis=0, keepdims=True)
        sent = [packed[k : k + 1] for k in range(piece)] + [diagonal]
        for k, line in enumerate(sent):
            gram_ref[pl.ds(k, planes, stride=len(sent)), :] = jnp.broadcast_to(
                line, (planes, LANES)
            )


def finish_kernel(grams_ref, stepped_ref, vectors_ref, growth_ref, w_ref, *, devices, vecs, panel):
    group = LANES // vecs
    half = vecs // 2
    piece = half // group

    @pl.when(pl.program_id(0) == 0)
    def _():
        lines = [
            jnp.sum(
                grams_ref[pl.ds(k, devices, stride=piece + 1), :], axis=0, keepdims=True
            )
            for k in range(piece + 1)
        ]
        packed = jnp.concatenate(lines[:piece], axis=0)
        square = jnp.concatenate(
            [pltpu.roll(packed, (LANES - k * vecs) % LANES, 1) for k in range(group)], axis=0
        )
        turned = jnp.concatenate([square, jnp.zeros((LANES - half, LANES), F32)], axis=0).T
        lane = lax.broadcasted_iota(jnp.int32, (half, LANES), 1)
        row = lax.broadcasted_iota(jnp.int32, (half, LANES), 0)
        top = jnp.where((lane < half) & (lane < row), turned[:half], square)
        right = jnp.where(lane < row, square, jnp.where(lane == row, lines[piece], turned[:half]))
        bottom = jnp.where(lane < half, turned[half:vecs], pltpu.roll(right, half, 1))
        gram = jnp.concatenate([top, bottom], axis=0)
        lane = lax.broadcasted_iota(jnp.int32, (vecs, LANES), 1)
        row = lax.broadcasted_iota(jnp.int32, (vecs, LANES), 0)
        work = jnp.where(lane < vecs, gram, jnp.where(lane == row + vecs, 1.0, 0.0))
        for first in range(0, vecs, panel):
            own = range(first, first + panel)
            columns = [jnp.broadcast_to(work[:, k : k + 1], (vecs, LANES)) for k in own]
            lines = [work[k : k + 1, :] for k in own]
            for j, k in enumerate(own):
                pivot = columns[j][k : k + 1]
                column = jnp.where(row > k, columns[j], 0.0)
                scaled = lines[j] / pivot
                for i in range(j + 1, panel):
                    columns[i] = columns[i] - column * (columns[i][k : k + 1] / pivot)
                    lines[i] = lines[i] - columns[j][first + i : first + i + 1] * scaled
                work = work - column * scaled
        pivots = jnp.sum(jnp.where(lane == row, work, 0.0), axis=1, keepdims=True)
        diagonal = jnp.sqrt(pivots)
        inverse = work / diagonal
        across = jnp.sum(jnp.where(lane == row, diagonal, 0.0), axis=0, keepdims=True)
        growth_ref[...] = jnp.log(across[:, :vecs])
        inverse = jnp.where((lane >= vecs) & (lane < 2 * vecs), inverse, 0.0)
        inverse = inverse + pltpu.roll(inverse, LANES // 2, 1)
        inverse = inverse + pltpu.roll(inverse, LANES // 4, 1)
        high, low = split(
            jnp.concatenate(
                [jnp.where(lane // vecs == k, inverse, 0.0) for k in range(group)], axis=0
            )
        )
        w_ref[...] = jnp.concatenate(
            [
                jnp.concatenate([high, high], axis=1),
                jnp.concatenate([low, jnp.zeros_like(low)], axis=1),
            ],
            axis=0,
        )

    block = vectors_ref.shape[0]
    rows = pl.ds(pl.multiple_of(pl.program_id(0) * block, block), block)
    for k in range(vectors_ref.shape[1] // LANES):
        at = slice(k * LANES, (k + 1) * LANES)
        both = dot(jnp.concatenate(split(stepped_ref[rows, at]), axis=1), w_ref[...], NT)
        vectors_ref[:, at] = both[:, :LANES] + both[:, LANES:]


def vmem():
    return pl.BlockSpec(memory_space=pltpu.VMEM)


def cost(flops, moved):
    return pl.CostEstimate(flops=int(flops), bytes_accessed=int(moved), transcendentals=0)


def body(tangents, base_flow, mode_mask, decay_rates, to_eigen, from_eigen):
    modes, planes, width = tangents.shape
    z_length = base_flow.shape[2]
    vecs = width // z_length
    row_devices, col_devices = lax.axis_size("row"), lax.axis_size("col")
    devices = row_devices * col_devices
    x_count, z_count = modes * row_devices, z_length * col_devices
    tiles = width // LANES
    rows = modes * tiles
    extra = -(-modes * z_length // LANES)
    size = tangents.size * 4
    both = ("col", "row")
    pitch = 8 * (z_count // 8 + 1 - z_count // 8 % 2)
    big = pltpu.CompilerParams(vmem_limit_bytes=40 * 2**20)
    small = pltpu.CompilerParams(vmem_limit_bytes=24 * 2**20)

    order = np.arange(x_count)
    order = (order % row_devices) * modes + order // row_devices
    halves = -(-x_count // LANES)
    points = np.arange(halves * LANES)
    points = np.where(points < x_count, points, points - (halves * LANES - x_count))
    sx_high, sx_low = halves_of_table(synthesis(x_count)[points][:, order].T)
    sx = np.concatenate([sx_high, sx_high, sx_low], axis=0)
    line_tables = parity_tables(z_count)
    gx = np.concatenate(
        halves_of_table(derivative_analysis(x_count, ALPHA_X)[order][:, points]), axis=0
    )

    steps = 1
    base = jnp.transpose(base_flow, (0, 2, 1)).reshape(modes * z_length, planes)
    packed = pl.pallas_call(
        functools.partial(pack_kernel, modes=modes, planes=planes, tiles=tiles, extra=extra),
        out_shape=jax.ShapeDtypeStruct((planes * (rows + extra), LANES), F32),
        in_specs=[vmem()] * 3,
        out_specs=vmem(),
        cost_estimate=cost(10**9, 2 * size),
        compiler_params=small,
        name="pack",
    )(base, tangents[: modes // 2], tangents[modes // 2 :])
    received = lax.all_to_all(
        packed.reshape(devices, rows + extra, 1, LANES), both, 0, 0, tiled=True
    ).reshape(packed.shape)

    returned = pl.pallas_call(
        functools.partial(
            transform_kernel, modes=modes, row_devices=row_devices,
            col_devices=col_devices, tiles=tiles, extra=extra, vecs=vecs,
        ),
        out_shape=jax.ShapeDtypeStruct((devices * rows, LANES), F32),
        in_specs=[vmem()] * 7,
        out_specs=vmem(),
        scratch_shapes=[pltpu.VMEM((z_count + 16, halves * LANES), F32)]
        + [pltpu.VMEM((pitch * vecs, LANES), F32)] * (2 * halves),
        cost_estimate=cost(2 * 10**10, 2 * size),
        compiler_params=big,
        name="transform",
    )(received, sx, *line_tables, gx)
    nonlinear = lax.all_to_all(
        returned.reshape(devices, rows, LANES), both, 0, 0, tiled=True
    ).reshape(returned.shape)

    lines = vecs * vecs // (2 * LANES) + 1
    height = modes * planes
    stepped, grams = pl.pallas_call(
        functools.partial(
            column_kernel, modes=modes, planes=planes, tiles=tiles, vecs=vecs,
            step_modes=modes // steps, x_count=x_count, z_count=z_count, z_length=z_length,
        ),
        out_shape=[
            jax.ShapeDtypeStruct((height, width), F32),
            jax.ShapeDtypeStruct((devices * lines, LANES), F32),
        ],
        grid=(steps,),
        in_specs=[vmem()] * 6,
        out_specs=[vmem()] * 2,
        scratch_shapes=[
            pltpu.VMEM((modes, width), F32),
            pltpu.VMEM((modes, width), F32),
            pltpu.VMEM((planes, LANES), F32),
            pltpu.VMEM((LANES, 2 * LANES), F32),
        ],
        cost_estimate=cost(10**10, 3 * size),
        compiler_params=small,
        name="column",
    )(nonlinear, tangents, mode_mask, decay_rates[None, :], to_eigen, from_eigen)
    grams = lax.all_to_all(
        grams.reshape(devices, lines, 1, LANES), both, 0, 0, tiled=True
    ).reshape(grams.shape)

    block = height // 2
    vectors, growth = pl.pallas_call(
        functools.partial(finish_kernel, devices=devices, vecs=vecs, panel=16),
        out_shape=[
            jax.ShapeDtypeStruct((height, width), F32),
            jax.ShapeDtypeStruct((1, vecs), F32),
        ],
        grid=(height // block,),
        in_specs=[vmem()] * 2,
        out_specs=[
            pl.BlockSpec((block, width), lambda i: (i, 0)),
            pl.BlockSpec((1, vecs), lambda i: (0, 0)),
        ],
        scratch_shapes=[pltpu.VMEM((2 * LANES, 2 * LANES), BF16)],
        cost_estimate=cost(2 * height * width * 256, 2 * size),
        compiler_params=small,
        name="finish",
    )(grams, stepped)
    return vectors.reshape(tangents.shape), growth[0]


def solution(mesh):
    placed = (P("row", None, "col"), P("row", None, "col"), P("row", "col"), P(), P(), P())
    return jax.shard_map(
        body, mesh=mesh, in_specs=placed, out_specs=(P("row", None, "col"), P()), check_vma=False
    )
```

```python
import functools

import jax
import jax.numpy as jnp
import numpy as np
from jax import lax
from jax.experimental import pallas as pl
from jax.experimental.pallas import tpu as pltpu
from jax.sharding import PartitionSpec as P

STEP_COEF = 10.0
VISCOSITY = 0.01
ALPHA_X = 0.5
BETA_Z = 1.0
LANES = 128
F32 = jnp.float32
BF16 = jnp.bfloat16
NN = (((1,), (0,)), ((), ()))
NT = (((1,), (1,)), ((), ()))
TN = (((0,), (0,)), ((), ()))


def synthesis(count):
    points = np.arange(count)[:, None]
    modes = np.arange(count)[None, :]
    middle = count // 2
    waves = np.where(modes <= middle, modes, modes - middle)
    angles = (points * waves % count) * (2.0 * np.pi / count)
    return np.where(modes <= middle, np.cos(angles), np.sin(angles))


def analysis(count):
    modes = np.arange(count)
    weights = np.where((modes == 0) | (modes == count // 2), 1.0 / count, 2.0 / count)
    return weights[:, None] * synthesis(count).T


def derivative_analysis(count, scale):
    middle = count // 2
    derivative = np.zeros((count, count))
    for k in range(1, middle):
        derivative[k, middle + k] = k
        derivative[middle + k, k] = -k
    return -scale * (derivative @ analysis(count))


def halves_of_table(table):
    table = np.asarray(table, np.float64)
    high = table.astype(np.float32).astype(jnp.bfloat16)
    low = (table - high.astype(np.float64)).astype(np.float32).astype(jnp.bfloat16)
    return np.stack([high, low])


def split(x):
    high = x.astype(BF16)
    return high, (x - high.astype(F32)).astype(BF16)


def dot(a, b, dims):
    return lax.dot_general(a, b, dims, preferred_element_type=F32)


def dot3(a, b, dims):
    return dot(a[0], b[0], dims) + (dot(a[0], b[1], dims) + dot(a[1], b[0], dims))


def stacked_dot(table, x):
    high, low = split(x)
    return dot(table, jnp.concatenate([high, high], axis=0), NN) + dot(
        table[:, : x.shape[0]], low, NN
    )


def tripled(table):
    high, low = halves_of_table(table)
    return np.concatenate([high, low, high], axis=1)


def table_dot(table_ref, high, low):
    return dot(table_ref[...], jnp.concatenate([high, high, low], axis=0), NN)


def parity_tables(count):
    middle = count // 2
    wide, tall = middle + 16, middle + 8
    to_points, to_modes = synthesis(count), analysis(count)
    weights = np.where(np.arange(middle + 1) % middle == 0, 1.0, 2.0)
    even_points = np.zeros((wide, wide))
    even_points[: middle + 1, : middle + 1] = to_points[: middle + 1, : middle + 1]
    odd_points = np.zeros((middle, middle))
    odd_points[1:, 1:] = to_points[1:middle, middle + 1 :]
    even_modes = np.zeros((tall, wide))
    even_modes[: middle + 1, : middle + 1] = to_modes[: middle + 1, : middle + 1] * weights
    odd_modes = np.zeros((middle, middle))
    odd_modes[1:, 1:] = 2.0 * to_modes[middle + 1 :, 1:middle]
    return [tripled(t) for t in (even_points, odd_points, even_modes, odd_modes)]


def to_parity_points(even_ref, odd_ref, x):
    high, low = split(x)
    wide, middle = even_ref.shape[0], odd_ref.shape[0]
    return (
        table_dot(even_ref, high[:wide], low[:wide]),
        table_dot(odd_ref, high[middle:], low[middle:]),
    )


def pack_kernel(base_ref, *refs, modes, planes, tiles, extra):
    q_refs, out_ref = refs[:-1], refs[-1]
    share = modes // len(q_refs)
    stride = modes * tiles + extra
    part = base_ref.shape[0] // extra
    fill = jnp.zeros((LANES - part, planes), F32)
    for k in range(extra):
        block = jnp.concatenate([base_ref[k * part : (k + 1) * part, :], fill], axis=0)
        out_ref[pl.ds(modes * tiles + k, planes, stride=stride), :] = block.T
    for m in range(modes):
        for nb in range(tiles):
            out_ref[pl.ds(nb * modes + m, planes, stride=stride), :] = q_refs[m // share][
                m % share, :, nb * LANES : (nb + 1) * LANES
            ]


def transform_kernel(
    d_ref, sx_ref, even_p_ref, odd_p_ref, even_m_ref, odd_m_ref, g_ref, out_ref, speed_ref,
    *scratch,
    modes, row_devices, col_devices, tiles, extra, vecs,
):
    halves = len(scratch) // 2
    y_refs, z_refs = scratch[:halves], scratch[halves:]
    rows = modes * tiles
    stride = rows + extra
    x_count = modes * row_devices
    wide, tall, middle = even_p_ref.shape[0], even_m_ref.shape[0], odd_p_ref.shape[0]
    z_count = 2 * middle
    z_length = z_count // col_devices
    pitch = y_refs[0].shape[0] // vecs
    per_tile = LANES // vecs

    def forward_x(c, carry):
        parts = []
        for nb in range(tiles):
            start = c * (row_devices * stride) + nb * modes
            block = jnp.concatenate(
                [d_ref[pl.ds(start + m, row_devices, stride=stride), :] for m in range(modes)],
                axis=0,
            )
            block = jnp.concatenate(split(block), axis=0).T
            parts.append(jnp.concatenate([block, block[:, :x_count]], axis=1))
        mixed = dot(jnp.concatenate(parts, axis=0), sx_ref[...], NN)
        for n in range(z_length):
            for k, y_ref in enumerate(y_refs):
                y_ref[pl.ds(c * z_length + n, vecs, stride=pitch), :] = mixed[
                    n * vecs : (n + 1) * vecs, k * LANES : (k + 1) * LANES
                ]
        return carry

    lax.fori_loop(0, col_devices, forward_x, 0, unroll=8)

    turned = []
    for k in range(extra):
        block = d_ref[pl.ds(rows + k, row_devices * col_devices, stride=stride), :]
        turned.append(block.T)
    slot = lax.broadcasted_iota(jnp.int32, (z_length, LANES), 1) // row_devices
    slots = LANES // row_devices
    share = modes // extra
    sheets = []
    for c in range(col_devices):
        parts = [jnp.zeros((z_length, LANES), F32) for _ in range(halves)]
        for m in range(modes):
            piece = turned[m // share][(m % share) * z_length : (m % share + 1) * z_length]
            shift = ((m % slots - c) * row_devices) % LANES
            piece = pltpu.roll(piece, shift, 1) if shift else piece
            parts[m // slots] = jnp.where(slot == m % slots, piece, parts[m // slots])
        sheets.append(jnp.concatenate(parts, axis=1))
    base = jnp.concatenate(sheets, axis=0)[:, :x_count]
    sx = (sx_ref[:x_count], sx_ref[2 * x_count :])
    even, odd = to_parity_points(even_p_ref, odd_p_ref, dot3(split(base), sx, NN))
    speed_ref[:wide] = even
    speed_ref[wide:] = odd

    y_low, y_high = y_refs
    z_low, z_high = z_refs
    first = lax.broadcasted_iota(jnp.int32, (z_count, LANES), 1) < LANES // 2
    batch = 8

    def plane(i, carry):
        ats = [
            pl.ds(pl.multiple_of((i * batch + j) * pitch, 8), z_count) for j in range(batch)
        ]
        mixed = jnp.concatenate(
            [y_low[at, :] for at in ats]
            + [
                jnp.where(first, y_high[ats[j], :], y_high[ats[j + 1], :])
                for j in range(0, batch, 2)
            ],
            axis=1,
        )
        speed = jnp.concatenate(
            [speed_ref[:, :LANES]] * batch + [speed_ref[:, LANES:]] * (batch // 2), axis=1
        )
        even, odd = to_parity_points(even_p_ref, odd_p_ref, mixed)
        even_speed, odd_speed = speed[:wide], speed[wide:]
        cross = even[:middle] * odd_speed + odd * even_speed[:middle]
        even = even * even_speed
        even = jnp.concatenate([even[:middle] + odd * odd_speed, even[middle:]], axis=0)
        even = table_dot(even_m_ref, *split(even))
        odd = table_dot(odd_m_ref, *split(cross))
        mixed = jnp.concatenate(
            [
                even[:middle],
                even[middle:] + odd[: tall - middle],
                odd[tall - middle :],
            ],
            axis=0,
        )
        for j, at in enumerate(ats):
            k = batch + j // 2
            z_low[at, :] = mixed[:, j * LANES : (j + 1) * LANES]
            z_high[at, :] = mixed[:, k * LANES : (k + 1) * LANES]
        return carry

    lax.fori_loop(0, vecs // batch, plane, 0, unroll=4)

    rows_of = lax.broadcasted_iota(jnp.int32, (vecs, LANES), 0)
    lanes_of = lax.broadcasted_iota(jnp.int32, (vecs, LANES), 1)
    mine = (rows_of % 2) == (lanes_of // (LANES // 2))

    def inverse_x(c, carry):
        block = jnp.concatenate(
            [
                jnp.concatenate(
                    [
                        z_low[pl.ds(c * z_length + n, vecs, stride=pitch), :],
                        jnp.where(
                            mine, z_high[pl.ds(c * z_length + n, vecs, stride=pitch), :], 0.0
                        ),
                    ],
                    axis=1,
                )
                for n in range(z_length)
            ],
            axis=0,
        )
        high, low = split(block)
        both = dot(g_ref[...], high, NT)
        back = both[:x_count] + (both[x_count:] + dot(g_ref[:x_count], low, NT))
        for nb in range(tiles):
            start = c * (row_devices * rows) + nb * modes
            for m in range(modes):
                out_ref[pl.ds(start + m, row_devices, stride=rows), :] = back[
                    m * row_devices : (m + 1) * row_devices, nb * LANES : (nb + 1) * LANES
                ]
        return carry

    lax.fori_loop(0, col_devices, inverse_x, 0, unroll=8)


def column_kernel(
    nl_ref, q_ref, mask_ref, decay_ref, to_ref, from_ref, stepped_ref, gram_ref,
    mask_s, wave_s, decay_s, gram_s,
    *, modes, planes, tiles, vecs, step_modes, x_count, z_count, z_length,
):
    width = tiles * LANES

    @pl.when(pl.program_id(0) == 0)
    def _():
        lane = lax.broadcasted_iota(jnp.int32, (z_length, width), 1) // vecs
        row = lax.broadcasted_iota(jnp.int32, (z_length, width), 0)
        spread = jnp.where(lane == row, 1.0, 0.0).astype(BF16)
        mask_s[...] = dot(mask_ref[...].astype(F32).astype(BF16), spread, NN)
        n = lax.broadcasted_iota(jnp.int32, (modes, width), 1) // vecs
        n = n + lax.axis_index("col") * z_length
        m = lax.broadcasted_iota(jnp.int32, (modes, width), 0)
        m = m + lax.axis_index("row") * modes
        wave_x = jnp.where(m <= x_count // 2, m, m - x_count // 2).astype(F32) * ALPHA_X
        wave_z = jnp.where(n <= z_count // 2, n, n - z_count // 2).astype(F32) * BETA_Z
        wave_s[...] = STEP_COEF + VISCOSITY * (wave_x * wave_x + wave_z * wave_z)
        decay_s[...] = jnp.broadcast_to(decay_ref[...], (LANES, planes)).T
        gram_s[...] = jnp.zeros_like(gram_s)

    to_eigen = jnp.concatenate(split(to_ref[...]), axis=1)
    from_eigen = jnp.concatenate(split(from_ref[...]), axis=1)
    decay = jnp.concatenate([decay_s[...]] * tiles, axis=1)
    gram = gram_s[...]
    for k in range(step_modes):
        m = pl.program_id(0) * step_modes + k
        nonlinear = jnp.concatenate(
            [
                nl_ref[pl.ds(nb * modes + m, planes, stride=tiles * modes), :]
                for nb in range(tiles)
            ],
            axis=1,
        )
        right = STEP_COEF * q_ref[m] + nonlinear * mask_s[pl.ds(m, 1), :]
        eigen = stacked_dot(to_eigen, right)
        eigen = eigen / (wave_s[pl.ds(m, 1), :] + decay)
        stepped = stacked_dot(from_eigen, eigen)
        stepped_ref[pl.ds(pl.multiple_of(m * planes, planes), planes), :] = stepped
        columns = [stepped[:, nb * LANES : (nb + 1) * LANES] for nb in range(tiles)]
        left = jnp.concatenate([x.T.astype(BF16) for x in columns], axis=1)
        right = jnp.concatenate(
            [jnp.concatenate(split(x), axis=1) for x in columns], axis=0
        )
        gram = gram + dot(left, right, NN)
    gram_s[...] = gram

    @pl.when(pl.program_id(0) == pl.num_programs(0) - 1)
    def _():
        high, cross = gram[:, :LANES], gram[:, LANES:]
        full = (high + (cross + cross.T)) * (1.0 / (x_count * planes * z_count))
        group = LANES // vecs
        lane = lax.broadcasted_iota(jnp.int32, (vecs, LANES), 1) // vecs
        folded = jnp.zeros((vecs, LANES), F32)
        for k in range(group):
            folded = folded + jnp.where(lane == k, full[k * vecs : (k + 1) * vecs], 0.0)
        folded = folded + pltpu.roll(folded, LANES // 2, 1)
        folded = folded + pltpu.roll(folded, LANES // 4, 1)
        half = vecs // 2
        lane = lax.broadcasted_iota(jnp.int32, (half, LANES), 1)
        row = lax.broadcasted_iota(jnp.int32, (half, LANES), 0)
        top, shifted = folded[:half], pltpu.roll(folded[half:], LANES - half, 1)
        square = jnp.where((lane % vecs < half) & (lane % vecs < row), shifted, top)
        piece = half // group
        spread = lane[:piece] // vecs
        packed = jnp.zeros((piece, LANES), F32)
        for k in range(group):
            packed = jnp.where(spread == k, square[k * piece : (k + 1) * piece], packed)
        diagonal = jnp.sum(jnp.where(lane % vecs == row, shifted, 0.0), axis=0, keepdims=True)
        sent = [packed[k : k + 1] for k in range(piece)] + [diagonal]
        for k, line in enumerate(sent):
            gram_ref[pl.ds(k, planes, stride=len(sent)), :] = jnp.broadcast_to(
                line, (planes, LANES)
            )


def finish_kernel(grams_ref, stepped_ref, vectors_ref, growth_ref, w_ref, *, devices, vecs, panel):
    group = LANES // vecs
    half = vecs // 2
    piece = half // group

    @pl.when(pl.program_id(0) == 0)
    def _():
        lines = [
            jnp.sum(
                grams_ref[pl.ds(k, devices, stride=piece + 1), :], axis=0, keepdims=True
            )
            for k in range(piece + 1)
        ]
        packed = jnp.concatenate(lines[:piece], axis=0)
        square = jnp.concatenate(
            [pltpu.roll(packed, (LANES - k * vecs) % LANES, 1) for k in range(group)], axis=0
        )
        turned = jnp.concatenate([square, jnp.zeros((LANES - half, LANES), F32)], axis=0).T
        lane = lax.broadcasted_iota(jnp.int32, (half, LANES), 1)
        row = lax.broadcasted_iota(jnp.int32, (half, LANES), 0)
        top = jnp.where((lane < half) & (lane < row), turned[:half], square)
        right = jnp.where(lane < row, square, jnp.where(lane == row, lines[piece], turned[:half]))
        bottom = jnp.where(lane < half, turned[half:vecs], pltpu.roll(right, half, 1))
        gram = jnp.concatenate([top, bottom], axis=0)
        lane = lax.broadcasted_iota(jnp.int32, (vecs, LANES), 1)
        row = lax.broadcasted_iota(jnp.int32, (vecs, LANES), 0)
        work = jnp.where(lane < vecs, gram, jnp.where(lane == row + vecs, 1.0, 0.0))
        for first in range(0, vecs, panel):
            own = range(first, first + panel)
            columns = [jnp.broadcast_to(work[:, k : k + 1], (vecs, LANES)) for k in own]
            lines = [work[k : k + 1, :] for k in own]
            for j, k in enumerate(own):
                pivot = columns[j][k : k + 1]
                column = jnp.where(row > k, columns[j], 0.0)
                scaled = lines[j] / pivot
                for i in range(j + 1, panel):
                    columns[i] = columns[i] - column * (columns[i][k : k + 1] / pivot)
                    lines[i] = lines[i] - columns[j][first + i : first + i + 1] * scaled
                work = work - column * scaled
        pivots = jnp.sum(jnp.where(lane == row, work, 0.0), axis=1, keepdims=True)
        diagonal = jnp.sqrt(pivots)
        inverse = work / diagonal
        across = jnp.sum(jnp.where(lane == row, diagonal, 0.0), axis=0, keepdims=True)
        growth_ref[...] = jnp.log(across[:, :vecs])
        inverse = jnp.where((lane >= vecs) & (lane < 2 * vecs), inverse, 0.0)
        inverse = inverse + pltpu.roll(inverse, LANES // 2, 1)
        inverse = inverse + pltpu.roll(inverse, LANES // 4, 1)
        high, low = split(
            jnp.concatenate(
                [jnp.where(lane // vecs == k, inverse, 0.0) for k in range(group)], axis=0
            )
        )
        w_ref[...] = jnp.concatenate(
            [
                jnp.concatenate([high, high], axis=1),
                jnp.concatenate([low, jnp.zeros_like(low)], axis=1),
            ],
            axis=0,
        )

    block = vectors_ref.shape[0]
    rows = pl.ds(pl.multiple_of(pl.program_id(0) * block, block), block)
    for k in range(vectors_ref.shape[1] // LANES):
        at = slice(k * LANES, (k + 1) * LANES)
        both = dot(jnp.concatenate(split(stepped_ref[rows, at]), axis=1), w_ref[...], NT)
        vectors_ref[:, at] = both[:, :LANES] + both[:, LANES:]


def vmem():
    return pl.BlockSpec(memory_space=pltpu.VMEM)


def cost(flops, moved):
    return pl.CostEstimate(flops=int(flops), bytes_accessed=int(moved), transcendentals=0)


def body(tangents, base_flow, mode_mask, decay_rates, to_eigen, from_eigen):
    modes, planes, width = tangents.shape
    z_length = base_flow.shape[2]
    vecs = width // z_length
    row_devices, col_devices = lax.axis_size("row"), lax.axis_size("col")
    devices = row_devices * col_devices
    x_count, z_count = modes * row_devices, z_length * col_devices
    tiles = width // LANES
    rows = modes * tiles
    extra = -(-modes * z_length // LANES)
    size = tangents.size * 4
    both = ("col", "row")
    pitch = 8 * (z_count // 8 + 1 - z_count // 8 % 2)
    big = pltpu.CompilerParams(vmem_limit_bytes=40 * 2**20)
    small = pltpu.CompilerParams(vmem_limit_bytes=24 * 2**20)

    order = np.arange(x_count)
    order = (order % row_devices) * modes + order // row_devices
    halves = -(-x_count // LANES)
    points = np.arange(halves * LANES)
    points = np.where(points < x_count, points, points - (halves * LANES - x_count))
    sx_high, sx_low = halves_of_table(synthesis(x_count)[points][:, order].T)
    sx = np.concatenate([sx_high, sx_high, sx_low], axis=0)
    line_tables = parity_tables(z_count)
    gx = np.concatenate(
        halves_of_table(derivative_analysis(x_count, ALPHA_X)[order][:, points]), axis=0
    )

    steps = 1
    base = jnp.transpose(base_flow, (0, 2, 1)).reshape(modes * z_length, planes)
    packed = pl.pallas_call(
        functools.partial(pack_kernel, modes=modes, planes=planes, tiles=tiles, extra=extra),
        out_shape=jax.ShapeDtypeStruct((planes * (rows + extra), LANES), F32),
        in_specs=[vmem()] * 3,
        out_specs=vmem(),
        cost_estimate=cost(10**9, 2 * size),
        compiler_params=small,
        name="pack",
    )(base, tangents[: modes // 2], tangents[modes // 2 :])
    received = lax.all_to_all(
        packed.reshape(devices, rows + extra, 1, LANES), both, 0, 0, tiled=True
    ).reshape(packed.shape)

    returned = pl.pallas_call(
        functools.partial(
            transform_kernel, modes=modes, row_devices=row_devices,
            col_devices=col_devices, tiles=tiles, extra=extra, vecs=vecs,
        ),
        out_shape=jax.ShapeDtypeStruct((devices * rows, LANES), F32),
        in_specs=[vmem()] * 7,
        out_specs=vmem(),
        scratch_shapes=[pltpu.VMEM((z_count + 16, halves * LANES), F32)]
        + [pltpu.VMEM((pitch * vecs, LANES), F32)] * (2 * halves),
        cost_estimate=cost(2 * 10**10, 2 * size),
        compiler_params=big,
        name="transform",
    )(received, sx, *line_tables, gx)
    nonlinear = lax.all_to_all(
        returned.reshape(devices, rows, LANES), both, 0, 0, tiled=True
    ).reshape(returned.shape)

    lines = vecs * vecs // (2 * LANES) + 1
    height = modes * planes
    stepped, grams = pl.pallas_call(
        functools.partial(
            column_kernel, modes=modes, planes=planes, tiles=tiles, vecs=vecs,
            step_modes=modes // steps, x_count=x_count, z_count=z_count, z_length=z_length,
        ),
        out_shape=[
            jax.ShapeDtypeStruct((height, width), F32),
            jax.ShapeDtypeStruct((devices * lines, LANES), F32),
        ],
        grid=(steps,),
        in_specs=[vmem()] * 6,
        out_specs=[vmem()] * 2,
        scratch_shapes=[
            pltpu.VMEM((modes, width), F32),
            pltpu.VMEM((modes, width), F32),
            pltpu.VMEM((planes, LANES), F32),
            pltpu.VMEM((LANES, 2 * LANES), F32),
        ],
        cost_estimate=cost(10**10, 3 * size),
        compiler_params=small,
        name="column",
    )(nonlinear, tangents, mode_mask, decay_rates[None, :], to_eigen, from_eigen)
    grams = lax.all_to_all(
        grams.reshape(devices, lines, 1, LANES), both, 0, 0, tiled=True
    ).reshape(grams.shape)

    block = height // 2
    vectors, growth = pl.pallas_call(
        functools.partial(finish_kernel, devices=devices, vecs=vecs, panel=8),
        out_shape=[
            jax.ShapeDtypeStruct((height, width), F32),
            jax.ShapeDtypeStruct((1, vecs), F32),
        ],
        grid=(height // block,),
        in_specs=[vmem()] * 2,
        out_specs=[
            pl.BlockSpec((block, width), lambda i: (i, 0)),
            pl.BlockSpec((1, vecs), lambda i: (0, 0)),
        ],
        scratch_shapes=[pltpu.VMEM((2 * LANES, 2 * LANES), BF16)],
        cost_estimate=cost(2 * height * width * 256, 2 * size),
        compiler_params=small,
        name="finish",
    )(grams, stepped)
    return vectors.reshape(tangents.shape), growth[0]


def solution(mesh):
    placed = (P("row", None, "col"), P("row", None, "col"), P("row", "col"), P(), P(), P())
    return jax.shard_map(
        body, mesh=mesh, in_specs=placed, out_specs=(P("row", None, "col"), P()), check_vma=False
    )
```

```python
import functools

import jax
import jax.numpy as jnp
import numpy as np
from jax import lax
from jax.experimental import pallas as pl
from jax.experimental.pallas import tpu as pltpu
from jax.sharding import PartitionSpec as P

STEP_COEF = 10.0
VISCOSITY = 0.01
ALPHA_X = 0.5
BETA_Z = 1.0
LANES = 128
F32 = jnp.float32
BF16 = jnp.bfloat16
NN = (((1,), (0,)), ((), ()))
NT = (((1,), (1,)), ((), ()))
TN = (((0,), (0,)), ((), ()))


def synthesis(count):
    points = np.arange(count)[:, None]
    modes = np.arange(count)[None, :]
    middle = count // 2
    waves = np.where(modes <= middle, modes, modes - middle)
    angles = (points * waves % count) * (2.0 * np.pi / count)
    return np.where(modes <= middle, np.cos(angles), np.sin(angles))


def analysis(count):
    modes = np.arange(count)
    weights = np.where((modes == 0) | (modes == count // 2), 1.0 / count, 2.0 / count)
    return weights[:, None] * synthesis(count).T


def derivative_analysis(count, scale):
    middle = count // 2
    derivative = np.zeros((count, count))
    for k in range(1, middle):
        derivative[k, middle + k] = k
        derivative[middle + k, k] = -k
    return -scale * (derivative @ analysis(count))


def halves_of_table(table):
    table = np.asarray(table, np.float64)
    high = table.astype(np.float32).astype(jnp.bfloat16)
    low = (table - high.astype(np.float64)).astype(np.float32).astype(jnp.bfloat16)
    return np.stack([high, low])


def split(x):
    high = x.astype(BF16)
    return high, (x - high.astype(F32)).astype(BF16)


def dot(a, b, dims):
    return lax.dot_general(a, b, dims, preferred_element_type=F32)


def dot3(a, b, dims):
    return dot(a[0], b[0], dims) + (dot(a[0], b[1], dims) + dot(a[1], b[0], dims))


def stacked_dot(table, x):
    high, low = split(x)
    return dot(table, jnp.concatenate([high, high], axis=0), NN) + dot(
        table[:, : x.shape[0]], low, NN
    )


def tripled(table):
    high, low = halves_of_table(table)
    return np.concatenate([high, low, high], axis=1)


def table_dot(table_ref, high, low):
    return dot(table_ref[...], jnp.concatenate([high, high, low], axis=0), NN)


def parity_tables(count):
    middle = count // 2
    wide, tall = middle + 16, middle + 8
    to_points, to_modes = synthesis(count), analysis(count)
    weights = np.where(np.arange(middle + 1) % middle == 0, 1.0, 2.0)
    even_points = np.zeros((wide, wide))
    even_points[: middle + 1, : middle + 1] = to_points[: middle + 1, : middle + 1]
    odd_points = np.zeros((middle, middle))
    odd_points[1:, 1:] = to_points[1:middle, middle + 1 :]
    even_modes = np.zeros((tall, wide))
    even_modes[: middle + 1, : middle + 1] = to_modes[: middle + 1, : middle + 1] * weights
    odd_modes = np.zeros((middle, middle))
    odd_modes[1:, 1:] = 2.0 * to_modes[middle + 1 :, 1:middle]
    return [tripled(t) for t in (even_points, odd_points, even_modes, odd_modes)]


def to_parity_points(even_ref, odd_ref, x):
    high, low = split(x)
    wide, middle = even_ref.shape[0], odd_ref.shape[0]
    return (
        table_dot(even_ref, high[:wide], low[:wide]),
        table_dot(odd_ref, high[middle:], low[middle:]),
    )


def pack_kernel(base_ref, *refs, modes, planes, tiles, extra):
    q_refs, out_ref = refs[:-1], refs[-1]
    share = modes // len(q_refs)
    stride = modes * tiles + extra
    part = base_ref.shape[0] // extra
    fill = jnp.zeros((LANES - part, planes), F32)
    for k in range(extra):
        block = jnp.concatenate([base_ref[k * part : (k + 1) * part, :], fill], axis=0)
        out_ref[pl.ds(modes * tiles + k, planes, stride=stride), :] = block.T
    for m in range(modes):
        for nb in range(tiles):
            out_ref[pl.ds(nb * modes + m, planes, stride=stride), :] = q_refs[m // share][
                m % share, :, nb * LANES : (nb + 1) * LANES
            ]


def transform_kernel(
    d_ref, sx_ref, even_p_ref, odd_p_ref, even_m_ref, odd_m_ref, g_ref, out_ref, speed_ref,
    *scratch,
    modes, row_devices, col_devices, tiles, extra, vecs,
):
    halves = len(scratch) // 2
    y_refs, z_refs = scratch[:halves], scratch[halves:]
    rows = modes * tiles
    stride = rows + extra
    x_count = modes * row_devices
    wide, tall, middle = even_p_ref.shape[0], even_m_ref.shape[0], odd_p_ref.shape[0]
    z_count = 2 * middle
    z_length = z_count // col_devices
    pitch = y_refs[0].shape[0] // vecs
    per_tile = LANES // vecs

    def forward_x(c, carry):
        parts = []
        for nb in range(tiles):
            start = c * (row_devices * stride) + nb * modes
            block = jnp.concatenate(
                [d_ref[pl.ds(start + m, row_devices, stride=stride), :] for m in range(modes)],
                axis=0,
            )
            block = jnp.concatenate(split(block), axis=0).T
            parts.append(jnp.concatenate([block, block[:, :x_count]], axis=1))
        mixed = dot(jnp.concatenate(parts, axis=0), sx_ref[...], NN)
        for n in range(z_length):
            for k, y_ref in enumerate(y_refs):
                y_ref[pl.ds(c * z_length + n, vecs, stride=pitch), :] = mixed[
                    n * vecs : (n + 1) * vecs, k * LANES : (k + 1) * LANES
                ]
        return carry

    lax.fori_loop(0, col_devices, forward_x, 0, unroll=8)

    turned = []
    for k in range(extra):
        block = d_ref[pl.ds(rows + k, row_devices * col_devices, stride=stride), :]
        turned.append(block.T)
    slot = lax.broadcasted_iota(jnp.int32, (z_length, LANES), 1) // row_devices
    slots = LANES // row_devices
    share = modes // extra
    sheets = []
    for c in range(col_devices):
        parts = [jnp.zeros((z_length, LANES), F32) for _ in range(halves)]
        for m in range(modes):
            piece = turned[m // share][(m % share) * z_length : (m % share + 1) * z_length]
            shift = ((m % slots - c) * row_devices) % LANES
            piece = pltpu.roll(piece, shift, 1) if shift else piece
            parts[m // slots] = jnp.where(slot == m % slots, piece, parts[m // slots])
        sheets.append(jnp.concatenate(parts, axis=1))
    base = jnp.concatenate(sheets, axis=0)[:, :x_count]
    sx = (sx_ref[:x_count], sx_ref[2 * x_count :])
    even, odd = to_parity_points(even_p_ref, odd_p_ref, dot3(split(base), sx, NN))
    speed_ref[:wide] = even
    speed_ref[wide:] = odd

    y_low, y_high = y_refs
    z_low, z_high = z_refs
    first = lax.broadcasted_iota(jnp.int32, (z_count, LANES), 1) < LANES // 2
    batch = 8

    def plane(i, carry):
        ats = [
            pl.ds(pl.multiple_of((i * batch + j) * pitch, 8), z_count) for j in range(batch)
        ]
        mixed = jnp.concatenate(
            [y_low[at, :] for at in ats]
            + [
                jnp.where(first, y_high[ats[j], :], y_high[ats[j + 1], :])
                for j in range(0, batch, 2)
            ],
            axis=1,
        )
        speed = jnp.concatenate(
            [speed_ref[:, :LANES]] * batch + [speed_ref[:, LANES:]] * (batch // 2), axis=1
        )
        even, odd = to_parity_points(even_p_ref, odd_p_ref, mixed)
        even_speed, odd_speed = speed[:wide], speed[wide:]
        cross = even[:middle] * odd_speed + odd * even_speed[:middle]
        even = even * even_speed
        even = jnp.concatenate([even[:middle] + odd * odd_speed, even[middle:]], axis=0)
        even = table_dot(even_m_ref, *split(even))
        odd = table_dot(odd_m_ref, *split(cross))
        mixed = jnp.concatenate(
            [
                even[:middle],
                even[middle:] + odd[: tall - middle],
                odd[tall - middle :],
            ],
            axis=0,
        )
        for j, at in enumerate(ats):
            k = batch + j // 2
            z_low[at, :] = mixed[:, j * LANES : (j + 1) * LANES]
            z_high[at, :] = mixed[:, k * LANES : (k + 1) * LANES]
        return carry

    lax.fori_loop(0, vecs // batch, plane, 0, unroll=4)

    rows_of = lax.broadcasted_iota(jnp.int32, (vecs, LANES), 0)
    lanes_of = lax.broadcasted_iota(jnp.int32, (vecs, LANES), 1)
    mine = (rows_of % 2) == (lanes_of // (LANES // 2))

    def inverse_x(c, carry):
        block = jnp.concatenate(
            [
                jnp.concatenate(
                    [
                        z_low[pl.ds(c * z_length + n, vecs, stride=pitch), :],
                        jnp.where(
                            mine, z_high[pl.ds(c * z_length + n, vecs, stride=pitch), :], 0.0
                        ),
                    ],
                    axis=1,
                )
                for n in range(z_length)
            ],
            axis=0,
        )
        high, low = split(block)
        both = dot(g_ref[...], high, NT)
        back = both[:x_count] + (both[x_count:] + dot(g_ref[:x_count], low, NT))
        for nb in range(tiles):
            start = c * (row_devices * rows) + nb * modes
            for m in range(modes):
                out_ref[pl.ds(start + m, row_devices, stride=rows), :] = back[
                    m * row_devices : (m + 1) * row_devices, nb * LANES : (nb + 1) * LANES
                ]
        return carry

    lax.fori_loop(0, col_devices, inverse_x, 0, unroll=8)


def column_kernel(
    nl_ref, q_ref, mask_ref, decay_ref, to_ref, from_ref, stepped_ref, gram_ref,
    mask_s, wave_s, decay_s, gram_s,
    *, modes, planes, tiles, vecs, step_modes, x_count, z_count, z_length,
):
    width = tiles * LANES

    @pl.when(pl.program_id(0) == 0)
    def _():
        lane = lax.broadcasted_iota(jnp.int32, (z_length, width), 1) // vecs
        row = lax.broadcasted_iota(jnp.int32, (z_length, width), 0)
        spread = jnp.where(lane == row, 1.0, 0.0).astype(BF16)
        mask_s[...] = dot(mask_ref[...].astype(F32).astype(BF16), spread, NN)
        n = lax.broadcasted_iota(jnp.int32, (modes, width), 1) // vecs
        n = n + lax.axis_index("col") * z_length
        m = lax.broadcasted_iota(jnp.int32, (modes, width), 0)
        m = m + lax.axis_index("row") * modes
        wave_x = jnp.where(m <= x_count // 2, m, m - x_count // 2).astype(F32) * ALPHA_X
        wave_z = jnp.where(n <= z_count // 2, n, n - z_count // 2).astype(F32) * BETA_Z
        wave_s[...] = STEP_COEF + VISCOSITY * (wave_x * wave_x + wave_z * wave_z)
        decay_s[...] = jnp.broadcast_to(decay_ref[...], (LANES, planes)).T
        gram_s[...] = jnp.zeros_like(gram_s)

    to_eigen = jnp.concatenate(split(to_ref[...]), axis=1)
    from_eigen = jnp.concatenate(split(from_ref[...]), axis=1)
    decay = jnp.concatenate([decay_s[...]] * tiles, axis=1)
    gram = gram_s[...]
    for k in range(step_modes):
        m = pl.program_id(0) * step_modes + k
        nonlinear = jnp.concatenate(
            [
                nl_ref[pl.ds(nb * modes + m, planes, stride=tiles * modes), :]
                for nb in range(tiles)
            ],
            axis=1,
        )
        right = STEP_COEF * q_ref[m] + nonlinear * mask_s[pl.ds(m, 1), :]
        eigen = stacked_dot(to_eigen, right)
        eigen = eigen / (wave_s[pl.ds(m, 1), :] + decay)
        stepped = stacked_dot(from_eigen, eigen)
        stepped_ref[pl.ds(pl.multiple_of(m * planes, planes), planes), :] = stepped
        columns = [stepped[:, nb * LANES : (nb + 1) * LANES] for nb in range(tiles)]
        left = jnp.concatenate([x.T.astype(BF16) for x in columns], axis=1)
        right = jnp.concatenate(
            [jnp.concatenate(split(x), axis=1) for x in columns], axis=0
        )
        gram = gram + dot(left, right, NN)
    gram_s[...] = gram

    @pl.when(pl.program_id(0) == pl.num_programs(0) - 1)
    def _():
        high, cross = gram[:, :LANES], gram[:, LANES:]
        full = (high + (cross + cross.T)) * (1.0 / (x_count * planes * z_count))
        group = LANES // vecs
        lane = lax.broadcasted_iota(jnp.int32, (vecs, LANES), 1) // vecs
        folded = jnp.zeros((vecs, LANES), F32)
        for k in range(group):
            folded = folded + jnp.where(lane == k, full[k * vecs : (k + 1) * vecs], 0.0)
        folded = folded + pltpu.roll(folded, LANES // 2, 1)
        folded = folded + pltpu.roll(folded, LANES // 4, 1)
        half = vecs // 2
        lane = lax.broadcasted_iota(jnp.int32, (half, LANES), 1)
        row = lax.broadcasted_iota(jnp.int32, (half, LANES), 0)
        top, shifted = folded[:half], pltpu.roll(folded[half:], LANES - half, 1)
        square = jnp.where((lane % vecs < half) & (lane % vecs < row), shifted, top)
        piece = half // group
        spread = lane[:piece] // vecs
        packed = jnp.zeros((piece, LANES), F32)
        for k in range(group):
            packed = jnp.where(spread == k, square[k * piece : (k + 1) * piece], packed)
        diagonal = jnp.sum(jnp.where(lane % vecs == row, shifted, 0.0), axis=0, keepdims=True)
        sent = [packed[k : k + 1] for k in range(piece)] + [diagonal]
        for k, line in enumerate(sent):
            gram_ref[pl.ds(k, planes, stride=len(sent)), :] = jnp.broadcast_to(
                line, (planes, LANES)
            )


def finish_kernel(grams_ref, stepped_ref, vectors_ref, growth_ref, w_ref, *, devices, vecs, panel):
    group = LANES // vecs
    half = vecs // 2
    piece = half // group

    @pl.when(pl.program_id(0) == 0)
    def _():
        lines = [
            jnp.sum(
                grams_ref[pl.ds(k, devices, stride=piece + 1), :], axis=0, keepdims=True
            )
            for k in range(piece + 1)
        ]
        packed = jnp.concatenate(lines[:piece], axis=0)
        square = jnp.concatenate(
            [pltpu.roll(packed, (LANES - k * vecs) % LANES, 1) for k in range(group)], axis=0
        )
        turned = jnp.concatenate([square, jnp.zeros((LANES - half, LANES), F32)], axis=0).T
        lane = lax.broadcasted_iota(jnp.int32, (half, LANES), 1)
        row = lax.broadcasted_iota(jnp.int32, (half, LANES), 0)
        top = jnp.where((lane < half) & (lane < row), turned[:half], square)
        right = jnp.where(lane < row, square, jnp.where(lane == row, lines[piece], turned[:half]))
        bottom = jnp.where(lane < half, turned[half:vecs], pltpu.roll(right, half, 1))
        gram = jnp.concatenate([top, bottom], axis=0)
        lane = lax.broadcasted_iota(jnp.int32, (vecs, LANES), 1)
        row = lax.broadcasted_iota(jnp.int32, (vecs, LANES), 0)
        work = jnp.where(lane < vecs, gram, jnp.where(lane == row + vecs, 1.0, 0.0))
        for first in range(0, vecs, panel):
            own = range(first, first + panel)
            columns = [jnp.broadcast_to(work[:, k : k + 1], (vecs, LANES)) for k in own]
            lines = [work[k : k + 1, :] for k in own]
            for j, k in enumerate(own):
                pivot = columns[j][k : k + 1]
                column = jnp.where(row > k, columns[j], 0.0)
                scaled = lines[j] / pivot
                for i in range(j + 1, panel):
                    columns[i] = columns[i] - column * (columns[i][k : k + 1] / pivot)
                    lines[i] = lines[i] - columns[j][first + i : first + i + 1] * scaled
                work = work - column * scaled
        pivots = jnp.sum(jnp.where(lane == row, work, 0.0), axis=1, keepdims=True)
        diagonal = jnp.sqrt(pivots)
        inverse = work / diagonal
        across = jnp.sum(jnp.where(lane == row, diagonal, 0.0), axis=0, keepdims=True)
        growth_ref[...] = jnp.log(across[:, :vecs])
        inverse = jnp.where((lane >= vecs) & (lane < 2 * vecs), inverse, 0.0)
        inverse = inverse + pltpu.roll(inverse, LANES // 2, 1)
        inverse = inverse + pltpu.roll(inverse, LANES // 4, 1)
        high, low = split(
            jnp.concatenate(
                [jnp.where(lane // vecs == k, inverse, 0.0) for k in range(group)], axis=0
            )
        )
        w_ref[...] = jnp.concatenate(
            [
                jnp.concatenate([high, high], axis=1),
                jnp.concatenate([low, jnp.zeros_like(low)], axis=1),
            ],
            axis=0,
        )

    block = vectors_ref.shape[0]
    rows = pl.ds(pl.multiple_of(pl.program_id(0) * block, block), block)
    for k in range(vectors_ref.shape[1] // LANES):
        at = slice(k * LANES, (k + 1) * LANES)
        both = dot(jnp.concatenate(split(stepped_ref[rows, at]), axis=1), w_ref[...], NT)
        vectors_ref[:, at] = both[:, :LANES] + both[:, LANES:]


def vmem():
    return pl.BlockSpec(memory_space=pltpu.VMEM)


def cost(flops, moved):
    return pl.CostEstimate(flops=int(flops), bytes_accessed=int(moved), transcendentals=0)


def body(tangents, base_flow, mode_mask, decay_rates, to_eigen, from_eigen):
    modes, planes, width = tangents.shape
    z_length = base_flow.shape[2]
    vecs = width // z_length
    row_devices, col_devices = lax.axis_size("row"), lax.axis_size("col")
    devices = row_devices * col_devices
    x_count, z_count = modes * row_devices, z_length * col_devices
    tiles = width // LANES
    rows = modes * tiles
    extra = -(-modes * z_length // LANES)
    size = tangents.size * 4
    both = ("col", "row")
    pitch = 8 * (z_count // 8 + 1 - z_count // 8 % 2)
    big = pltpu.CompilerParams(vmem_limit_bytes=40 * 2**20)
    small = pltpu.CompilerParams(vmem_limit_bytes=24 * 2**20)

    order = np.arange(x_count)
    order = (order % row_devices) * modes + order // row_devices
    halves = -(-x_count // LANES)
    points = np.arange(halves * LANES)
    points = np.where(points < x_count, points, points - (halves * LANES - x_count))
    sx_high, sx_low = halves_of_table(synthesis(x_count)[points][:, order].T)
    sx = np.concatenate([sx_high, sx_high, sx_low], axis=0)
    line_tables = parity_tables(z_count)
    gx = np.concatenate(
        halves_of_table(derivative_analysis(x_count, ALPHA_X)[order][:, points]), axis=0
    )

    steps = 1
    base = jnp.transpose(base_flow, (0, 2, 1)).reshape(modes * z_length, planes)
    packed = pl.pallas_call(
        functools.partial(pack_kernel, modes=modes, planes=planes, tiles=tiles, extra=extra),
        out_shape=jax.ShapeDtypeStruct((planes * (rows + extra), LANES), F32),
        in_specs=[vmem()] * 3,
        out_specs=vmem(),
        cost_estimate=cost(10**9, 2 * size),
        compiler_params=small,
        name="pack",
    )(base, tangents[: modes // 2], tangents[modes // 2 :])
    received = lax.all_to_all(
        packed.reshape(devices, rows + extra, 1, LANES), both, 0, 0, tiled=True
    ).reshape(packed.shape)

    returned = pl.pallas_call(
        functools.partial(
            transform_kernel, modes=modes, row_devices=row_devices,
            col_devices=col_devices, tiles=tiles, extra=extra, vecs=vecs,
        ),
        out_shape=jax.ShapeDtypeStruct((devices * rows, LANES), F32),
        in_specs=[vmem()] * 7,
        out_specs=vmem(),
        scratch_shapes=[pltpu.VMEM((z_count + 16, halves * LANES), F32)]
        + [pltpu.VMEM((pitch * vecs, LANES), F32)] * (2 * halves),
        cost_estimate=cost(2 * 10**10, 2 * size),
        compiler_params=big,
        name="transform",
    )(received, sx, *line_tables, gx)
    nonlinear = lax.all_to_all(
        returned.reshape(devices, rows, LANES), both, 0, 0, tiled=True
    ).reshape(returned.shape)

    lines = vecs * vecs // (2 * LANES) + 1
    height = modes * planes
    stepped, grams = pl.pallas_call(
        functools.partial(
            column_kernel, modes=modes, planes=planes, tiles=tiles, vecs=vecs,
            step_modes=modes // steps, x_count=x_count, z_count=z_count, z_length=z_length,
        ),
        out_shape=[
            jax.ShapeDtypeStruct((height, width), F32),
            jax.ShapeDtypeStruct((devices * lines, LANES), F32),
        ],
        grid=(steps,),
        in_specs=[vmem()] * 6,
        out_specs=[vmem()] * 2,
        scratch_shapes=[
            pltpu.VMEM((modes, width), F32),
            pltpu.VMEM((modes, width), F32),
            pltpu.VMEM((planes, LANES), F32),
            pltpu.VMEM((LANES, 2 * LANES), F32),
        ],
        cost_estimate=cost(10**10, 3 * size),
        compiler_params=small,
        name="column",
    )(nonlinear, tangents, mode_mask, decay_rates[None, :], to_eigen, from_eigen)
    grams = lax.all_to_all(
        grams.reshape(devices, lines, 1, LANES), both, 0, 0, tiled=True
    ).reshape(grams.shape)

    block = height // 2
    vectors, growth = pl.pallas_call(
        functools.partial(finish_kernel, devices=devices, vecs=vecs, panel=16),
        out_shape=[
            jax.ShapeDtypeStruct((height, width), F32),
            jax.ShapeDtypeStruct((1, vecs), F32),
        ],
        grid=(height // block,),
        in_specs=[vmem()] * 2,
        out_specs=[
            pl.BlockSpec((block, width), lambda i: (i, 0)),
            pl.BlockSpec((1, vecs), lambda i: (0, 0)),
        ],
        scratch_shapes=[pltpu.VMEM((2 * LANES, 2 * LANES), BF16)],
        cost_estimate=cost(2 * height * width * 256, 2 * size),
        compiler_params=small,
        name="finish",
    )(grams, stepped)
    return vectors.reshape(tangents.shape), growth[0]


def solution(mesh):
    placed = (P("row", None, "col"), P("row", None, "col"), P("row", "col"), P(), P(), P())
    return jax.shard_map(
        body, mesh=mesh, in_specs=placed, out_specs=(P("row", None, "col"), P()), check_vma=False
    )
```
